128 devices in a mesh: seq: 16 (over z_hi, y, core), tensor: 8 (over z_lo, x).
Axes of the slice: x: 4, y: 4, z: 4 (z_hi: 2, z_lo: 2; z = z_hi * 2 + z_lo), core: 2. Of those that a mesh axis runs over, the one named last changes fastest.
Arguments:
- tokens: bfloat16 [11520, 1536], P('seq'), may hold values from -6 to 6
- norm_gain: float32 [1536], replicated, may hold values from 0.1 to 1.9
- w_qkv: bfloat16 [1536, 3, 1536], P(None, None, 'tensor'), may hold values from -8 to 8
- w_out: bfloat16 [1536, 1536], P('tensor'), may hold values from -0.15625 to 0.15625
- post_gain: float32 [1536], replicated, may hold values from 0.1 to 1.9
- w_up: bfloat16 [1536, 6144], P(None, 'tensor'), may hold values from -0.15625 to 0.15625
- w_down: bfloat16 [6144, 1536], P('tensor'), may hold values from -0.078125 to 0.078125
Outputs:
- layer_out: bfloat16 [11520, 1536], P('seq')
The draws below stay inside these ranges and needn't reach their ends.
All inputs are finite; a program needn't handle non-finite values.
Results may differ from the reference program's by a relative error of at most 0.015.
Values may be sent and summed in bfloat16 or wider, within the bound.
A program may use at most 128 MiB of HBM per device.

```python
import math
import jax
import jax.numpy as jnp
from jax import lax

D = 1536
HEADS = 32
HD = 48
FF = 6144
TOK_DEV = 720
TOKENS = 11520
N_TENSOR = 8


def draw_w_qkv(key, part):
    base = jax.random.normal(key, (D, 3, HEADS * HD), jnp.float32) * D ** (-0.5)
    levels = jax.random.uniform(jax.random.fold_in(key, 3), (HEADS,), jnp.float32, math.log(1.5), math.log(3.5))
    sharpness = jnp.repeat(jnp.exp(levels), HD)
    query = base[:, 0, :] * sharpness[None, :]
    stacked = jnp.stack([query, base[:, 1, :], base[:, 2, :]], axis=1)
    return jnp.clip(stacked, -8.0, 8.0).astype(jnp.bfloat16)


def level_of(stream_key, shape, cuts, least, top_value):
    def one(dim, parts):
        steps = jax.random.uniform(jax.random.fold_in(jax.random.fold_in(stream_key, 6), dim), (parts,), jnp.float32, least / len(cuts), top_value / len(cuts))
        return jnp.repeat(jnp.exp(steps), shape[dim] // parts).reshape((-1,) + (1,) * (len(shape) - dim - 1))

    level = one(*cuts[0])
    for cut in cuts[1:]:
        level = level * one(*cut)
    return level


def scatter_about(rng, extent, scale, bound, split=(), dtype=jnp.bfloat16):
    loudness = level_of(rng, extent, split, -0.22, 0.18) if split else 1.0
    array = jax.random.normal(rng, extent, jnp.float32) * scale * loudness
    return jnp.minimum(jnp.maximum(array, -bound), bound).astype(dtype)


def setup_inputs(seed: int = 0) -> dict:
    key_list = jax.random.split(jax.random.key(seed), 8)
    return {
        "tokens": scatter_about(key_list[0], (TOKENS, D), 1.0, 6.0, ((0, 16),)),
        "norm_gain": jnp.clip(1.0 + 0.18 * jax.random.normal(key_list[1], (D,), jnp.float32), 0.1, 1.9),
        "w_qkv": draw_w_qkv(jax.random.fold_in(key_list[7], 71), 0),
        "w_out": scatter_about(key_list[3], (HEADS * HD, D), (HEADS * HD) ** -0.5, 0.15625, ((0, 8),)),
        "post_gain": jnp.clip(1.0 + 0.18 * jax.random.normal(key_list[4], (D,), jnp.float32), 0.1, 1.9),
        "w_up": scatter_about(key_list[5], (D, FF), D ** -0.5, 0.15625, ((1, 8),)),
        "w_down": scatter_about(key_list[6], (FF, D), FF ** -0.5, 0.078125, ((0, 8),)),
    }


def layer_norm(values, gain):
    mean = lax.optimization_barrier(jnp.mean(values, axis=-1, keepdims=True))
    centred = values - mean
    var = lax.optimization_barrier(jnp.mean(centred * centred, axis=-1, keepdims=True))
    return centred * lax.rsqrt(var + 1e-05) * gain

def one_head(operands):
    query, key, value = operands
    scale = 1.0 / HD ** 0.5

    def block(query_block):
        scores = jnp.dot(query_block, key.T, preferred_element_type=jnp.float32) * scale
        peak = lax.optimization_barrier(jnp.max(scores, axis=-1, keepdims=True))
        weights = jnp.exp(scores - peak)
        total = lax.optimization_barrier(jnp.sum(weights, axis=-1, keepdims=True))
        return jnp.dot(weights.astype(jnp.bfloat16), value, preferred_element_type=jnp.float32) / total
    blocks = query.reshape(TOKENS // TOK_DEV, TOK_DEV, HD)
    return lax.map(block, blocks).reshape(TOKENS, HD)

def grouped_sum(left, right):
    width = left.shape[1] // N_TENSOR
    result = jnp.zeros((left.shape[0], right.shape[1]), jnp.float32)
    for group in range(N_TENSOR):
        term = jnp.dot(left[:, group * width:(group + 1) * width], right[group * width:(group + 1) * width], preferred_element_type=jnp.float32)
        term = lax.optimization_barrier(term.astype(jnp.bfloat16))
        result = result + term.astype(jnp.float32)
    return result

def reference(tokens, norm_gain, w_qkv, w_out, post_gain, w_up, w_down):
    base = tokens.astype(jnp.float32)
    normed = layer_norm(base, norm_gain).astype(jnp.bfloat16)
    qkv = jnp.dot(normed, w_qkv.reshape(D, 3 * HEADS * HD), preferred_element_type=jnp.float32).astype(jnp.bfloat16)
    qkv = qkv.reshape(TOKENS, 3, HEADS, HD)
    query = jnp.transpose(qkv[:, 0], (1, 0, 2))
    key = jnp.transpose(qkv[:, 1], (1, 0, 2))
    value = jnp.transpose(qkv[:, 2], (1, 0, 2))
    heads = lax.map(one_head, (query, key, value))
    attended = jnp.transpose(heads, (1, 0, 2)).reshape(TOKENS, HEADS * HD).astype(jnp.bfloat16)
    mixed = base + grouped_sum(attended, w_out)
    post = layer_norm(mixed, post_gain).astype(jnp.bfloat16)
    hidden = jax.nn.gelu(jnp.dot(post, w_up, preferred_element_type=jnp.float32), approximate=True).astype(jnp.bfloat16)
    return (mixed + grouped_sum(hidden, w_down)).astype(jnp.bfloat16)
```

```python
import functools
import jax
import jax.numpy as jnp
from jax import lax
from jax.experimental import pallas as pl
from jax.experimental.pallas import tpu as pltpu
from jax.sharding import PartitionSpec as P

HD = 48
LOG2E = 1.4426950408889634
MESH = pl.DeviceIdType.MESH
F32 = jnp.float32
BF16 = jnp.bfloat16
RING = 4
BLOCKS = 16
TILES = (slice(0, 256), slice(256, 512), slice(512, 720))


def layer_norm(values, gain):
    mean = jnp.mean(values, axis=-1, keepdims=True)
    centred = values - mean
    var = jnp.mean(centred * centred, axis=-1, keepdims=True)
    return centred * lax.rsqrt(var + 1e-05) * gain


def dot(a, b):
    return jnp.dot(a, b, preferred_element_type=F32)


def remote(src, dst, send, recv, seq):
    return pltpu.make_async_remote_copy(
        src_ref=src, dst_ref=dst, send_sem=send, recv_sem=recv, device_id={"seq": seq}, device_id_type=MESH
    )


def attend_kernel(
    q_ref, kv_ref, out_ref, q_in, kv_in, key_rows, values, acc, peak, scores, obuf,
    q_send, q_recv, y_send, z_send, d_send, kv_recv, o_send, o_recv,
):
    rows = q_ref.shape[2]
    me = lax.axis_index("seq")
    half, y, core = me // (2 * RING), (me // 2) % RING, me % 2

    def at(step):
        return half * (2 * RING) + lax.rem(y + step, RING) * 2 + core

    twin = me - core + (1 - core)
    far = lax.rem(me + 2 * RING, BLOCKS)
    peers = [at(1), at(2), at(3), twin, far]
    barrier = pltpu.get_barrier_semaphore()
    for peer in peers:
        pl.semaphore_signal(barrier, inc=1, device_id={"seq": peer}, device_id_type=MESH)
    pl.semaphore_wait(barrier, len(peers))

    def q_copy(step):
        return remote(
            q_ref.at[lax.rem(y + step, RING)], q_in.at[RING - step], q_send.at[step], q_recv.at[RING - step], at(step)
        )

    def y_copy(step):
        slot = {1: 3, 2: 4, 3: 2}[step]
        return remote(
            kv_ref.at[lax.rem(y + step, RING)], kv_in.at[slot], y_send.at[step], kv_recv.at[slot], at(step)
        )

    def z_copy(src, slot):
        return remote(src, kv_in.at[slot], z_send.at[slot], kv_recv.at[slot], far)

    def d_copy(src, slot):
        return remote(src, kv_in.at[slot], d_send.at[slot], kv_recv.at[slot], twin)

    own = kv_ref.at[y]
    for step in (1, 3, 2):
        q_copy(step).start()
    d_copy(own, 1).start()
    for step in (1, 3, 2):
        y_copy(step).start()
    z_copy(own, 8).start()

    values[:, HD:, :] = jnp.ones((BLOCKS, values.shape[1] - HD, rows), BF16)
    acc[...] = jnp.zeros_like(acc)
    peak[...] = jnp.full_like(peak, -1e30)
    q_in[0] = q_ref[y]
    key_rows[0] = kv_ref[y, :HD].T
    values[0, :HD] = kv_ref[y, HD:]

    def arrive(c):
        d_copy(kv_in.at[c], c).wait_recv()

        @pl.when((c >= 2) & (c <= 4))
        def _():
            d_copy(kv_in.at[c], c + 3).start()
            z_copy(kv_in.at[c], 2 * c + 6).start()

        @pl.when((c >= 8) & (lax.rem(c, 2) == 0))
        def _():
            d_copy(kv_in.at[c], c + 1).start()

        key_rows[c] = kv_in[c, :HD].T
        values[c, :HD] = kv_in[c, HD:]

    def score(c, s, b):
        for lanes in TILES:
            found = dot(key_rows[c], q_in[s, :, lanes])
            scores[b, :rows, lanes] = found
            scores[b, rows : rows + 1, lanes] = jnp.max(found, axis=0, keepdims=True)

    def weigh(c, s, b):
        for lanes in TILES:
            old = peak[s, :, lanes]
            new = jnp.maximum(old, scores[b, rows : rows + 1, lanes])
            peak[s, :, lanes] = new
            weights = jnp.exp2(scores[b, :rows, lanes] - new).astype(BF16)
            acc[s, :, lanes] = acc[s, :, lanes] * jnp.exp2(old - new) + dot(values[c], weights)

    order = (0, 1, 3, 2)

    def block(c, first=False):
        for i, s in enumerate(order):
            b = i % 2
            if i == 2:
                score(c, order[3], 1)
                weigh(c, s, 0)

                @pl.when(c < BLOCKS - 1)
                def _():
                    arrive(c + 1)
            elif i == 3:
                score(jnp.minimum(c + 1, BLOCKS - 1), order[0], 0)
                weigh(c, s, 1)
            else:
                if first:
                    q_copy(RING - order[i + 1]).wait_recv()
                    if i == 1:
                        q_copy(RING - order[3]).wait_recv()
                score(c, order[i + 1], 1 - b)
                weigh(c, s, b)

    score(0, order[0], 0)
    block(jnp.int32(0), True)

    def body(c, carry):
        block(c)
        return carry

    lax.fori_loop(1, BLOCKS, body, 0)

    def o_copy(step):
        return remote(obuf.at[step], out_ref.at[y], o_send.at[step], o_recv.at[RING - step], at(step))

    for s in (2, 1, 3):
        obuf[s] = (acc[s, :HD] / acc[s, HD : HD + 1]).astype(BF16)
        o_copy(s).start()
    out_ref[y] = (acc[0, :HD] / acc[0, HD : HD + 1]).astype(BF16)

    def o_wait(step):
        return remote(
            obuf.at[step], out_ref.at[lax.rem(y + step, RING)], o_send.at[step], o_recv.at[step], at(step)
        )

    for step in (1, 2, 3):
        q_copy(step).wait_send()
        y_copy(step).wait_send()
        o_copy(step).wait_send()
    for slot in (8, 10, 12, 14):
        z_copy(own, slot).wait_send()
    for slot in (1, 5, 6, 7, 9, 11, 13, 15):
        d_copy(own, slot).wait_send()
    for step in (1, 3, 2):
        o_wait(step).wait_recv()


def attend(query, kv):
    heads, width, rows = query.shape
    dma = lambda n: pltpu.SemaphoreType.DMA((n,))
    vmem = pl.BlockSpec(memory_space=pltpu.VMEM)
    return pl.pallas_call(
        attend_kernel,
        in_specs=[vmem, vmem],
        out_specs=vmem,
        out_shape=jax.ShapeDtypeStruct(query.shape, BF16),
        scratch_shapes=[
            pltpu.VMEM((heads, width, rows), BF16),
            pltpu.VMEM((BLOCKS, 2 * width, rows), BF16),
            pltpu.VMEM((BLOCKS, rows, width), BF16),
            pltpu.VMEM((BLOCKS, width + 16, rows), BF16),
            pltpu.VMEM((heads, width + 16, rows), F32),
            pltpu.VMEM((heads, 1, rows), F32),
            pltpu.VMEM((2, rows + 8, rows), F32),
            pltpu.VMEM((heads, width, rows), BF16),
            dma(RING), dma(RING), dma(RING), dma(BLOCKS), dma(BLOCKS), dma(BLOCKS), dma(RING), dma(RING),
        ],
        cost_estimate=pl.CostEstimate(flops=40 * 10**9, bytes_accessed=8 << 20, transcendentals=0),
        compiler_params=pltpu.CompilerParams(
            vmem_limit_bytes=40 << 20, collective_id=0, has_side_effects=True
        ),
    )(query, kv)


def per_device(n_seq, n_tensor, tokens, norm_gain, w_qkv, w_out, post_gain, w_up, w_down):
    rows, model = tokens.shape
    span = w_qkv.shape[2]
    heads = span // HD
    part = rows // n_tensor
    me = lax.axis_index("tensor")

    w_out_all = lax.all_gather(w_out, "tensor", axis=0, tiled=True)

    base = tokens.astype(F32)
    normed = layer_norm(base, norm_gain).astype(BF16)
    qkv = lax.dot_general(
        w_qkv.reshape(model, -1), normed, (((0,), (1,)), ((), ())), preferred_element_type=F32
    ).reshape(3, heads, HD, rows)
    query = (qkv[0] * (LOG2E / HD**0.5)).astype(BF16)
    kv = jnp.concatenate([qkv[1], qkv[2]], axis=1).astype(BF16)
    attended = attend(query, kv).reshape(span, rows)
    mine = attended.T.reshape(n_tensor, part, span)
    mine = lax.all_to_all(mine, "tensor", 0, 0, tiled=True)
    mine = mine.transpose(1, 0, 2).reshape(part, n_tensor * span)
    own = lax.dynamic_slice_in_dim(tokens, me * part, part, 0).astype(F32)
    mixed = own + dot(mine, w_out_all)
    post = layer_norm(mixed, post_gain).astype(BF16)
    post = lax.all_gather(post, "tensor", axis=0, tiled=True)
    hidden = jax.nn.gelu(dot(post, w_up), approximate=True).astype(BF16)
    term = dot(hidden, w_down).astype(BF16)
    terms = lax.all_to_all(term.reshape(n_tensor, part, model), "tensor", 0, 0, tiled=True)
    out = (mixed + jnp.sum(terms.astype(F32), axis=0)).astype(BF16)
    return lax.all_gather(out, "tensor", axis=0, tiled=True)


def solution(mesh):
    placed = (
        P("seq", None),
        P(),
        P(None, None, "tensor"),
        P("tensor", None),
        P(),
        P(None, "tensor"),
        P("tensor", None),
    )
    body = functools.partial(per_device, mesh.shape["seq"], mesh.shape["tensor"])
    return jax.shard_map(
        body, mesh=mesh, in_specs=placed, out_specs=P("seq", None), check_vma=False
    )
```

```python
import functools
import jax
import jax.numpy as jnp
from jax import lax
from jax.experimental import pallas as pl
from jax.experimental.pallas import tpu as pltpu
from jax.sharding import PartitionSpec as P

HD = 48
LOG2E = 1.4426950408889634
MESH = pl.DeviceIdType.MESH
F32 = jnp.float32
BF16 = jnp.bfloat16
RING = 4
BLOCKS = 16
TILES = (slice(0, 256), slice(256, 512), slice(512, 720))


def layer_norm(values, gain):
    mean = jnp.mean(values, axis=-1, keepdims=True)
    centred = values - mean
    var = jnp.mean(centred * centred, axis=-1, keepdims=True)
    return centred * lax.rsqrt(var + 1e-05) * gain


def dot(a, b):
    return jnp.dot(a, b, preferred_element_type=F32)


def remote(src, dst, send, recv, seq):
    return pltpu.make_async_remote_copy(
        src_ref=src, dst_ref=dst, send_sem=send, recv_sem=recv, device_id={"seq": seq}, device_id_type=MESH
    )


def attend_kernel(
    q_ref, kv_ref, w_ref, out_ref, w_all, q_in, kv_in, key_rows, values, acc, peak, scores, obuf,
    q_send, q_recv, y_send, z_send, d_send, kv_recv, o_send, o_recv, w_send, w_recv, t_send, t_recv, w_own,
):
    rows = q_ref.shape[2]
    me = lax.axis_index("seq")
    half, y, core = me // (2 * RING), (me // 2) % RING, me % 2

    def at(step):
        return half * (2 * RING) + lax.rem(y + step, RING) * 2 + core

    twin = me - core + (1 - core)
    far = lax.rem(me + 2 * RING, BLOCKS)
    peers = [at(1), at(2), at(3), twin, far]
    tensor = lax.axis_index("tensor")
    plane, x = tensor // RING, lax.rem(tensor, RING)

    def on(side, step):
        return side * RING + lax.rem(x + step, RING)

    friends = [on(plane, 1), on(plane, 2), on(plane, 3), on(1 - plane, 0)]
    barrier = pltpu.get_barrier_semaphore()
    for peer in peers:
        pl.semaphore_signal(barrier, inc=1, device_id={"seq": peer}, device_id_type=MESH)
    for friend in friends:
        pl.semaphore_signal(barrier, inc=1, device_id={"tensor": friend}, device_id_type=MESH)
    pl.semaphore_wait(barrier, len(peers) + len(friends))

    cut = w_ref.shape[0] // 2
    rows_of = lambda which: pl.ds(pl.multiple_of(which * cut, cut), cut)

    def w_copy(src, owner, index, friend):
        return pltpu.make_async_remote_copy(
            src_ref=src, dst_ref=w_all.at[owner, rows_of(core)], send_sem=w_send.at[index], recv_sem=w_recv.at[index],
            device_id={"tensor": friend}, device_id_type=MESH,
        )

    def w_of(side, step, index, friend):
        owner = on(side, step)
        return w_copy(w_all.at[owner, rows_of(core)], owner, index, friend)

    def t_copy(index, which):
        owner = on(plane, index + 1) if index < 3 else on(1 - plane, index - 3)
        return remote(
            w_all.at[owner, rows_of(which)], w_all.at[owner, rows_of(which)], t_send.at[index], t_recv.at[index], twin
        )

    w_mine = w_ref.at[rows_of(core)]
    w_local = pltpu.make_async_copy(w_ref, w_all.at[tensor], w_own.at[0])

    def arrived(index):
        w_copy(w_mine, tensor, index, tensor).wait_recv()
        t_copy(index, core).start()

    def pass_on(c):
        @pl.when(c == 6)
        def _():
            arrived(3)
            for step in (1, 3, 2):
                w_copy(w_all.at[on(1 - plane, 0), rows_of(core)], on(1 - plane, 0), 3 + RING - step, on(plane, step)).start()

        @pl.when(c == 10)
        def _():
            for index in (0, 2, 1):
                arrived(index)

        @pl.when(c == BLOCKS - 1)
        def _():
            for index in (4, 6, 5):
                arrived(index)

    def q_copy(step):
        return remote(
            q_ref.at[lax.rem(y + step, RING)], q_in.at[RING - step], q_send.at[step], q_recv.at[RING - step], at(step)
        )

    def y_copy(step):
        slot = {1: 3, 2: 4, 3: 2}[step]
        return remote(
            kv_ref.at[lax.rem(y + step, RING)], kv_in.at[slot], y_send.at[step], kv_recv.at[slot], at(step)
        )

    def z_copy(src, slot):
        return remote(src, kv_in.at[slot], z_send.at[slot], kv_recv.at[slot], far)

    def d_copy(src, slot):
        return remote(src, kv_in.at[slot], d_send.at[slot], kv_recv.at[slot], twin)

    own = kv_ref.at[y]
    for step in (1, 3, 2):
        q_copy(step).start()
    d_copy(own, 1).start()
    for step in (1, 3, 2):
        y_copy(step).start()
    z_copy(own, 8).start()
    w_local.start()
    w_copy(w_mine, tensor, 3, on(1 - plane, 0)).start()
    for step in (1, 3, 2):
        w_copy(w_mine, tensor, RING - step - 1, on(plane, step)).start()

    values[:, HD:, :] = jnp.ones((BLOCKS, values.shape[1] - HD, rows), BF16)
    acc[...] = jnp.zeros_like(acc)
    peak[...] = jnp.full_like(peak, -1e30)
    q_in[0] = q_ref[y]
    obuf[:, :, rows:] = jnp.zeros((RING, HD, obuf.shape[2] - rows), BF16)
    key_rows[0] = kv_ref[y, :HD].T
    values[0, :HD] = kv_ref[y, HD:]

    def arrive(c):
        d_copy(kv_in.at[c], c).wait_recv()

        @pl.when((c >= 2) & (c <= 4))
        def _():
            d_copy(kv_in.at[c], c + 3).start()
            z_copy(kv_in.at[c], 2 * c + 6).start()

        @pl.when((c >= 8) & (lax.rem(c, 2) == 0))
        def _():
            d_copy(kv_in.at[c], c + 1).start()

        pass_on(c)

    def score(c, s, b):
        for lanes in TILES:
            found = dot(key_rows[c], q_in[s, :, lanes])
            scores[b, :rows, lanes] = found
            scores[b, rows : rows + 1, lanes] = jnp.max(found, axis=0, keepdims=True)

    def weigh(c, s, b):
        for lanes in TILES:
            old = peak[s, :, lanes]
            new = jnp.maximum(old, scores[b, rows : rows + 1, lanes])
            peak[s, :, lanes] = new
            weights = jnp.exp2(scores[b, :rows, lanes] - new).astype(BF16)
            acc[s, :, lanes] = acc[s, :, lanes] * jnp.exp2(old - new) + dot(values[c], weights)

    order = (0, 1, 3, 2)

    def block(c, first=False):
        after = jnp.minimum(c + 1, BLOCKS - 1)
        if first:
            arrive(after)
        else:
            @pl.when(c < BLOCKS - 1)
            def _():
                arrive(after)

        key_rows[after] = kv_in[after, :HD].T
        values[after, :HD] = kv_in[after, HD:]
        for i, s in enumerate(order):
            if first and i < 3:
                q_copy(RING - order[i + 1]).wait_recv()
            if i < 3:
                score(c, order[i + 1], 1 - i % 2)
            else:
                score(after, order[0], 0)
            weigh(c, s, i % 2)

    score(0, order[0], 0)
    block(jnp.int32(0), True)

    def body(c, carry):
        block(c)
        return carry

    lax.fori_loop(1, BLOCKS, body, 0)

    def o_copy(step):
        return remote(obuf.at[step], out_ref.at[y], o_send.at[step], o_recv.at[RING - step], at(step))

    for s in (2, 1, 3):
        obuf[s, :, :rows] = (acc[s, :HD] / acc[s, HD : HD + 1]).astype(BF16)
        o_copy(s).start()
    out_ref[y, :, :rows] = (acc[0, :HD] / acc[0, HD : HD + 1]).astype(BF16)
    out_ref[y, :, rows:] = jnp.zeros((HD, out_ref.shape[2] - rows), BF16)

    def o_wait(step):
        return remote(
            obuf.at[step], out_ref.at[lax.rem(y + step, RING)], o_send.at[step], o_recv.at[step], at(step)
        )

    for step in (1, 2, 3):
        q_copy(step).wait_send()
        y_copy(step).wait_send()
        o_copy(step).wait_send()
    for slot in (8, 10, 12, 14):
        z_copy(own, slot).wait_send()
    for slot in (1, 5, 6, 7, 9, 11, 13, 15):
        d_copy(own, slot).wait_send()
    for index in range(7):
        w_copy(w_mine, tensor, index, tensor).wait_send()
        t_copy(index, core).wait_send()
        t_copy(index, 1 - core).wait_recv()
    w_local.wait()
    for step in (1, 3, 2):
        o_wait(step).wait_recv()


def attend(query, kv, w_out, padded, n_tensor):
    heads, width, rows = query.shape
    dma = lambda n: pltpu.SemaphoreType.DMA((n,))
    vmem = pl.BlockSpec(memory_space=pltpu.VMEM)
    return pl.pallas_call(
        attend_kernel,
        in_specs=[vmem, vmem, vmem],
        out_specs=[vmem, pl.BlockSpec(memory_space=pl.ANY)],
        out_shape=[
            jax.ShapeDtypeStruct((heads, width, padded), BF16),
            jax.ShapeDtypeStruct((n_tensor, *w_out.shape), BF16),
        ],
        scratch_shapes=[
            pltpu.VMEM((heads, width, rows), BF16),
            pltpu.VMEM((BLOCKS, 2 * width, rows), BF16),
            pltpu.VMEM((BLOCKS, rows, width), BF16),
            pltpu.VMEM((BLOCKS, width + 16, rows), BF16),
            pltpu.VMEM((heads, width + 16, rows), F32),
            pltpu.VMEM((heads, 1, rows), F32),
            pltpu.VMEM((2, rows + 8, rows), F32),
            pltpu.VMEM((heads, width, padded), BF16),
            dma(RING), dma(RING), dma(RING), dma(BLOCKS), dma(BLOCKS), dma(BLOCKS), dma(RING), dma(RING),
            dma(7), dma(7), dma(7), dma(7), dma(1),
        ],
        cost_estimate=pl.CostEstimate(flops=40 * 10**9, bytes_accessed=8 << 20, transcendentals=0),
        compiler_params=pltpu.CompilerParams(
            vmem_limit_bytes=40 << 20, collective_id=0, has_side_effects=True
        ),
    )(query, kv, w_out)


class Tensor:
    def __init__(self):
        self.me = lax.axis_index("tensor")
        self.plane, self.x = self.me // RING, lax.rem(self.me, RING)
        self.right, self.left = self.on(self.plane, 1), self.on(self.plane, 3)
        self.pair = self.on(1 - self.plane, 0)

    def on(self, side, step):
        return side * RING + lax.rem(self.x + step, RING)

    def meet(self):
        barrier = pltpu.get_barrier_semaphore()
        for friend in (self.right, self.left, self.pair):
            pl.semaphore_signal(barrier, inc=1, device_id={"tensor": friend}, device_id_type=MESH)
        pl.semaphore_wait(barrier, 3)


def send(src, dst, send_sem, recv_sem, friend):
    return pltpu.make_async_remote_copy(
        src_ref=src, dst_ref=dst, send_sem=send_sem, recv_sem=recv_sem,
        device_id={"tensor": friend}, device_id_type=MESH,
    )


def gather(t, mine, buf, cut, send_sem, recv_sem):
    lo, hi = pl.ds(0, cut), pl.ds(cut, cut)
    copies = {
        "right": (mine, t.me, None, t.right, 0),
        "left": (mine, t.me, None, t.left, 1),
        "pair": (mine, t.me, None, t.pair, 2),
        "far lo": (None, t.left, lo, t.right, 3),
        "far hi": (None, t.right, hi, t.left, 4),
        "over right": (None, t.pair, None, t.right, 5),
        "over left": (None, t.pair, None, t.left, 6),
        "pair lo": (None, t.on(t.plane, 2), lo, t.pair, 7),
        "pair hi": (None, t.on(t.plane, 2), hi, t.pair, 8),
    }

    def copy(name):
        src, block, part, to, i = copies[name]
        dst = buf.at[block] if part is None else buf.at[block, part]
        return send(dst if src is None else src, dst, send_sem.at[i], recv_sem.at[i], to)

    for name in ("right", "left", "pair"):
        copy(name).start()
    copy("right").wait_recv()
    copy("far lo").start()
    copy("left").wait_recv()
    copy("far hi").start()
    copy("pair").wait_recv()
    copy("over right").start()
    copy("over left").start()
    copy("far lo").wait_recv()
    copy("pair lo").start()
    copy("far hi").wait_recv()
    copy("pair hi").start()
    for name in ("over right", "over left", "pair lo", "pair hi"):
        copy(name).wait_recv()
    for name in copies:
        copy(name).wait_send()


def gather_kernel(x_ref, out_ref, send_sem, recv_sem):
    t = Tensor()
    t.meet()
    out_ref[t.me] = x_ref[...]
    gather(t, x_ref, out_ref, x_ref.shape[0] // 2, send_sem, recv_sem)


def gather_heads(x, n_tensor):
    dma = lambda n: pltpu.SemaphoreType.DMA((n,))
    return pl.pallas_call(
        gather_kernel,
        in_specs=[pl.BlockSpec(memory_space=pltpu.VMEM)],
        out_specs=pl.BlockSpec(memory_space=pltpu.VMEM),
        out_shape=jax.ShapeDtypeStruct((n_tensor, *x.shape), x.dtype),
        scratch_shapes=[dma(9), dma(9)],
        cost_estimate=pl.CostEstimate(flops=20 * 10**9, bytes_accessed=8 << 20, transcendentals=0),
        compiler_params=pltpu.CompilerParams(vmem_limit_bytes=16 << 20, collective_id=1, has_side_effects=True),
    )(x)


def finish_kernel(
    term_ref, mixed_ref, out_ref, own, far_in, over_in, half_in, edge_in, pair_in, far_sum, over_sum, edge_sum,
    s_send, s_recv, g_send, g_recv,
):
    t = Tensor()
    part = mixed_ref.shape[0]
    cut = part // 2
    lo, hi = pl.ds(0, cut), pl.ds(cut, cut)
    there = 1 - t.plane
    t.meet()
    copies = {}

    def go(name, src, dst, to):
        i = len(copies)
        copies[name] = send(src, dst, s_send.at[i], s_recv.at[i], to)
        copies[name].start()

    wait = lambda name: copies[name].wait_recv()
    far, far_over = t.on(t.plane, 2), t.on(there, 2)
    go("far", term_ref.at[far_over], far_in, t.pair)
    go("over right", term_ref.at[t.on(there, 1)], over_in.at[0], t.right)
    go("over left", term_ref.at[t.on(there, 3)], over_in.at[1], t.left)
    go("edge right", term_ref.at[t.right, lo], edge_in.at[0, lo], t.right)
    go("edge left", term_ref.at[t.left, hi], edge_in.at[1, hi], t.left)
    wait("far")
    far_sum[...] = (far_in[...].astype(F32) + term_ref[far].astype(F32)).astype(BF16)
    go("half left", far_sum.at[lo], half_in.at[0], t.left)
    go("half right", far_sum.at[hi], half_in.at[1], t.right)
    wait("over right")
    wait("over left")
    over_sum[...] = (
        over_in[0].astype(F32) + over_in[1].astype(F32) + term_ref[t.pair].astype(F32)
    ).astype(BF16)
    go("pair", over_sum, pair_in, t.pair)
    wait("half left")
    edge_sum[0] = (half_in[0].astype(F32) + term_ref[t.left, lo].astype(F32)).astype(BF16)
    go("sum left", edge_sum.at[0], edge_in.at[1, lo], t.left)
    wait("half right")
    edge_sum[1] = (half_in[1].astype(F32) + term_ref[t.right, hi].astype(F32)).astype(BF16)
    go("sum right", edge_sum.at[1], edge_in.at[0, hi], t.right)
    for name in ("edge right", "edge left", "sum left", "sum right", "pair"):
        wait(name)
    own[...] = (
        mixed_ref[...]
        + term_ref[t.me].astype(F32)
        + edge_in[0].astype(F32)
        + edge_in[1].astype(F32)
        + pair_in[...].astype(F32)
    ).astype(BF16)
    out_ref[t.me] = own[...]
    for name in copies:
        copies[name].wait_send()
    gather(t, own, out_ref, cut, g_send, g_recv)


def finish(term, mixed):
    n_tensor, part, model = term.shape
    dma = lambda n: pltpu.SemaphoreType.DMA((n,))
    vmem = pl.BlockSpec(memory_space=pltpu.VMEM)
    block = lambda *lead: pltpu.VMEM((*lead, part, model), BF16)
    half = pltpu.VMEM((2, part // 2, model), BF16)
    return pl.pallas_call(
        finish_kernel,
        in_specs=[vmem, vmem],
        out_specs=vmem,
        out_shape=jax.ShapeDtypeStruct(term.shape, BF16),
        scratch_shapes=[
            block(), block(), block(2), half, block(2), block(), block(), block(), half,
            dma(10), dma(10), dma(9), dma(9),
        ],
        cost_estimate=pl.CostEstimate(flops=40 * 10**9, bytes_accessed=8 << 20, transcendentals=0),
        compiler_params=pltpu.CompilerParams(vmem_limit_bytes=32 << 20, collective_id=2, has_side_effects=True),
    )(term, mixed)


def per_device(n_seq, n_tensor, tokens, norm_gain, w_qkv, w_out, post_gain, w_up, w_down):
    rows, model = tokens.shape
    span = w_qkv.shape[2]
    heads = span // HD
    part = -(-rows // (16 * n_tensor)) * 16
    padded = n_tensor * part
    me = lax.axis_index("tensor")

    base = tokens.astype(F32)
    normed = layer_norm(base, norm_gain).astype(BF16)
    qkv = lax.dot_general(
        w_qkv.reshape(model, -1), normed, (((0,), (1,)), ((), ())), preferred_element_type=F32
    ).reshape(3, heads, HD, rows)
    query = (qkv[0] * (LOG2E / HD**0.5)).astype(BF16)
    kv = jnp.concatenate([qkv[1], qkv[2]], axis=1).astype(BF16)
    attended, w_out_all = attend(query, kv, w_out, padded, n_tensor)
    attended = gather_heads(attended.reshape(span, padded), n_tensor).reshape(n_tensor * span, padded)
    mixed = jnp.pad(base, ((0, padded - rows), (0, 0))) + lax.dot_general(
        attended, w_out_all.reshape(n_tensor * span, model), (((0,), (0,)), ((), ())), preferred_element_type=F32
    )
    post = layer_norm(mixed, post_gain).astype(BF16)
    hidden = jax.nn.gelu(dot(post, w_up), approximate=True).astype(BF16)
    term = dot(hidden, w_down).astype(BF16).reshape(n_tensor, part, model)
    own = lax.dynamic_slice_in_dim(mixed, me * part, part, 0)
    return finish(term, own).reshape(padded, model)[:rows]


def solution(mesh):
    placed = (
        P("seq", None),
        P(),
        P(None, None, "tensor"),
        P("tensor", None),
        P(),
        P(None, "tensor"),
        P("tensor", None),
    )
    body = functools.partial(per_device, mesh.shape["seq"], mesh.shape["tensor"])
    return jax.shard_map(
        body, mesh=mesh, in_specs=placed, out_specs=P("seq", None), check_vma=False
    )
```

```python
import functools
import jax
import jax.numpy as jnp
from jax import lax
from jax.experimental import pallas as pl
from jax.experimental.pallas import tpu as pltpu
from jax.sharding import PartitionSpec as P

HD = 48
LOG2E = 1.4426950408889634
MESH = pl.DeviceIdType.MESH
F32 = jnp.float32
BF16 = jnp.bfloat16
RING = 4
BLOCKS = 16
TILES = (slice(0, 256), slice(256, 512), slice(512, 720))


def layer_norm(values, gain):
    mean = jnp.mean(values, axis=-1, keepdims=True)
    centred = values - mean
    var = jnp.mean(centred * centred, axis=-1, keepdims=True)
    return centred * lax.rsqrt(var + 1e-05) * gain


def dot(a, b):
    return jnp.dot(a, b, preferred_element_type=F32)


def remote(src, dst, send, recv, seq):
    return pltpu.make_async_remote_copy(
        src_ref=src, dst_ref=dst, send_sem=send, recv_sem=recv, device_id={"seq": seq}, device_id_type=MESH
    )


def attend_kernel(
    q_ref, kv_ref, w_hbm, up_ref, down_ref, out_ref, w_all, up_all, down_all, w_ref, q_in, kv_in, key_rows, values, acc, peak, scores, obuf,
    q_send, q_recv, y_send, z_send, d_send, kv_recv, o_send, o_recv, w_send, w_recv, t_send, t_recv, w_own,
    f_send, f_recv, g_send, g_recv, h_send, h_recv,
):
    rows = q_ref.shape[2]
    me = lax.axis_index("seq")
    half, y, core = me // (2 * RING), (me // 2) % RING, me % 2

    def at(step):
        return half * (2 * RING) + lax.rem(y + step, RING) * 2 + core

    twin = me - core + (1 - core)
    far = lax.rem(me + 2 * RING, BLOCKS)
    peers = [at(1), at(2), at(3), twin, far]
    tensor = lax.axis_index("tensor")
    plane, x = tensor // RING, lax.rem(tensor, RING)

    def on(side, step):
        return side * RING + lax.rem(x + step, RING)

    friends = [on(plane, 1), on(plane, 2), on(plane, 3), on(1 - plane, 0)]
    barrier = pltpu.get_barrier_semaphore()
    for peer in peers:
        pl.semaphore_signal(barrier, inc=1, device_id={"seq": peer}, device_id_type=MESH)
    for friend in friends:
        pl.semaphore_signal(barrier, inc=1, device_id={"tensor": friend}, device_id_type=MESH)
    across = on(1 - plane, 0)
    pl.semaphore_signal(barrier, inc=1, device_id={"seq": far, "tensor": across}, device_id_type=MESH)
    w_load = pltpu.make_async_copy(w_hbm, w_ref, w_own.at[0])
    w_load.start()
    values[:, HD:, :] = jnp.ones((BLOCKS, values.shape[1] - HD, rows), BF16)
    acc[...] = jnp.zeros_like(acc)
    peak[...] = jnp.full_like(peak, -1e30)
    q_in[0] = q_ref[y]
    obuf[:, :, rows:] = jnp.zeros((RING, HD, obuf.shape[2] - rows), BF16)
    key_rows[0] = kv_ref[y, :HD].T
    values[0, :HD] = kv_ref[y, HD:]
    pl.semaphore_wait(barrier, len(peers) + len(friends) + 1)

    pieces = 2 * RING
    both = ((up_ref, up_all), (down_ref, down_all))

    def piece(j, which):
        return lax.rem(y + (0, 2, 1, 3)[j], RING) * 2 + which

    def f_copy(k, j):
        ref, whole = both[k]
        size = ref.shape[0] // pieces
        number = piece(j, core)
        src = ref.at[pl.ds(pl.multiple_of(number * size, size), size)]
        device = {"tensor": across} if k == 0 else {"seq": far, "tensor": across}
        return pltpu.make_async_remote_copy(
            src_ref=src, dst_ref=whole.at[number], send_sem=f_send.at[2 * k + j], recv_sem=f_recv.at[2 * k + j],
            device_id=device, device_id_type=MESH,
        )

    def g_copy(k, step):
        whole = both[k][1]
        number = piece(0, core)
        i = 2 * k + step // 2
        j = 2 * k + 1 - step // 2
        return remote(whole.at[number], whole.at[number], g_send.at[i], g_recv.at[j], at(step))

    def h_copy(k, j, which):
        whole = both[k][1]
        number = piece(j, which)
        i = 4 * k + j
        return remote(whole.at[number], whole.at[number], h_send.at[i], h_recv.at[i], twin)

    cut = w_ref.shape[0] // 2
    rows_of = lambda which: pl.ds(pl.multiple_of(which * cut, cut), cut)

    def w_copy(src, owner, index, friend):
        return pltpu.make_async_remote_copy(
            src_ref=src, dst_ref=w_all.at[owner, rows_of(core)], send_sem=w_send.at[index], recv_sem=w_recv.at[index],
            device_id={"tensor": friend}, device_id_type=MESH,
        )

    def w_of(side, step, index, friend):
        owner = on(side, step)
        return w_copy(w_all.at[owner, rows_of(core)], owner, index, friend)

    def t_copy(index, which):
        owner = on(plane, index + 1) if index < 3 else on(1 - plane, index - 3)
        return remote(
            w_all.at[owner, rows_of(which)], w_all.at[owner, rows_of(which)], t_send.at[index], t_recv.at[index], twin
        )

    w_mine = w_ref.at[rows_of(core)]
    w_local = pltpu.make_async_copy(w_ref, w_all.at[tensor], w_own.at[1])

    def arrived(index):
        w_copy(w_mine, tensor, index, tensor).wait_recv()
        t_copy(index, core).start()

    def pass_on(c):
        @pl.when(c == 5)
        def _():
            for k in range(2):
                f_copy(k, 1).start()
                f_copy(k, 0).wait_recv()
                for step in (1, 3):
                    g_copy(k, step).start()
                h_copy(k, 0, core).start()

        @pl.when(c == 13)
        def _():
            for k in range(2):
                for step in (1, 3):
                    g_copy(k, step).wait_recv()
                for j in (2, 3):
                    h_copy(k, j, core).start()

        @pl.when(c == BLOCKS - 1)
        def _():
            for k in range(2):
                f_copy(k, 1).wait_recv()
                h_copy(k, 1, core).start()

        @pl.when(c == 6)
        def _():
            arrived(3)
            for step in (1, 3, 2):
                w_copy(w_all.at[on(1 - plane, 0), rows_of(core)], on(1 - plane, 0), 3 + RING - step, on(plane, step)).start()

        @pl.when(c == 10)
        def _():
            for index in (0, 2, 1):
                arrived(index)

        @pl.when(c == BLOCKS - 1)
        def _():
            for index in (4, 6, 5):
                arrived(index)

    def q_copy(step):
        return remote(
            q_ref.at[lax.rem(y + step, RING)], q_in.at[RING - step], q_send.at[step], q_recv.at[RING - step], at(step)
        )

    def y_copy(step):
        slot = {1: 3, 2: 4, 3: 2}[step]
        return remote(
            kv_ref.at[lax.rem(y + step, RING)], kv_in.at[slot], y_send.at[step], kv_recv.at[slot], at(step)
        )

    def z_copy(src, slot):
        return remote(src, kv_in.at[slot], z_send.at[slot], kv_recv.at[slot], far)

    def d_copy(src, slot):
        return remote(src, kv_in.at[slot], d_send.at[slot], kv_recv.at[slot], twin)

    own = kv_ref.at[y]
    for step in (1, 3, 2):
        q_copy(step).start()
    d_copy(own, 1).start()
    for step in (1, 3, 2):
        y_copy(step).start()
    z_copy(own, 8).start()
    f_copy(0, 0).start()
    f_copy(1, 0).start()
    w_load.wait()
    w_local.start()
    w_copy(w_mine, tensor, 3, across).start()
    for step in (1, 3, 2):
        w_copy(w_mine, tensor, RING - step - 1, on(plane, step)).start()

    def arrive(c):
        d_copy(kv_in.at[c], c).wait_recv()

        @pl.when((c >= 2) & (c <= 4))
        def _():
            d_copy(kv_in.at[c], c + 3).start()
            z_copy(kv_in.at[c], 2 * c + 6).start()

        @pl.when((c >= 8) & (lax.rem(c, 2) == 0))
        def _():
            d_copy(kv_in.at[c], c + 1).start()

        pass_on(c)

    def score(c, s, b):
        for lanes in TILES:
            found = dot(key_rows[c], q_in[s, :, lanes])
            scores[b, :rows, lanes] = found
            scores[b, rows : rows + 1, lanes] = jnp.max(found, axis=0, keepdims=True)

    def weigh(c, s, b):
        for lanes in TILES:
            old = peak[s, :, lanes]
            new = jnp.maximum(old, scores[b, rows : rows + 1, lanes])
            peak[s, :, lanes] = new
            weights = jnp.exp2(scores[b, :rows, lanes] - new).astype(BF16)
            acc[s, :, lanes] = acc[s, :, lanes] * jnp.exp2(old - new) + dot(values[c], weights)

    order = (0, 1, 3, 2)

    def block(c, first=False):
        after = jnp.minimum(c + 1, BLOCKS - 1)
        if first:
            arrive(after)
        else:
            @pl.when(c < BLOCKS - 1)
            def _():
                arrive(after)

        key_rows[after] = kv_in[after, :HD].T
        values[after, :HD] = kv_in[after, HD:]
        for i, s in enumerate(order):
            if first and i < 3:
                q_copy(RING - order[i + 1]).wait_recv()
            if i < 3:
                score(c, order[i + 1], 1 - i % 2)
            else:
                score(after, order[0], 0)
            weigh(c, s, i % 2)

    score(0, order[0], 0)
    block(jnp.int32(0), True)

    def body(c, carry):
        block(c)
        return carry

    lax.fori_loop(1, BLOCKS, body, 0)

    def o_copy(step):
        return remote(obuf.at[step], out_ref.at[y], o_send.at[step], o_recv.at[RING - step], at(step))

    for s in (2, 1, 3):
        obuf[s, :, :rows] = (acc[s, :HD] / acc[s, HD : HD + 1]).astype(BF16)
        o_copy(s).start()
    out_ref[y, :, :rows] = (acc[0, :HD] / acc[0, HD : HD + 1]).astype(BF16)
    out_ref[y, :, rows:] = jnp.zeros((HD, out_ref.shape[2] - rows), BF16)

    def o_wait(step):
        return remote(
            obuf.at[step], out_ref.at[lax.rem(y + step, RING)], o_send.at[step], o_recv.at[step], at(step)
        )

    for step in (1, 2, 3):
        q_copy(step).wait_send()
        y_copy(step).wait_send()
        o_copy(step).wait_send()
    for slot in (8, 10, 12, 14):
        z_copy(own, slot).wait_send()
    for slot in (1, 5, 6, 7, 9, 11, 13, 15):
        d_copy(own, slot).wait_send()
    for index in range(7):
        w_copy(w_mine, tensor, index, tensor).wait_send()
        t_copy(index, core).wait_send()
        t_copy(index, 1 - core).wait_recv()
    w_local.wait()
    for k in range(2):
        for j in range(2):
            f_copy(k, j).wait_send()
        for step in (1, 3):
            g_copy(k, step).wait_send()
        for j in range(4):
            h_copy(k, j, core).wait_send()
            h_copy(k, j, 1 - core).wait_recv()
    for step in (1, 3, 2):
        o_wait(step).wait_recv()


def attend(query, kv, w_out, w_up, w_down, padded, n_tensor):
    heads, width, rows = query.shape
    dma = lambda n: pltpu.SemaphoreType.DMA((n,))
    vmem = pl.BlockSpec(memory_space=pltpu.VMEM)
    hbm = pl.BlockSpec(memory_space=pl.ANY)
    return pl.pallas_call(
        attend_kernel,
        in_specs=[vmem, vmem, hbm, hbm, hbm],
        out_specs=[vmem, hbm, hbm, hbm],
        out_shape=[
            jax.ShapeDtypeStruct((heads, width, padded), BF16),
            jax.ShapeDtypeStruct((n_tensor, *w_out.shape), BF16),
            *(jax.ShapeDtypeStruct((2 * RING, w.shape[0] // (2 * RING), w.shape[1]), BF16) for w in (w_up, w_down)),
        ],
        scratch_shapes=[
            pltpu.VMEM(w_out.shape, BF16),
            pltpu.VMEM((heads, width, rows), BF16),
            pltpu.VMEM((BLOCKS, 2 * width, rows), BF16),
            pltpu.VMEM((BLOCKS, rows, width), BF16),
            pltpu.VMEM((BLOCKS, width + 16, rows), BF16),
            pltpu.VMEM((heads, width + 16, rows), F32),
            pltpu.VMEM((heads, 1, rows), F32),
            pltpu.VMEM((2, rows + 8, rows), F32),
            pltpu.VMEM((heads, width, padded), BF16),
            dma(RING), dma(RING), dma(RING), dma(BLOCKS), dma(BLOCKS), dma(BLOCKS), dma(RING), dma(RING),
            dma(7), dma(7), dma(7), dma(7), dma(2),
            dma(4), dma(4), dma(4), dma(4), dma(8), dma(8),
        ],
        cost_estimate=pl.CostEstimate(flops=40 * 10**9, bytes_accessed=8 << 20, transcendentals=0),
        compiler_params=pltpu.CompilerParams(
            vmem_limit_bytes=40 << 20, collective_id=0, has_side_effects=True
        ),
    )(query, kv, w_out, w_up, w_down)


class Tensor:
    def __init__(self):
        self.me = lax.axis_index("tensor")
        self.plane, self.x = self.me // RING, lax.rem(self.me, RING)
        self.right, self.left = self.on(self.plane, 1), self.on(self.plane, 3)
        self.pair = self.on(1 - self.plane, 0)

    def on(self, side, step):
        return side * RING + lax.rem(self.x + step, RING)

    def meet(self):
        barrier = pltpu.get_barrier_semaphore()
        for friend in (self.right, self.left, self.pair):
            pl.semaphore_signal(barrier, inc=1, device_id={"tensor": friend}, device_id_type=MESH)
        pl.semaphore_wait(barrier, 3)


def send(src, dst, send_sem, recv_sem, friend):
    return pltpu.make_async_remote_copy(
        src_ref=src, dst_ref=dst, send_sem=send_sem, recv_sem=recv_sem,
        device_id={"tensor": friend}, device_id_type=MESH,
    )


def gather(t, mine, buf, cut, send_sem, recv_sem):
    lo, hi = pl.ds(0, cut), pl.ds(cut, cut)
    copies = {
        "right": (mine, t.me, None, t.right, 0),
        "left": (mine, t.me, None, t.left, 1),
        "pair": (mine, t.me, None, t.pair, 2),
        "far lo": (None, t.left, lo, t.right, 3),
        "far hi": (None, t.right, hi, t.left, 4),
        "over right": (None, t.pair, None, t.right, 5),
        "over left": (None, t.pair, None, t.left, 6),
        "pair lo": (None, t.on(t.plane, 2), lo, t.pair, 7),
        "pair hi": (None, t.on(t.plane, 2), hi, t.pair, 8),
    }

    def copy(name):
        src, block, part, to, i = copies[name]
        dst = buf.at[block] if part is None else buf.at[block, part]
        return send(dst if src is None else src, dst, send_sem.at[i], recv_sem.at[i], to)

    for name in ("right", "left", "pair"):
        copy(name).start()
    copy("right").wait_recv()
    copy("far lo").start()
    copy("left").wait_recv()
    copy("far hi").start()
    copy("pair").wait_recv()
    copy("over right").start()
    copy("over left").start()
    copy("far lo").wait_recv()
    copy("pair lo").start()
    copy("far hi").wait_recv()
    copy("pair hi").start()
    for name in ("over right", "over left", "pair lo", "pair hi"):
        copy(name).wait_recv()
    for name in copies:
        copy(name).wait_send()


def heads_kernel(x_ref, out_ref, send_sem, recv_sem):
    t = Tensor()
    width = x_ref.shape[1] // 2
    cut = x_ref.shape[0] // 2
    lo, hi = pl.ds(0, cut), pl.ds(cut, cut)
    part = lambda plane: x_ref.at[:, pl.ds(pl.multiple_of(plane * width, width), width)]
    there = 1 - t.plane
    t.meet()

    def copy(src, block, rows, to, i):
        dst = out_ref.at[block] if rows is None else out_ref.at[block, rows]
        return send(dst if src is None else src, dst, send_sem.at[i], recv_sem.at[i], to)

    copies = [
        copy(part(t.plane), t.me, None, t.right, 0),
        copy(part(t.plane), t.me, None, t.left, 1),
        copy(part(there), t.me, None, t.pair, 2),
        copy(None, t.left, lo, t.right, 3),
        copy(None, t.right, hi, t.left, 4),
        copy(None, t.pair, None, t.right, 5),
        copy(None, t.pair, None, t.left, 6),
        copy(None, t.on(there, 3), lo, t.right, 7),
        copy(None, t.on(there, 1), hi, t.left, 8),
    ]
    for i in (2, 0, 1):
        copies[i].start()
    out_ref[t.me] = x_ref[:, pl.ds(pl.multiple_of(t.plane * width, width), width)]
    copies[2].wait_recv()
    copies[5].start()
    copies[6].start()
    copies[0].wait_recv()
    copies[3].start()
    copies[1].wait_recv()
    copies[4].start()
    copies[5].wait_recv()
    copies[7].start()
    copies[6].wait_recv()
    copies[8].start()
    for i in (3, 4, 7, 8):
        copies[i].wait_recv()
    for one in copies:
        one.wait_send()


def gather_heads(x, n_tensor):
    dma = lambda n: pltpu.SemaphoreType.DMA((n,))
    vmem = pl.BlockSpec(memory_space=pltpu.VMEM)
    return pl.pallas_call(
        heads_kernel,
        in_specs=[vmem],
        out_specs=vmem,
        out_shape=jax.ShapeDtypeStruct((n_tensor, x.shape[0], x.shape[1] // 2), x.dtype),
        scratch_shapes=[dma(9), dma(9)],
        cost_estimate=pl.CostEstimate(flops=20 * 10**9, bytes_accessed=8 << 20, transcendentals=0),
        compiler_params=pltpu.CompilerParams(vmem_limit_bytes=16 << 20, collective_id=1, has_side_effects=True),
    )(x)


def finish_kernel(
    term_ref, mixed_ref, out_ref, base, own, half_in, edge_in, edge_sum, s_send, s_recv, g_send, g_recv, load_sem
):
    t = Tensor()
    part = own.shape[0]
    cut = part // 2
    lo, hi = pl.ds(0, cut), pl.ds(cut, cut)
    right, left, far = (lax.rem(t.x + step, RING) for step in (1, 3, 2))
    load = pltpu.make_async_copy(mixed_ref.at[t.x], base, load_sem.at[0])
    load.start()
    t.meet()
    copies = {}

    def go(name, src, dst, to):
        i = len(copies)
        copies[name] = send(src, dst, s_send.at[i], s_recv.at[i], to)
        copies[name].start()

    wait = lambda name: copies[name].wait_recv()
    go("half left", term_ref.at[far, lo], half_in.at[0], t.left)
    go("half right", term_ref.at[far, hi], half_in.at[1], t.right)
    go("edge right", term_ref.at[right, lo], edge_in.at[0, lo], t.right)
    go("edge left", term_ref.at[left, hi], edge_in.at[1, hi], t.left)
    load.wait()
    base[...] += term_ref[t.x].astype(F32)
    wait("half left")
    edge_sum[0] = (half_in[0].astype(F32) + term_ref[left, lo].astype(F32)).astype(BF16)
    go("sum left", edge_sum.at[0], edge_in.at[1, lo], t.left)
    wait("half right")
    edge_sum[1] = (half_in[1].astype(F32) + term_ref[right, hi].astype(F32)).astype(BF16)
    go("sum right", edge_sum.at[1], edge_in.at[0, hi], t.right)
    for name in ("edge right", "edge left", "sum left", "sum right"):
        wait(name)
    own[...] = (base[...] + edge_in[0].astype(F32) + edge_in[1].astype(F32)).astype(BF16)
    out_ref[t.me] = own[...]
    for name in copies:
        copies[name].wait_send()
    gather(t, own, out_ref, cut, g_send, g_recv)


def finish(term, mixed, n_tensor):
    ring, part, model = term.shape
    dma = lambda n: pltpu.SemaphoreType.DMA((n,))
    vmem = pl.BlockSpec(memory_space=pltpu.VMEM)
    half = pltpu.VMEM((2, part // 2, model), BF16)
    return pl.pallas_call(
        finish_kernel,
        in_specs=[vmem, pl.BlockSpec(memory_space=pl.ANY)],
        out_specs=vmem,
        out_shape=jax.ShapeDtypeStruct((n_tensor, part, model), BF16),
        scratch_shapes=[
            pltpu.VMEM((part, model), F32), pltpu.VMEM((part, model), BF16),
            half, pltpu.VMEM((2, part, model), BF16), half,
            dma(6), dma(6), dma(9), dma(9), dma(1),
        ],
        cost_estimate=pl.CostEstimate(flops=40 * 10**9, bytes_accessed=8 << 20, transcendentals=0),
        compiler_params=pltpu.CompilerParams(vmem_limit_bytes=32 << 20, collective_id=2, has_side_effects=True),
    )(term, mixed)


def per_device(n_seq, n_tensor, tokens, norm_gain, w_qkv, w_out, post_gain, w_up, w_down):
    rows, model = tokens.shape
    span = w_qkv.shape[2]
    heads = span // HD
    part = -(-rows // (16 * n_tensor)) * 16
    padded = n_tensor * part
    me = lax.axis_index("tensor")

    base = tokens.astype(F32)
    normed = layer_norm(base, norm_gain).astype(BF16)
    qkv = lax.dot_general(
        w_qkv.reshape(model, -1), normed, (((0,), (1,)), ((), ())), preferred_element_type=F32
    ).reshape(3, heads, HD, rows)
    query = (qkv[0] * (LOG2E / HD**0.5)).astype(BF16)
    kv = jnp.concatenate([qkv[1], qkv[2]], axis=1).astype(BF16)
    attended, w_out_all, up_pair, down_pair = attend(query, kv, w_out, w_up, w_down, padded, n_tensor)
    attended = gather_heads(attended.reshape(span, padded), n_tensor).reshape(n_tensor * span, padded // 2)
    plane = me // RING
    base = jnp.pad(tokens, ((0, padded - rows), (0, 0)))
    base = lax.dynamic_slice_in_dim(base, plane * (padded // 2), padded // 2, 0)
    mixed = base.astype(F32) + lax.dot_general(
        attended, w_out_all.reshape(n_tensor * span, model), (((0,), (0,)), ((), ())), preferred_element_type=F32
    )
    post = layer_norm(mixed, post_gain).astype(BF16)
    wide = lambda w: jax.nn.gelu(dot(post, w), approximate=True).astype(BF16)
    term = dot(wide(w_up), w_down) + dot(wide(up_pair.reshape(w_up.shape)), down_pair.reshape(w_down.shape))
    term = term.astype(BF16).reshape(RING, part, model)
    return finish(term, mixed.reshape(RING, part, model), n_tensor).reshape(padded, model)[:rows]


def solution(mesh):
    placed = (
        P("seq", None),
        P(),
        P(None, None, "tensor"),
        P("tensor", None),
        P(),
        P(None, "tensor"),
        P("tensor", None),
    )
    body = functools.partial(per_device, mesh.shape["seq"], mesh.shape["tensor"])
    return jax.shard_map(
        body, mesh=mesh, in_specs=placed, out_specs=P("seq", None), check_vma=False
    )
```

```python
import functools
import jax
import jax.numpy as jnp
from jax import lax
from jax.experimental import pallas as pl
from jax.experimental.pallas import tpu as pltpu
from jax.sharding import PartitionSpec as P

HD = 48
LOG2E = 1.4426950408889634
MESH = pl.DeviceIdType.MESH
F32 = jnp.float32
BF16 = jnp.bfloat16
RING = 4
BLOCKS = 16
TILES = (slice(0, 256), slice(256, 512), slice(512, 720))


def layer_norm(values, gain):
    mean = jnp.mean(values, axis=-1, keepdims=True)
    centred = values - mean
    var = jnp.mean(centred * centred, axis=-1, keepdims=True)
    return centred * lax.rsqrt(var + 1e-05) * gain


def dot(a, b):
    return jnp.dot(a, b, preferred_element_type=F32)


def remote(src, dst, send, recv, seq):
    return pltpu.make_async_remote_copy(
        src_ref=src, dst_ref=dst, send_sem=send, recv_sem=recv, device_id={"seq": seq}, device_id_type=MESH
    )


def attend_kernel(
    q_ref, kv_ref, w_hbm, up_ref, down_ref, out_ref, w_all, up_all, down_all, w_ref, q_in, kv_in, key_rows, values, acc, peak, scores, obuf,
    q_send, q_recv, y_send, z_send, d_send, kv_recv, o_send, o_recv, w_send, w_recv, t_send, t_recv, w_own,
    f_send, f_recv, g_send, g_recv, h_send, h_recv,
):
    rows = q_ref.shape[2]
    me = lax.axis_index("seq")
    half, y, core = me // (2 * RING), (me // 2) % RING, me % 2

    def at(step):
        return half * (2 * RING) + lax.rem(y + step, RING) * 2 + core

    twin = me - core + (1 - core)
    far = lax.rem(me + 2 * RING, BLOCKS)
    peers = [at(1), at(2), at(3), twin, far]
    tensor = lax.axis_index("tensor")
    plane, x = tensor // RING, lax.rem(tensor, RING)

    def on(side, step):
        return side * RING + lax.rem(x + step, RING)

    friends = [on(plane, 1), on(plane, 2), on(plane, 3), on(1 - plane, 0)]
    barrier = pltpu.get_barrier_semaphore()
    for peer in peers:
        pl.semaphore_signal(barrier, inc=1, device_id={"seq": peer}, device_id_type=MESH)
    for friend in friends:
        pl.semaphore_signal(barrier, inc=1, device_id={"tensor": friend}, device_id_type=MESH)
    across = on(1 - plane, 0)
    pl.semaphore_signal(barrier, inc=1, device_id={"seq": far, "tensor": across}, device_id_type=MESH)
    w_load = pltpu.make_async_copy(w_hbm, w_ref, w_own.at[0])
    w_load.start()
    values[:, HD:, :] = jnp.ones((BLOCKS, values.shape[1] - HD, rows), BF16)
    acc[...] = jnp.zeros_like(acc)
    peak[...] = jnp.full_like(peak, -1e30)
    q_in[0] = q_ref[y]
    obuf[:, :, rows:] = jnp.zeros((RING, HD, obuf.shape[2] - rows), BF16)
    key_rows[0] = kv_ref[y, :HD].T
    values[0, :HD] = kv_ref[y, HD:]
    pl.semaphore_wait(barrier, len(peers) + len(friends) + 1)

    pieces = 2 * RING
    both = ((up_ref, up_all), (down_ref, down_all))

    def piece(j, which):
        return lax.rem(y + (0, 2, 1, 3)[j], RING) * 2 + which

    def f_copy(k, j):
        ref, whole = both[k]
        size = ref.shape[0] // pieces
        number = piece(j, core)
        src = ref.at[pl.ds(pl.multiple_of(number * size, size), size)]
        device = {"tensor": across} if k == 0 else {"seq": far, "tensor": across}
        return pltpu.make_async_remote_copy(
            src_ref=src, dst_ref=whole.at[number], send_sem=f_send.at[2 * k + j], recv_sem=f_recv.at[2 * k + j],
            device_id=device, device_id_type=MESH,
        )

    def g_copy(k, step):
        whole = both[k][1]
        number = piece(0, core)
        i = 2 * k + step // 2
        j = 2 * k + 1 - step // 2
        return remote(whole.at[number], whole.at[number], g_send.at[i], g_recv.at[j], at(step))

    def h_copy(k, j, which):
        whole = both[k][1]
        number = piece(j, which)
        i = 4 * k + j
        return remote(whole.at[number], whole.at[number], h_send.at[i], h_recv.at[i], twin)

    cut = w_ref.shape[0] // 2
    rows_of = lambda which: pl.ds(pl.multiple_of(which * cut, cut), cut)

    def w_copy(src, owner, index, friend):
        return pltpu.make_async_remote_copy(
            src_ref=src, dst_ref=w_all.at[owner, rows_of(core)], send_sem=w_send.at[index], recv_sem=w_recv.at[index],
            device_id={"tensor": friend}, device_id_type=MESH,
        )

    def w_of(side, step, index, friend):
        owner = on(side, step)
        return w_copy(w_all.at[owner, rows_of(core)], owner, index, friend)

    def t_copy(index, which):
        owner = on(plane, index + 1) if index < 3 else on(1 - plane, index - 3)
        return remote(
            w_all.at[owner, rows_of(which)], w_all.at[owner, rows_of(which)], t_send.at[index], t_recv.at[index], twin
        )

    w_mine = w_ref.at[rows_of(core)]
    w_local = pltpu.make_async_copy(w_ref, w_all.at[tensor], w_own.at[1])

    def arrived(index):
        w_copy(w_mine, tensor, index, tensor).wait_recv()
        t_copy(index, core).start()

    def pass_on(c):
        @pl.when(c == 5)
        def _():
            for k in range(2):
                f_copy(k, 1).start()
                f_copy(k, 0).wait_recv()
                for step in (1, 3):
                    g_copy(k, step).start()
                h_copy(k, 0, core).start()

        @pl.when(c == 13)
        def _():
            for k in range(2):
                for step in (1, 3):
                    g_copy(k, step).wait_recv()
                for j in (2, 3):
                    h_copy(k, j, core).start()

        @pl.when(c == BLOCKS - 1)
        def _():
            for k in range(2):
                f_copy(k, 1).wait_recv()
                h_copy(k, 1, core).start()

        @pl.when(c == 6)
        def _():
            arrived(3)
            for step in (1, 3, 2):
                w_copy(w_all.at[on(1 - plane, 0), rows_of(core)], on(1 - plane, 0), 3 + RING - step, on(plane, step)).start()

        @pl.when(c == 10)
        def _():
            for index in (0, 2, 1):
                arrived(index)

        @pl.when(c == BLOCKS - 1)
        def _():
            for index in (4, 6, 5):
                arrived(index)

    def q_copy(step):
        return remote(
            q_ref.at[lax.rem(y + step, RING)], q_in.at[RING - step], q_send.at[step], q_recv.at[RING - step], at(step)
        )

    def y_copy(step):
        slot = {1: 3, 2: 4, 3: 2}[step]
        return remote(
            kv_ref.at[lax.rem(y + step, RING)], kv_in.at[slot], y_send.at[step], kv_recv.at[slot], at(step)
        )

    def z_copy(src, slot):
        return remote(src, kv_in.at[slot], z_send.at[slot], kv_recv.at[slot], far)

    def d_copy(src, slot):
        return remote(src, kv_in.at[slot], d_send.at[slot], kv_recv.at[slot], twin)

    own = kv_ref.at[y]
    for step in (1, 3, 2):
        q_copy(step).start()
    d_copy(own, 1).start()
    for step in (1, 3, 2):
        y_copy(step).start()
    z_copy(own, 8).start()
    f_copy(0, 0).start()
    f_copy(1, 0).start()
    w_load.wait()
    w_local.start()
    w_copy(w_mine, tensor, 3, across).start()
    for step in (1, 3, 2):
        w_copy(w_mine, tensor, RING - step - 1, on(plane, step)).start()

    def arrive(c):
        d_copy(kv_in.at[c], c).wait_recv()

        @pl.when((c >= 2) & (c <= 4))
        def _():
            d_copy(kv_in.at[c], c + 3).start()
            z_copy(kv_in.at[c], 2 * c + 6).start()

        @pl.when((c >= 8) & (lax.rem(c, 2) == 0))
        def _():
            d_copy(kv_in.at[c], c + 1).start()

        pass_on(c)

    def score(c, s, b):
        for lanes in TILES:
            found = dot(key_rows[c], q_in[s, :, lanes])
            scores[b, :rows, lanes] = found
            scores[b, rows : rows + 1, lanes] = jnp.max(found, axis=0, keepdims=True)

    def weigh(c, s, b):
        for lanes in TILES:
            old = peak[s, :, lanes]
            new = jnp.maximum(old, scores[b, rows : rows + 1, lanes])
            peak[s, :, lanes] = new
            weights = jnp.exp2(scores[b, :rows, lanes] - new).astype(BF16)
            acc[s, :, lanes] = acc[s, :, lanes] * jnp.exp2(old - new) + dot(values[c], weights)

    order = (0, 1, 3, 2)

    def block(c, first=False):
        after = jnp.minimum(c + 1, BLOCKS - 1)
        if first:
            arrive(after)
        else:
            @pl.when(c < BLOCKS - 1)
            def _():
                arrive(after)

        key_rows[after] = kv_in[after, :HD].T
        values[after, :HD] = kv_in[after, HD:]
        for i, s in enumerate(order):
            if first and i < 3:
                q_copy(RING - order[i + 1]).wait_recv()
            if i < 3:
                score(c, order[i + 1], 1 - i % 2)
            else:
                score(after, order[0], 0)
            weigh(c, s, i % 2)

    score(0, order[0], 0)
    block(jnp.int32(0), True)

    def body(c, carry):
        block(c)
        return carry

    lax.fori_loop(1, BLOCKS, body, 0)

    def o_copy(step):
        return remote(obuf.at[step], out_ref.at[y], o_send.at[step], o_recv.at[RING - step], at(step))

    for s in (2, 1, 3):
        obuf[s, :, :rows] = (acc[s, :HD] / acc[s, HD : HD + 1]).astype(BF16)
        o_copy(s).start()
    out_ref[y, :, :rows] = (acc[0, :HD] / acc[0, HD : HD + 1]).astype(BF16)
    out_ref[y, :, rows:] = jnp.zeros((HD, out_ref.shape[2] - rows), BF16)

    def o_wait(step):
        return remote(
            obuf.at[step], out_ref.at[lax.rem(y + step, RING)], o_send.at[step], o_recv.at[step], at(step)
        )

    for step in (1, 2, 3):
        q_copy(step).wait_send()
        y_copy(step).wait_send()
        o_copy(step).wait_send()
    for slot in (8, 10, 12, 14):
        z_copy(own, slot).wait_send()
    for slot in (1, 5, 6, 7, 9, 11, 13, 15):
        d_copy(own, slot).wait_send()
    for index in range(7):
        w_copy(w_mine, tensor, index, tensor).wait_send()
        t_copy(index, core).wait_send()
        t_copy(index, 1 - core).wait_recv()
    w_local.wait()
    for k in range(2):
        for j in range(2):
            f_copy(k, j).wait_send()
        for step in (1, 3):
            g_copy(k, step).wait_send()
        for j in range(4):
            h_copy(k, j, core).wait_send()
            h_copy(k, j, 1 - core).wait_recv()
    for step in (1, 3, 2):
        o_wait(step).wait_recv()


def attend(query, kv, w_out, w_up, w_down, padded, n_tensor):
    heads, width, rows = query.shape
    dma = lambda n: pltpu.SemaphoreType.DMA((n,))
    vmem = pl.BlockSpec(memory_space=pltpu.VMEM)
    hbm = pl.BlockSpec(memory_space=pltpu.HBM)
    return pl.pallas_call(
        attend_kernel,
        in_specs=[vmem, vmem, hbm, hbm, hbm],
        out_specs=[vmem, hbm, hbm, hbm],
        out_shape=[
            jax.ShapeDtypeStruct((heads, width, padded), BF16),
            jax.ShapeDtypeStruct((n_tensor, *w_out.shape), BF16),
            *(jax.ShapeDtypeStruct((2 * RING, w.shape[0] // (2 * RING), w.shape[1]), BF16) for w in (w_up, w_down)),
        ],
        scratch_shapes=[
            pltpu.VMEM(w_out.shape, BF16),
            pltpu.VMEM((heads, width, rows), BF16),
            pltpu.VMEM((BLOCKS, 2 * width, rows), BF16),
            pltpu.VMEM((BLOCKS, rows, width), BF16),
            pltpu.VMEM((BLOCKS, width + 16, rows), BF16),
            pltpu.VMEM((heads, width + 16, rows), F32),
            pltpu.VMEM((heads, 1, rows), F32),
            pltpu.VMEM((2, rows + 8, rows), F32),
            pltpu.VMEM((heads, width, padded), BF16),
            dma(RING), dma(RING), dma(RING), dma(BLOCKS), dma(BLOCKS), dma(BLOCKS), dma(RING), dma(RING),
            dma(7), dma(7), dma(7), dma(7), dma(2),
            dma(4), dma(4), dma(4), dma(4), dma(8), dma(8),
        ],
        cost_estimate=pl.CostEstimate(flops=40 * 10**9, bytes_accessed=8 << 20, transcendentals=0),
        compiler_params=pltpu.CompilerParams(
            vmem_limit_bytes=40 << 20, collective_id=0, has_side_effects=True
        ),
    )(query, kv, w_out, w_up, w_down)


class Tensor:
    def __init__(self):
        self.me = lax.axis_index("tensor")
        self.plane, self.x = self.me // RING, lax.rem(self.me, RING)
        self.right, self.left = self.on(self.plane, 1), self.on(self.plane, 3)
        self.pair = self.on(1 - self.plane, 0)

    def on(self, side, step):
        return side * RING + lax.rem(self.x + step, RING)

    def meet(self):
        barrier = pltpu.get_barrier_semaphore()
        for friend in (self.right, self.left, self.pair):
            pl.semaphore_signal(barrier, inc=1, device_id={"tensor": friend}, device_id_type=MESH)
        pl.semaphore_wait(barrier, 3)


def send(src, dst, send_sem, recv_sem, friend):
    return pltpu.make_async_remote_copy(
        src_ref=src, dst_ref=dst, send_sem=send_sem, recv_sem=recv_sem,
        device_id={"tensor": friend}, device_id_type=MESH,
    )


def gather(t, mine, buf, cut, send_sem, recv_sem):
    lo, hi = pl.ds(0, cut), pl.ds(cut, cut)
    copies = {
        "right": (mine, t.me, None, t.right, 0),
        "left": (mine, t.me, None, t.left, 1),
        "pair": (mine, t.me, None, t.pair, 2),
        "far lo": (None, t.left, lo, t.right, 3),
        "far hi": (None, t.right, hi, t.left, 4),
        "over right": (None, t.pair, None, t.right, 5),
        "over left": (None, t.pair, None, t.left, 6),
        "pair lo": (None, t.on(t.plane, 2), lo, t.pair, 7),
        "pair hi": (None, t.on(t.plane, 2), hi, t.pair, 8),
    }

    def copy(name):
        src, block, part, to, i = copies[name]
        dst = buf.at[block] if part is None else buf.at[block, part]
        return send(dst if src is None else src, dst, send_sem.at[i], recv_sem.at[i], to)

    for name in ("right", "left", "pair"):
        copy(name).start()
    copy("right").wait_recv()
    copy("far lo").start()
    copy("left").wait_recv()
    copy("far hi").start()
    copy("pair").wait_recv()
    copy("over right").start()
    copy("over left").start()
    copy("far lo").wait_recv()
    copy("pair lo").start()
    copy("far hi").wait_recv()
    copy("pair hi").start()
    for name in ("over right", "over left", "pair lo", "pair hi"):
        copy(name).wait_recv()
    for name in copies:
        copy(name).wait_send()


def tail_kernel(
    heads_ref, tokens_hbm, gain_ref, w_hbm, up_hbm, up_pair_hbm, down_hbm, down_pair_hbm, out_ref,
    heads, w_out, up, down, tokens, mixed, term, own, half_in, edge_in, edge_sum,
    a_send, a_recv, s_send, s_recv, g_send, g_recv, load_sem,
):
    t = Tensor()
    half, model = mixed.shape
    part = half // RING
    there = 1 - t.plane
    valid = tokens_hbm.shape[0] - half
    loads = [
        pltpu.make_async_copy(w_hbm, w_out, load_sem.at[0]),
        pltpu.make_async_copy(up_hbm, up.at[0], load_sem.at[1]),
        pltpu.make_async_copy(up_pair_hbm, up.at[1], load_sem.at[2]),
        pltpu.make_async_copy(down_hbm, down.at[0], load_sem.at[3]),
        pltpu.make_async_copy(down_pair_hbm, down.at[1], load_sem.at[4]),
    ]
    first = pltpu.make_async_copy(tokens_hbm.at[pl.ds(0, half)], tokens, load_sem.at[5])
    second = pltpu.make_async_copy(tokens_hbm.at[pl.ds(half, valid)], tokens.at[pl.ds(0, valid)], load_sem.at[5])

    @pl.when(t.plane == 0)
    def _():
        first.start()

    @pl.when(t.plane == 1)
    def _():
        second.start()
        tokens[valid:] = jnp.zeros((half - valid, model), BF16)

    for load in loads:
        load.start()
    t.meet()

    cut = heads_ref.shape[0] // 2
    lo, hi = pl.ds(0, cut), pl.ds(cut, cut)
    lanes = lambda plane: pl.ds(pl.multiple_of(plane * half, half), half)

    def copy(src, block, rows, to, i):
        dst = heads.at[block] if rows is None else heads.at[block, rows]
        return send(dst if src is None else src, dst, a_send.at[i], a_recv.at[i], to)

    mine, theirs = heads_ref.at[:, lanes(t.plane)], heads_ref.at[:, lanes(there)]
    copies = [
        copy(mine, t.me, None, t.right, 0),
        copy(mine, t.me, None, t.left, 1),
        copy(theirs, t.me, None, t.pair, 2),
        copy(None, t.left, lo, t.right, 3),
        copy(None, t.right, hi, t.left, 4),
        copy(None, t.pair, None, t.right, 5),
        copy(None, t.pair, None, t.left, 6),
        copy(None, t.on(there, 3), lo, t.right, 7),
        copy(None, t.on(there, 1), hi, t.left, 8),
    ]
    for i in (2, 0, 1):
        copies[i].start()
    heads[t.me] = heads_ref[:, lanes(t.plane)]

    @pl.when(t.plane == 0)
    def _():
        first.wait()

    @pl.when(t.plane == 1)
    def _():
        second.wait()

    mixed[...] = tokens[...].astype(F32)
    loads[0].wait()

    def group(i, carry):
        for when, waits, starts in (
            (1, (2,), (5, 6)),
            (2, (0,), (3,)),
            (3, (1, 5), (4, 7)),
            (4, (6,), (8,)),
            (6, (3, 4), ()),
            (7, (7, 8), ()),
        ):
            @pl.when(i == when)
            def _():
                for one in waits:
                    copies[one].wait_recv()
                for one in starts:
                    copies[one].start()

        step = lax.rem(3 * (i // 2) * (i // 2 + 1) // 2, RING)
        side = lax.rem(t.plane + i, 2)
        who = side * RING + lax.rem(t.x + step, RING)
        mixed[...] += lax.dot_general(
            heads[who], w_out[who], (((0,), (0,)), ((), ())), preferred_element_type=F32
        )
        return carry

    lax.fori_loop(0, 2 * RING, group, 0)
    for load in loads[1:]:
        load.wait()

    cut = part // 2
    lo, hi = pl.ds(0, cut), pl.ds(cut, cut)
    right, left, far = (lax.rem(t.x + step, RING) for step in (1, 3, 2))

    def sums(src, dst, i, to):
        return send(src, dst, s_send.at[i], s_recv.at[i], to)

    half_left = sums(term.at[far, lo], half_in.at[0], 0, t.left)
    half_right = sums(term.at[far, hi], half_in.at[1], 1, t.right)
    edge_right = sums(term.at[right, lo], edge_in.at[0, lo], 2, t.right)
    edge_left = sums(term.at[left, hi], edge_in.at[1, hi], 3, t.left)
    sum_left = sums(edge_sum.at[0], edge_in.at[1, lo], 4, t.left)
    sum_right = sums(edge_sum.at[1], edge_in.at[0, hi], 5, t.right)
    rows_of = lambda b: pl.ds(pl.multiple_of(b * part, part), part)

    def feed(i, carry):
        b = lax.rem(t.x + 2 + 3 * i * (i + 1) // 2, RING)
        post = layer_norm(mixed[rows_of(b)], gain_ref[...]).astype(BF16)
        wide = lambda k: jax.nn.gelu(dot(post, up[k]), approximate=True).astype(BF16)
        term[b] = (dot(wide(0), down[0]) + dot(wide(1), down[1])).astype(BF16)
        for when, starts in ((0, (half_left, half_right)), (1, (edge_right,)), (2, (edge_left,))):
            @pl.when(i == when)
            def _():
                for one in starts:
                    one.start()
        return carry

    lax.fori_loop(0, RING, feed, 0)
    half_left.wait_recv()
    edge_sum[0] = (half_in[0].astype(F32) + term[left, lo].astype(F32)).astype(BF16)
    sum_left.start()
    half_right.wait_recv()
    edge_sum[1] = (half_in[1].astype(F32) + term[right, hi].astype(F32)).astype(BF16)
    sum_right.start()
    base = mixed[rows_of(t.x)] + term[t.x].astype(F32)
    mixed[rows_of(t.x)] = base
    for one in (edge_right, edge_left, sum_left, sum_right):
        one.wait_recv()
    own[...] = (mixed[rows_of(t.x)] + edge_in[0].astype(F32) + edge_in[1].astype(F32)).astype(BF16)
    out_ref[t.me] = own[...]
    for one in (*copies, half_left, half_right, edge_right, edge_left, sum_left, sum_right):
        one.wait_send()
    gather(t, own, out_ref, cut, g_send, g_recv)


def tail(heads, tokens, gain, w_out, up, up_pair, down, down_pair, part):
    n_tensor, span, model = w_out.shape
    half = RING * part
    dma = lambda n: pltpu.SemaphoreType.DMA((n,))
    vmem = pl.BlockSpec(memory_space=pltpu.VMEM)
    hbm = pl.BlockSpec(memory_space=pltpu.HBM)
    return pl.pallas_call(
        tail_kernel,
        in_specs=[vmem, hbm, vmem, hbm, hbm, hbm, hbm, hbm],
        out_specs=vmem,
        out_shape=jax.ShapeDtypeStruct((n_tensor, part, model), BF16),
        scratch_shapes=[
            pltpu.VMEM((n_tensor, span, half), BF16),
            pltpu.VMEM(w_out.shape, BF16),
            pltpu.VMEM((2, *up.shape), BF16),
            pltpu.VMEM((2, *down.shape), BF16),
            pltpu.VMEM((half, model), BF16),
            pltpu.VMEM((half, model), F32),
            pltpu.VMEM((RING, part, model), BF16),
            pltpu.VMEM((part, model), BF16),
            pltpu.VMEM((2, part // 2, model), BF16),
            pltpu.VMEM((2, part, model), BF16),
            pltpu.VMEM((2, part // 2, model), BF16),
            dma(9), dma(9), dma(6), dma(6), dma(9), dma(9), dma(6),
        ],
        cost_estimate=pl.CostEstimate(flops=60 * 10**9, bytes_accessed=20 << 20, transcendentals=0),
        compiler_params=pltpu.CompilerParams(vmem_limit_bytes=48 << 20, collective_id=1, has_side_effects=True),
    )(heads, tokens, gain, w_out, up, up_pair, down, down_pair)


def per_device(n_seq, n_tensor, tokens, norm_gain, w_qkv, w_out, post_gain, w_up, w_down):
    rows, model = tokens.shape
    span = w_qkv.shape[2]
    heads = span // HD
    part = -(-rows // (16 * n_tensor)) * 16
    padded = n_tensor * part

    base = tokens.astype(F32)
    normed = layer_norm(base, norm_gain).astype(BF16)
    qkv = lax.dot_general(
        w_qkv.reshape(model, -1), normed, (((0,), (1,)), ((), ())), preferred_element_type=F32
    ).reshape(3, heads, HD, rows)
    query = (qkv[0] * (LOG2E / HD**0.5)).astype(BF16)
    kv = jnp.concatenate([qkv[1], qkv[2]], axis=1).astype(BF16)
    attended, w_out_all, up_pair, down_pair = attend(query, kv, w_out, w_up, w_down, padded, n_tensor)
    out = tail(
        attended.reshape(span, padded), tokens, post_gain.reshape(1, model), w_out_all,
        w_up, up_pair.reshape(w_up.shape), w_down, down_pair.reshape(w_down.shape), part,
    )
    return out.reshape(padded, model)[:rows]


def solution(mesh):
    placed = (
        P("seq", None),
        P(),
        P(None, None, "tensor"),
        P("tensor", None),
        P(),
        P(None, "tensor"),
        P("tensor", None),
    )
    body = functools.partial(per_device, mesh.shape["seq"], mesh.shape["tensor"])
    return jax.shard_map(
        body, mesh=mesh, in_specs=placed, out_specs=P("seq", None), check_vma=False
    )
```

```python
import functools
import jax
import jax.numpy as jnp
from jax import lax
from jax.experimental import pallas as pl
from jax.experimental.pallas import tpu as pltpu
from jax.sharding import PartitionSpec as P

HD = 48
LOG2E = 1.4426950408889634
MESH = pl.DeviceIdType.MESH
F32 = jnp.float32
BF16 = jnp.bfloat16
RING = 4
BLOCKS = 16
TILES = (slice(0, 256), slice(256, 512), slice(512, 720))


def layer_norm(values, gain):
    mean = jnp.mean(values, axis=-1, keepdims=True)
    centred = values - mean
    var = jnp.mean(centred * centred, axis=-1, keepdims=True)
    return centred * lax.rsqrt(var + 1e-05) * gain


def dot(a, b):
    return jnp.dot(a, b, preferred_element_type=F32)


def remote(src, dst, send, recv, seq):
    return pltpu.make_async_remote_copy(
        src_ref=src, dst_ref=dst, send_sem=send, recv_sem=recv, device_id={"seq": seq}, device_id_type=MESH
    )


def attend_kernel(
    q_ref, kv_ref, w_hbm, up_ref, down_ref, out_ref, w_all, up_all, down_all, w_ref, q_in, kv_in, key_rows, values, acc, peak, scores, obuf,
    q_send, q_recv, y_send, z_send, d_send, kv_recv, o_send, o_recv, w_send, w_recv, t_send, t_recv, w_own,
    f_send, f_recv, g_send, g_recv, h_send, h_recv,
):
    rows = q_ref.shape[2]
    me = lax.axis_index("seq")
    half, y, core = me // (2 * RING), (me // 2) % RING, me % 2

    def at(step):
        return half * (2 * RING) + lax.rem(y + step, RING) * 2 + core

    twin = me - core + (1 - core)
    far = lax.rem(me + 2 * RING, BLOCKS)
    peers = [at(1), at(2), at(3), twin, far]
    tensor = lax.axis_index("tensor")
    plane, x = tensor // RING, lax.rem(tensor, RING)

    def on(side, step):
        return side * RING + lax.rem(x + step, RING)

    friends = [on(plane, 1), on(plane, 2), on(plane, 3), on(1 - plane, 0)]
    barrier = pltpu.get_barrier_semaphore()
    for peer in peers:
        pl.semaphore_signal(barrier, inc=1, device_id={"seq": peer}, device_id_type=MESH)
    for friend in friends:
        pl.semaphore_signal(barrier, inc=1, device_id={"tensor": friend}, device_id_type=MESH)
    across = on(1 - plane, 0)
    pl.semaphore_signal(barrier, inc=1, device_id={"seq": far, "tensor": across}, device_id_type=MESH)
    w_load = pltpu.make_async_copy(w_hbm, w_ref, w_own.at[0])
    w_load.start()
    values[:, HD:, :] = jnp.ones((BLOCKS, values.shape[1] - HD, rows), BF16)
    acc[...] = jnp.zeros_like(acc)
    peak[...] = jnp.full_like(peak, -1e30)
    q_in[0] = q_ref[y]
    obuf[:, :, rows:] = jnp.zeros((RING, HD, obuf.shape[2] - rows), BF16)
    key_rows[0] = kv_ref[y, :HD].T
    values[0, :HD] = kv_ref[y, HD:]
    pl.semaphore_wait(barrier, len(peers) + len(friends) + 1)

    pieces = 2 * RING
    both = ((up_ref, up_all), (down_ref, down_all))

    def piece(j, which):
        return lax.rem(y + (0, 2, 1, 3)[j], RING) * 2 + which

    def f_copy(k, j):
        ref, whole = both[k]
        size = ref.shape[0] // pieces
        number = piece(j, core)
        src = ref.at[pl.ds(pl.multiple_of(number * size, size), size)]
        device = {"tensor": across} if k == 0 else {"seq": far, "tensor": across}
        return pltpu.make_async_remote_copy(
            src_ref=src, dst_ref=whole.at[number], send_sem=f_send.at[2 * k + j], recv_sem=f_recv.at[2 * k + j],
            device_id=device, device_id_type=MESH,
        )

    def g_copy(k, step):
        whole = both[k][1]
        number = piece(0, core)
        i = 2 * k + step // 2
        j = 2 * k + 1 - step // 2
        return remote(whole.at[number], whole.at[number], g_send.at[i], g_recv.at[j], at(step))

    def h_copy(k, j, which):
        whole = both[k][1]
        number = piece(j, which)
        i = 4 * k + j
        return remote(whole.at[number], whole.at[number], h_send.at[i], h_recv.at[i], twin)

    cut = w_ref.shape[0] // 2
    rows_of = lambda which: pl.ds(pl.multiple_of(which * cut, cut), cut)

    def w_copy(src, owner, index, friend):
        return pltpu.make_async_remote_copy(
            src_ref=src, dst_ref=w_all.at[owner, rows_of(core)], send_sem=w_send.at[index], recv_sem=w_recv.at[index],
            device_id={"tensor": friend}, device_id_type=MESH,
        )

    def w_of(side, step, index, friend):
        owner = on(side, step)
        return w_copy(w_all.at[owner, rows_of(core)], owner, index, friend)

    def t_copy(index, which):
        owner = on(plane, index + 1) if index < 3 else on(1 - plane, index - 3)
        return remote(
            w_all.at[owner, rows_of(which)], w_all.at[owner, rows_of(which)], t_send.at[index], t_recv.at[index], twin
        )

    w_mine = w_ref.at[rows_of(core)]
    w_local = pltpu.make_async_copy(w_ref, w_all.at[tensor], w_own.at[1])

    def arrived(index):
        w_copy(w_mine, tensor, index, tensor).wait_recv()
        t_copy(index, core).start()

    def pass_on(c):
        @pl.when(c == 5)
        def _():
            for k in range(2):
                f_copy(k, 0).wait_recv()
                for step in (1, 3):
                    g_copy(k, step).start()
                h_copy(k, 0, core).start()

        @pl.when(c == 6)
        def _():
            arrived(3)
            for step in (1, 3, 2):
                w_copy(w_all.at[across, rows_of(core)], across, 3 + RING - step, on(plane, step)).start()

        @pl.when(c == 7)
        def _():
            for k in range(2):
                f_copy(k, 1).start()

        @pl.when(c == 11)
        def _():
            for index in (0, 2, 1):
                arrived(index)

    def q_copy(step):
        return remote(
            q_ref.at[lax.rem(y + step, RING)], q_in.at[RING - step], q_send.at[step], q_recv.at[RING - step], at(step)
        )

    def y_copy(step):
        slot = {1: 3, 2: 6, 3: 2}[step]
        return remote(
            kv_ref.at[lax.rem(y + step, RING)], kv_in.at[slot], y_send.at[step], kv_recv.at[slot], at(step)
        )

    def z_copy(src, slot):
        return remote(src, kv_in.at[slot], z_send.at[slot], kv_recv.at[slot], far)

    def d_copy(src, slot):
        return remote(src, kv_in.at[slot], d_send.at[slot], kv_recv.at[slot], twin)

    own = kv_ref.at[y]
    for step in (1, 3, 2):
        q_copy(step).start()
    d_copy(own, 1).start()
    for step in (1, 3, 2):
        y_copy(step).start()
    z_copy(own, 8).start()
    f_copy(0, 0).start()
    f_copy(1, 0).start()
    w_load.wait()
    w_local.start()
    w_copy(w_mine, tensor, 3, across).start()
    for step in (1, 3, 2):
        w_copy(w_mine, tensor, RING - step - 1, on(plane, step)).start()

    def arrive(c):
        d_copy(kv_in.at[c], c).wait_recv()

        @pl.when((c == 2) | (c == 3))
        def _():
            d_copy(kv_in.at[c], c + 2).start()
            z_copy(kv_in.at[c], 2 * c + 6).start()

        @pl.when(c == 6)
        def _():
            d_copy(kv_in.at[c], c + 1).start()
            z_copy(kv_in.at[c], 14).start()

        @pl.when((c >= 8) & (lax.rem(c, 2) == 0))
        def _():
            d_copy(kv_in.at[c], c + 1).start()

        pass_on(c)

    def prepare(c):
        key_rows[c] = kv_in[c, :HD].T
        values[c, :HD] = kv_in[c, HD:]

    def score(c, s, b):
        for lanes in TILES:
            found = dot(key_rows[c], q_in[s, :, lanes])
            scores[b, :rows, lanes] = found
            scores[b, rows : rows + 1, lanes] = jnp.max(found, axis=0, keepdims=True)

    def weigh(c, s, b):
        for lanes in TILES:
            old = peak[s, :, lanes]
            new = jnp.maximum(old, scores[b, rows : rows + 1, lanes])
            peak[s, :, lanes] = new
            weights = jnp.exp2(scores[b, :rows, lanes] - new).astype(BF16)
            acc[s, :, lanes] = acc[s, :, lanes] * jnp.exp2(old - new) + dot(values[c], weights)

    def o_copy(step):
        return remote(obuf.at[step], out_ref.at[y], o_send.at[step], o_recv.at[RING - step], at(step))

    opening = [(c, s) for s in (0, 1, 3, 2) for c in (0, 1)]
    last = 12
    order = (3, 0, 1, 2)
    score(0, 0, 0)
    for i, (c, s) in enumerate(opening):
        if i == 0:
            arrive(jnp.int32(1))
            prepare(1)
        elif i == len(opening) - 1:
            arrive(jnp.int32(2))
            prepare(2)
        after = opening[i + 1] if i + 1 < len(opening) else (2, order[0])
        if i in (1, 3, 5):
            q_copy(RING - after[1]).wait_recv()
        score(*after, (i + 1) % 2)
        weigh(c, s, i % 2)

    def body(c, carry):
        arrive(c + 1)

        @pl.when(c == last - 1)
        def _():
            arrive(jnp.int32(14))

        prepare(c + 1)
        for i, s in enumerate(order):
            if i < 3:
                score(c, order[i + 1], 1 - i % 2)
            else:
                score(c + 1, order[0], 0)
            weigh(c, s, i % 2)
        return carry

    lax.fori_loop(2, last, body, 0)

    arrive(jnp.int32(13))
    arrive(jnp.int32(15))
    for k in range(2):
        for step in (1, 3):
            g_copy(k, step).wait_recv()
        for j in (2, 3):
            h_copy(k, j, core).start()
    for c in range(last + 1, BLOCKS):
        prepare(c)

    def close(i, carry):
        s = RING - 1 - i
        for k in range(RING):
            if k < RING - 1:
                score(last + k + 1, s, 1 - k % 2)
            else:
                score(last, jnp.maximum(s - 1, 0), 0)
            weigh(last + k, s, k % 2)
        result = (acc[s, :HD] / acc[s, HD : HD + 1]).astype(BF16)

        @pl.when(s > 0)
        def _():
            obuf[s, :, :rows] = result
            o_copy(s).start()

        @pl.when(s == 0)
        def _():
            out_ref[y, :, :rows] = result

        @pl.when(s == 1)
        def _():
            for k in range(2):
                f_copy(k, 1).wait_recv()
                h_copy(k, 1, core).start()
            for index in (4, 6, 5):
                arrived(index)

        return carry

    lax.fori_loop(0, RING, close, 0)
    out_ref[y, :, rows:] = jnp.zeros((HD, out_ref.shape[2] - rows), BF16)

    def o_wait(step):
        return remote(
            obuf.at[step], out_ref.at[lax.rem(y + step, RING)], o_send.at[step], o_recv.at[step], at(step)
        )

    for step in (1, 2, 3):
        q_copy(step).wait_send()
        y_copy(step).wait_send()
        o_copy(step).wait_send()
    for slot in (8, 10, 12, 14):
        z_copy(own, slot).wait_send()
    for slot in (1, 4, 5, 7, 9, 11, 13, 15):
        d_copy(own, slot).wait_send()
    for index in range(7):
        w_copy(w_mine, tensor, index, tensor).wait_send()
        t_copy(index, core).wait_send()
        t_copy(index, 1 - core).wait_recv()
    w_local.wait()
    for k in range(2):
        for j in range(2):
            f_copy(k, j).wait_send()
        for step in (1, 3):
            g_copy(k, step).wait_send()
        for j in range(4):
            h_copy(k, j, core).wait_send()
            h_copy(k, j, 1 - core).wait_recv()
    for step in (1, 3, 2):
        o_wait(step).wait_recv()


def attend(query, kv, w_out, w_up, w_down, padded, n_tensor):
    heads, width, rows = query.shape
    dma = lambda n: pltpu.SemaphoreType.DMA((n,))
    vmem = pl.BlockSpec(memory_space=pltpu.VMEM)
    hbm = pl.BlockSpec(memory_space=pltpu.HBM)
    return pl.pallas_call(
        attend_kernel,
        in_specs=[vmem, vmem, hbm, hbm, hbm],
        out_specs=[vmem, hbm, hbm, hbm],
        out_shape=[
            jax.ShapeDtypeStruct((heads, width, padded), BF16),
            jax.ShapeDtypeStruct((n_tensor, *w_out.shape), BF16),
            *(jax.ShapeDtypeStruct((2 * RING, w.shape[0] // (2 * RING), w.shape[1]), BF16) for w in (w_up, w_down)),
        ],
        scratch_shapes=[
            pltpu.VMEM(w_out.shape, BF16),
            pltpu.VMEM((heads, width, rows), BF16),
            pltpu.VMEM((BLOCKS, 2 * width, rows), BF16),
            pltpu.VMEM((BLOCKS, rows, width), BF16),
            pltpu.VMEM((BLOCKS, width + 16, rows), BF16),
            pltpu.VMEM((heads, width + 16, rows), F32),
            pltpu.VMEM((heads, 1, rows), F32),
            pltpu.VMEM((2, rows + 8, rows), F32),
            pltpu.VMEM((heads, width, padded), BF16),
            dma(RING), dma(RING), dma(RING), dma(BLOCKS), dma(BLOCKS), dma(BLOCKS), dma(RING), dma(RING),
            dma(7), dma(7), dma(7), dma(7), dma(2),
            dma(4), dma(4), dma(4), dma(4), dma(8), dma(8),
        ],
        cost_estimate=pl.CostEstimate(flops=40 * 10**9, bytes_accessed=8 << 20, transcendentals=0),
        compiler_params=pltpu.CompilerParams(
            vmem_limit_bytes=62 << 20, collective_id=0, has_side_effects=True
        ),
    )(query, kv, w_out, w_up, w_down)


class Tensor:
    def __init__(self):
        self.me = lax.axis_index("tensor")
        self.plane, self.x = self.me // RING, lax.rem(self.me, RING)
        self.right, self.left = self.on(self.plane, 1), self.on(self.plane, 3)
        self.pair = self.on(1 - self.plane, 0)

    def on(self, side, step):
        return side * RING + lax.rem(self.x + step, RING)

    def meet(self):
        barrier = pltpu.get_barrier_semaphore()
        for friend in (self.right, self.left, self.pair):
            pl.semaphore_signal(barrier, inc=1, device_id={"tensor": friend}, device_id_type=MESH)
        pl.semaphore_wait(barrier, 3)


def send(src, dst, send_sem, recv_sem, friend):
    return pltpu.make_async_remote_copy(
        src_ref=src, dst_ref=dst, send_sem=send_sem, recv_sem=recv_sem,
        device_id={"tensor": friend}, device_id_type=MESH,
    )


def gather(t, mine, buf, cut, send_sem, recv_sem):
    lo, hi = pl.ds(0, cut), pl.ds(cut, cut)
    copies = {
        "right": (mine, t.me, None, t.right, 0),
        "left": (mine, t.me, None, t.left, 1),
        "pair": (mine, t.me, None, t.pair, 2),
        "far lo": (None, t.left, lo, t.right, 3),
        "far hi": (None, t.right, hi, t.left, 4),
        "over right": (None, t.pair, None, t.right, 5),
        "over left": (None, t.pair, None, t.left, 6),
        "pair lo": (None, t.on(t.plane, 2), lo, t.pair, 7),
        "pair hi": (None, t.on(t.plane, 2), hi, t.pair, 8),
    }

    def copy(name):
        src, block, part, to, i = copies[name]
        dst = buf.at[block] if part is None else buf.at[block, part]
        return send(dst if src is None else src, dst, send_sem.at[i], recv_sem.at[i], to)

    for name in ("right", "left", "pair"):
        copy(name).start()
    copy("right").wait_recv()
    copy("far lo").start()
    copy("left").wait_recv()
    copy("far hi").start()
    copy("pair").wait_recv()
    copy("over right").start()
    copy("over left").start()
    copy("far lo").wait_recv()
    copy("pair lo").start()
    copy("far hi").wait_recv()
    copy("pair hi").start()
    for name in ("over right", "over left", "pair lo", "pair hi"):
        copy(name).wait_recv()
    for name in copies:
        copy(name).wait_send()


def tail_kernel(
    heads_ref, tokens_hbm, gain_ref, w_hbm, up_hbm, up_pair_hbm, down_hbm, down_pair_hbm, out_ref,
    heads, w_out, up, down, tokens, mixed, term, own, half_in, edge_in, edge_sum,
    a_send, a_recv, s_send, s_recv, g_send, g_recv, load_sem,
):
    t = Tensor()
    half, model = mixed.shape
    part = half // RING
    there = 1 - t.plane
    valid = tokens_hbm.shape[0] - half
    loads = [
        pltpu.make_async_copy(w_hbm, w_out, load_sem.at[0]),
        pltpu.make_async_copy(up_hbm, up.at[0], load_sem.at[1]),
        pltpu.make_async_copy(up_pair_hbm, up.at[1], load_sem.at[2]),
        pltpu.make_async_copy(down_hbm, down.at[0], load_sem.at[3]),
        pltpu.make_async_copy(down_pair_hbm, down.at[1], load_sem.at[4]),
    ]
    first = pltpu.make_async_copy(tokens_hbm.at[pl.ds(0, half)], tokens, load_sem.at[5])
    second = pltpu.make_async_copy(tokens_hbm.at[pl.ds(half, valid)], tokens.at[pl.ds(0, valid)], load_sem.at[5])

    @pl.when(t.plane == 0)
    def _():
        first.start()

    @pl.when(t.plane == 1)
    def _():
        second.start()
        tokens[valid:] = jnp.zeros((half - valid, model), BF16)

    for load in loads:
        load.start()
    t.meet()

    cut = heads_ref.shape[0] // 2
    lo, hi = pl.ds(0, cut), pl.ds(cut, cut)
    lanes = lambda plane: pl.ds(pl.multiple_of(plane * half, half), half)

    def copy(src, block, rows, to, i):
        dst = heads.at[block] if rows is None else heads.at[block, rows]
        return send(dst if src is None else src, dst, a_send.at[i], a_recv.at[i], to)

    mine, theirs = heads_ref.at[:, lanes(t.plane)], heads_ref.at[:, lanes(there)]
    copies = [
        copy(mine, t.me, None, t.right, 0),
        copy(mine, t.me, None, t.left, 1),
        copy(theirs, t.me, None, t.pair, 2),
        copy(None, t.left, lo, t.right, 3),
        copy(None, t.right, hi, t.left, 4),
        copy(None, t.pair, None, t.right, 5),
        copy(None, t.pair, None, t.left, 6),
        copy(None, t.on(there, 3), lo, t.right, 7),
        copy(None, t.on(there, 1), hi, t.left, 8),
    ]
    for i in (2, 0, 1):
        copies[i].start()
    heads[t.me] = heads_ref[:, lanes(t.plane)]

    @pl.when(t.plane == 0)
    def _():
        first.wait()

    @pl.when(t.plane == 1)
    def _():
        second.wait()

    mixed[...] = tokens[...].astype(F32)
    loads[0].wait()

    def group(i, carry):
        for when, waits, starts in (
            (1, (2,), (5, 6)),
            (2, (0,), (3,)),
            (3, (1, 5), (4, 7)),
            (4, (6,), (8,)),
            (6, (3, 4), ()),
            (7, (7, 8), ()),
        ):
            @pl.when(i == when)
            def _():
                for one in waits:
                    copies[one].wait_recv()
                for one in starts:
                    copies[one].start()

        step = lax.rem(3 * (i // 2) * (i // 2 + 1) // 2, RING)
        side = lax.rem(t.plane + i, 2)
        who = side * RING + lax.rem(t.x + step, RING)
        mixed[...] += lax.dot_general(
            heads[who], w_out[who], (((0,), (0,)), ((), ())), preferred_element_type=F32
        )
        return carry

    lax.fori_loop(0, 2 * RING, group, 0)
    for load in loads[1:]:
        load.wait()

    cut = part // 2
    lo, hi = pl.ds(0, cut), pl.ds(cut, cut)
    right, left, far = (lax.rem(t.x + step, RING) for step in (1, 3, 2))

    def sums(src, dst, i, to):
        return send(src, dst, s_send.at[i], s_recv.at[i], to)

    half_left = sums(term.at[far, lo], half_in.at[0], 0, t.left)
    half_right = sums(term.at[far, hi], half_in.at[1], 1, t.right)
    edge_right = sums(term.at[right, lo], edge_in.at[0, lo], 2, t.right)
    edge_left = sums(term.at[left, hi], edge_in.at[1, hi], 3, t.left)
    sum_left = sums(edge_sum.at[0], edge_in.at[1, lo], 4, t.left)
    sum_right = sums(edge_sum.at[1], edge_in.at[0, hi], 5, t.right)
    rows_of = lambda b: pl.ds(pl.multiple_of(b * part, part), part)

    def feed(i, carry):
        b = lax.rem(t.x + 2 + 3 * i * (i + 1) // 2, RING)
        post = layer_norm(mixed[rows_of(b)], gain_ref[...]).astype(BF16)
        wide = lambda k: jax.nn.gelu(dot(post, up[k]), approximate=True).astype(BF16)
        term[b] = (dot(wide(0), down[0]) + dot(wide(1), down[1])).astype(BF16)
        for when, starts in ((0, (half_left, half_right)), (1, (edge_right,)), (2, (edge_left,))):
            @pl.when(i == when)
            def _():
                for one in starts:
                    one.start()
        return carry

    lax.fori_loop(0, RING, feed, 0)
    half_left.wait_recv()
    edge_sum[0] = (half_in[0].astype(F32) + term[left, lo].astype(F32)).astype(BF16)
    sum_left.start()
    half_right.wait_recv()
    edge_sum[1] = (half_in[1].astype(F32) + term[right, hi].astype(F32)).astype(BF16)
    sum_right.start()
    base = mixed[rows_of(t.x)] + term[t.x].astype(F32)
    mixed[rows_of(t.x)] = base
    for one in (edge_right, edge_left, sum_left, sum_right):
        one.wait_recv()
    own[...] = (mixed[rows_of(t.x)] + edge_in[0].astype(F32) + edge_in[1].astype(F32)).astype(BF16)
    out_ref[t.me] = own[...]
    for one in (*copies, half_left, half_right, edge_right, edge_left, sum_left, sum_right):
        one.wait_send()
    gather(t, own, out_ref, cut, g_send, g_recv)


def tail(heads, tokens, gain, w_out, up, up_pair, down, down_pair, part):
    n_tensor, span, model = w_out.shape
    half = RING * part
    dma = lambda n: pltpu.SemaphoreType.DMA((n,))
    vmem = pl.BlockSpec(memory_space=pltpu.VMEM)
    hbm = pl.BlockSpec(memory_space=pltpu.HBM)
    return pl.pallas_call(
        tail_kernel,
        in_specs=[vmem, hbm, vmem, hbm, hbm, hbm, hbm, hbm],
        out_specs=vmem,
        out_shape=jax.ShapeDtypeStruct((n_tensor, part, model), BF16),
        scratch_shapes=[
            pltpu.VMEM((n_tensor, span, half), BF16),
            pltpu.VMEM(w_out.shape, BF16),
            pltpu.VMEM((2, *up.shape), BF16),
            pltpu.VMEM((2, *down.shape), BF16),
            pltpu.VMEM((half, model), BF16),
            pltpu.VMEM((half, model), F32),
            pltpu.VMEM((RING, part, model), BF16),
            pltpu.VMEM((part, model), BF16),
            pltpu.VMEM((2, part // 2, model), BF16),
            pltpu.VMEM((2, part, model), BF16),
            pltpu.VMEM((2, part // 2, model), BF16),
            dma(9), dma(9), dma(6), dma(6), dma(9), dma(9), dma(6),
        ],
        cost_estimate=pl.CostEstimate(flops=60 * 10**9, bytes_accessed=20 << 20, transcendentals=0),
        compiler_params=pltpu.CompilerParams(vmem_limit_bytes=48 << 20, collective_id=1, has_side_effects=True),
    )(heads, tokens, gain, w_out, up, up_pair, down, down_pair)


def per_device(n_seq, n_tensor, tokens, norm_gain, w_qkv, w_out, post_gain, w_up, w_down):
    rows, model = tokens.shape
    span = w_qkv.shape[2]
    heads = span // HD
    part = -(-rows // (16 * n_tensor)) * 16
    padded = n_tensor * part

    base = tokens.astype(F32)
    normed = layer_norm(base, norm_gain).astype(BF16)
    qkv = lax.dot_general(
        w_qkv.reshape(model, -1), normed, (((0,), (1,)), ((), ())), preferred_element_type=F32
    ).reshape(3, heads, HD, rows)
    query = (qkv[0] * (LOG2E / HD**0.5)).astype(BF16)
    kv = jnp.concatenate([qkv[1], qkv[2]], axis=1).astype(BF16)
    attended, w_out_all, up_pair, down_pair = attend(query, kv, w_out, w_up, w_down, padded, n_tensor)
    out = tail(
        attended.reshape(span, padded), tokens, post_gain.reshape(1, model), w_out_all,
        w_up, up_pair.reshape(w_up.shape), w_down, down_pair.reshape(w_down.shape), part,
    )
    return out.reshape(padded, model)[:rows]


def solution(mesh):
    placed = (
        P("seq", None),
        P(),
        P(None, None, "tensor"),
        P("tensor", None),
        P(),
        P(None, "tensor"),
        P("tensor", None),
    )
    body = functools.partial(per_device, mesh.shape["seq"], mesh.shape["tensor"])
    return jax.shard_map(
        body, mesh=mesh, in_specs=placed, out_specs=P("seq", None), check_vma=False
    )
```

```python
import functools
import jax
import jax.numpy as jnp
from jax import lax
from jax.experimental import pallas as pl
from jax.experimental.pallas import tpu as pltpu
from jax.sharding import PartitionSpec as P

HD = 48
LOG2E = 1.4426950408889634
MESH = pl.DeviceIdType.MESH
F32 = jnp.float32
BF16 = jnp.bfloat16
RING = 4
BLOCKS = 16
TILES = (slice(0, 256), slice(256, 512), slice(512, 720))


def layer_norm(values, gain):
    mean = jnp.mean(values, axis=-1, keepdims=True)
    centred = values - mean
    var = jnp.mean(centred * centred, axis=-1, keepdims=True)
    return centred * lax.rsqrt(var + 1e-05) * gain


def dot(a, b):
    return jnp.dot(a, b, preferred_element_type=F32)


def remote(src, dst, send, recv, seq):
    return pltpu.make_async_remote_copy(
        src_ref=src, dst_ref=dst, send_sem=send, recv_sem=recv, device_id={"seq": seq}, device_id_type=MESH
    )


def attend_kernel(
    tokens_hbm, gain_ref, w_qkv_hbm, w_hbm, up_ref, down_ref, out_ref, w_all, up_all, down_all,
    tokens, w_qkv, q_ref, kv_ref, w_ref, q_in, kv_in, key_rows, values, acc, peak, scores, obuf,
    q_send, q_recv, y_send, z_send, d_send, kv_recv, o_send, o_recv, w_send, w_recv, t_send, t_recv, w_own,
    f_send, f_recv, g_send, g_recv, h_send, h_recv, load_sem,
):
    rows = q_ref.shape[2]
    loads = (
        pltpu.make_async_copy(tokens_hbm, tokens, load_sem.at[0]),
        pltpu.make_async_copy(w_qkv_hbm, w_qkv, load_sem.at[1]),
    )
    for load in loads:
        load.start()
    me = lax.axis_index("seq")
    half, y, core = me // (2 * RING), (me // 2) % RING, me % 2

    def at(step):
        return half * (2 * RING) + lax.rem(y + step, RING) * 2 + core

    twin = me - core + (1 - core)
    far = lax.rem(me + 2 * RING, BLOCKS)
    peers = [at(1), at(2), at(3), twin, far]
    tensor = lax.axis_index("tensor")
    plane, x = tensor // RING, lax.rem(tensor, RING)

    def on(side, step):
        return side * RING + lax.rem(x + step, RING)

    friends = [on(plane, 1), on(plane, 2), on(plane, 3), on(1 - plane, 0)]
    barrier = pltpu.get_barrier_semaphore()
    for peer in peers:
        pl.semaphore_signal(barrier, inc=1, device_id={"seq": peer}, device_id_type=MESH)
    for friend in friends:
        pl.semaphore_signal(barrier, inc=1, device_id={"tensor": friend}, device_id_type=MESH)
    across = on(1 - plane, 0)
    pl.semaphore_signal(barrier, inc=1, device_id={"seq": far, "tensor": across}, device_id_type=MESH)
    w_load = pltpu.make_async_copy(w_hbm, w_ref, w_own.at[0])
    w_load.start()
    values[:, HD:, :] = jnp.ones((BLOCKS, values.shape[1] - HD, rows), BF16)
    acc[...] = jnp.zeros_like(acc)
    peak[...] = jnp.full_like(peak, -1e30)
    obuf[:, :, rows:] = jnp.zeros((RING, HD, obuf.shape[2] - rows), BF16)
    loads[0].wait()
    some = rows // 5

    def norm(i, carry):
        where = pl.ds(pl.multiple_of(i * some, some), some)
        tokens[where] = layer_norm(tokens[where].astype(F32), gain_ref[...]).astype(BF16)
        return carry

    lax.fori_loop(0, 5, norm, 0)
    loads[1].wait()
    for lanes in TILES:
        found = lax.dot_general(
            w_qkv[...], tokens[lanes], (((1,), (1,)), ((), ())), preferred_element_type=F32
        ).reshape(3, RING, HD, lanes.stop - lanes.start)
        q_ref[:, :, lanes] = (found[0] * (LOG2E / HD**0.5)).astype(BF16)
        kv_ref[:, :HD, lanes] = found[1].astype(BF16)
        kv_ref[:, HD:, lanes] = found[2].astype(BF16)
    pl.semaphore_wait(barrier, len(peers) + len(friends) + 1)

    pieces = 2 * RING
    both = ((up_ref, up_all), (down_ref, down_all))

    def piece(j, which):
        return lax.rem(y + (0, 2, 1, 3)[j], RING) * 2 + which

    def f_copy(k, j):
        ref, whole = both[k]
        size = ref.shape[0] // pieces
        number = piece(j, core)
        src = ref.at[pl.ds(pl.multiple_of(number * size, size), size)]
        device = {"tensor": across} if k == 0 else {"seq": far, "tensor": across}
        return pltpu.make_async_remote_copy(
            src_ref=src, dst_ref=whole.at[number], send_sem=f_send.at[2 * k + j], recv_sem=f_recv.at[2 * k + j],
            device_id=device, device_id_type=MESH,
        )

    def g_copy(k, step):
        whole = both[k][1]
        number = piece(0, core)
        i = 2 * k + step // 2
        j = 2 * k + 1 - step // 2
        return remote(whole.at[number], whole.at[number], g_send.at[i], g_recv.at[j], at(step))

    def h_copy(k, j, which):
        whole = both[k][1]
        number = piece(j, which)
        i = 4 * k + j
        return remote(whole.at[number], whole.at[number], h_send.at[i], h_recv.at[i], twin)

    cut = w_ref.shape[0] // 2
    rows_of = lambda which: pl.ds(pl.multiple_of(which * cut, cut), cut)

    def w_copy(src, owner, index, friend):
        return pltpu.make_async_remote_copy(
            src_ref=src, dst_ref=w_all.at[owner, rows_of(core)], send_sem=w_send.at[index], recv_sem=w_recv.at[index],
            device_id={"tensor": friend}, device_id_type=MESH,
        )

    def w_of(side, step, index, friend):
        owner = on(side, step)
        return w_copy(w_all.at[owner, rows_of(core)], owner, index, friend)

    def t_copy(index, which):
        owner = on(plane, index + 1) if index < 3 else on(1 - plane, index - 3)
        return remote(
            w_all.at[owner, rows_of(which)], w_all.at[owner, rows_of(which)], t_send.at[index], t_recv.at[index], twin
        )

    w_mine = w_ref.at[rows_of(core)]
    w_local = pltpu.make_async_copy(w_ref, w_all.at[tensor], w_own.at[1])

    def arrived(index):
        w_copy(w_mine, tensor, index, tensor).wait_recv()
        t_copy(index, core).start()

    def pass_on(c):
        @pl.when(c == 5)
        def _():
            for k in range(2):
                f_copy(k, 0).wait_recv()
                for step in (1, 3):
                    g_copy(k, step).start()
                h_copy(k, 0, core).start()

        @pl.when(c == 6)
        def _():
            arrived(3)
            for step in (1, 3, 2):
                w_copy(w_all.at[across, rows_of(core)], across, 3 + RING - step, on(plane, step)).start()

        @pl.when(c == 7)
        def _():
            for k in range(2):
                f_copy(k, 1).start()

        @pl.when(c == 11)
        def _():
            for index in (0, 2, 1):
                arrived(index)

    def q_copy(step):
        return remote(
            q_ref.at[lax.rem(y + step, RING)], q_in.at[RING - step], q_send.at[step], q_recv.at[RING - step], at(step)
        )

    def y_copy(step):
        slot = {1: 3, 2: 6, 3: 2}[step]
        return remote(
            kv_ref.at[lax.rem(y + step, RING)], kv_in.at[slot], y_send.at[step], kv_recv.at[slot], at(step)
        )

    def z_copy(src, slot):
        return remote(src, kv_in.at[slot], z_send.at[slot], kv_recv.at[slot], far)

    def d_copy(src, slot):
        return remote(src, kv_in.at[slot], d_send.at[slot], kv_recv.at[slot], twin)

    own = kv_ref.at[y]
    for step in (1, 3, 2):
        q_copy(step).start()
    d_copy(own, 1).start()
    for step in (1, 3, 2):
        y_copy(step).start()
    z_copy(own, 8).start()
    f_copy(0, 0).start()
    f_copy(1, 0).start()
    w_load.wait()
    w_local.start()
    w_copy(w_mine, tensor, 3, across).start()
    for step in (1, 3, 2):
        w_copy(w_mine, tensor, RING - step - 1, on(plane, step)).start()

    q_in[0] = q_ref[y]
    key_rows[0] = kv_ref[y, :HD].T
    values[0, :HD] = kv_ref[y, HD:]

    def arrive(c):
        d_copy(kv_in.at[c], c).wait_recv()

        @pl.when((c == 2) | (c == 3))
        def _():
            d_copy(kv_in.at[c], c + 2).start()
            z_copy(kv_in.at[c], 2 * c + 6).start()

        @pl.when(c == 6)
        def _():
            d_copy(kv_in.at[c], c + 1).start()
            z_copy(kv_in.at[c], 14).start()

        @pl.when((c >= 8) & (lax.rem(c, 2) == 0))
        def _():
            d_copy(kv_in.at[c], c + 1).start()

        pass_on(c)

    def prepare(c):
        key_rows[c] = kv_in[c, :HD].T
        values[c, :HD] = kv_in[c, HD:]

    def score(c, s, b):
        for lanes in TILES:
            found = dot(key_rows[c], q_in[s, :, lanes])
            scores[b, :rows, lanes] = found
            scores[b, rows : rows + 1, lanes] = jnp.max(found, axis=0, keepdims=True)

    def weigh(c, s, b):
        for lanes in TILES:
            old = peak[s, :, lanes]
            new = jnp.maximum(old, scores[b, rows : rows + 1, lanes])
            peak[s, :, lanes] = new
            weights = jnp.exp2(scores[b, :rows, lanes] - new).astype(BF16)
            acc[s, :, lanes] = acc[s, :, lanes] * jnp.exp2(old - new) + dot(values[c], weights)

    def o_copy(step):
        return remote(obuf.at[step], out_ref.at[y], o_send.at[step], o_recv.at[RING - step], at(step))

    opening = [(c, s) for s in (0, 1, 3, 2) for c in (0, 1)]
    last = 12
    order = (3, 0, 1, 2)
    score(0, 0, 0)
    for i, (c, s) in enumerate(opening):
        if i == 0:
            arrive(jnp.int32(1))
            prepare(1)
        elif i == len(opening) - 1:
            arrive(jnp.int32(2))
            prepare(2)
        after = opening[i + 1] if i + 1 < len(opening) else (2, order[0])
        if i in (1, 3, 5):
            q_copy(RING - after[1]).wait_recv()
        score(*after, (i + 1) % 2)
        weigh(c, s, i % 2)

    def body(c, carry):
        arrive(c + 1)

        @pl.when(c == last - 1)
        def _():
            arrive(jnp.int32(14))

        for i, s in enumerate(order):
            if i < 3:
                score(c, order[i + 1], 1 - i % 2)
            else:
                score(c + 1, order[0], 0)
            if i == 2:
                prepare(c + 1)
            weigh(c, s, i % 2)
        return carry

    lax.fori_loop(2, last, body, 0)

    arrive(jnp.int32(13))
    arrive(jnp.int32(15))
    for k in range(2):
        for step in (1, 3):
            g_copy(k, step).wait_recv()
        for j in (2, 3):
            h_copy(k, j, core).start()
    for c in range(last + 1, BLOCKS):
        prepare(c)

    def close(i, carry):
        s = RING - 1 - i
        for k in range(RING):
            if k < RING - 1:
                score(last + k + 1, s, 1 - k % 2)
            else:
                score(last, jnp.maximum(s - 1, 0), 0)
            weigh(last + k, s, k % 2)
        result = (acc[s, :HD] / acc[s, HD : HD + 1]).astype(BF16)

        @pl.when(s > 0)
        def _():
            obuf[s, :, :rows] = result
            o_copy(s).start()

        @pl.when(s == 0)
        def _():
            out_ref[y, :, :rows] = result

        @pl.when(s == 1)
        def _():
            for k in range(2):
                f_copy(k, 1).wait_recv()
                h_copy(k, 1, core).start()
            for index in (4, 6, 5):
                arrived(index)

        return carry

    lax.fori_loop(0, RING, close, 0)
    out_ref[y, :, rows:] = jnp.zeros((HD, out_ref.shape[2] - rows), BF16)

    def o_wait(step):
        return remote(
            obuf.at[step], out_ref.at[lax.rem(y + step, RING)], o_send.at[step], o_recv.at[step], at(step)
        )

    for step in (1, 2, 3):
        q_copy(step).wait_send()
        y_copy(step).wait_send()
        o_copy(step).wait_send()
    for slot in (8, 10, 12, 14):
        z_copy(own, slot).wait_send()
    for slot in (1, 4, 5, 7, 9, 11, 13, 15):
        d_copy(own, slot).wait_send()
    for index in range(7):
        w_copy(w_mine, tensor, index, tensor).wait_send()
        t_copy(index, core).wait_send()
        t_copy(index, 1 - core).wait_recv()
    w_local.wait()
    for k in range(2):
        for j in range(2):
            f_copy(k, j).wait_send()
        for step in (1, 3):
            g_copy(k, step).wait_send()
        for j in range(4):
            h_copy(k, j, core).wait_send()
            h_copy(k, j, 1 - core).wait_recv()
    for step in (1, 3, 2):
        o_wait(step).wait_recv()


def attend(tokens, gain, w_qkv, w_out, w_up, w_down, padded, n_tensor):
    rows = tokens.shape[0]
    heads, width = RING, HD
    dma = lambda n: pltpu.SemaphoreType.DMA((n,))
    vmem = pl.BlockSpec(memory_space=pltpu.VMEM)
    hbm = pl.BlockSpec(memory_space=pltpu.HBM)
    return pl.pallas_call(
        attend_kernel,
        in_specs=[hbm, vmem, hbm, hbm, hbm, hbm],
        out_specs=[vmem, hbm, hbm, hbm],
        out_shape=[
            jax.ShapeDtypeStruct((heads, width, padded), BF16),
            jax.ShapeDtypeStruct((n_tensor, *w_out.shape), BF16),
            *(jax.ShapeDtypeStruct((2 * RING, w.shape[0] // (2 * RING), w.shape[1]), BF16) for w in (w_up, w_down)),
        ],
        scratch_shapes=[
            pltpu.VMEM(tokens.shape, BF16),
            pltpu.VMEM(w_qkv.shape, BF16),
            pltpu.VMEM((heads, width, rows), BF16),
            pltpu.VMEM((heads, 2 * width, rows), BF16),
            pltpu.VMEM(w_out.shape, BF16),
            pltpu.VMEM((heads, width, rows), BF16),
            pltpu.VMEM((BLOCKS, 2 * width, rows), BF16),
            pltpu.VMEM((BLOCKS, rows, width), BF16),
            pltpu.VMEM((BLOCKS, width + 16, rows), BF16),
            pltpu.VMEM((heads, width + 16, rows), F32),
            pltpu.VMEM((heads, 1, rows), F32),
            pltpu.VMEM((2, rows + 8, rows), F32),
            pltpu.VMEM((heads, width, padded), BF16),
            dma(RING), dma(RING), dma(RING), dma(BLOCKS), dma(BLOCKS), dma(BLOCKS), dma(RING), dma(RING),
            dma(7), dma(7), dma(7), dma(7), dma(2),
            dma(4), dma(4), dma(4), dma(4), dma(8), dma(8), dma(2),
        ],
        cost_estimate=pl.CostEstimate(flops=40 * 10**9, bytes_accessed=8 << 20, transcendentals=0),
        compiler_params=pltpu.CompilerParams(
            vmem_limit_bytes=62 << 20, collective_id=0, has_side_effects=True
        ),
    )(tokens, gain, w_qkv, w_out, w_up, w_down)


class Tensor:
    def __init__(self):
        self.me = lax.axis_index("tensor")
        self.plane, self.x = self.me // RING, lax.rem(self.me, RING)
        self.right, self.left = self.on(self.plane, 1), self.on(self.plane, 3)
        self.pair = self.on(1 - self.plane, 0)

    def on(self, side, step):
        return side * RING + lax.rem(self.x + step, RING)

    def meet(self):
        barrier = pltpu.get_barrier_semaphore()
        for friend in (self.right, self.left, self.pair):
            pl.semaphore_signal(barrier, inc=1, device_id={"tensor": friend}, device_id_type=MESH)
        pl.semaphore_wait(barrier, 3)


def send(src, dst, send_sem, recv_sem, friend):
    return pltpu.make_async_remote_copy(
        src_ref=src, dst_ref=dst, send_sem=send_sem, recv_sem=recv_sem,
        device_id={"tensor": friend}, device_id_type=MESH,
    )


def gather(t, mine, buf, cut, send_sem, recv_sem):
    lo, hi = pl.ds(0, cut), pl.ds(cut, cut)
    copies = {
        "right": (mine, t.me, None, t.right, 0),
        "left": (mine, t.me, None, t.left, 1),
        "pair": (mine, t.me, None, t.pair, 2),
        "far lo": (None, t.left, lo, t.right, 3),
        "far hi": (None, t.right, hi, t.left, 4),
        "over right": (None, t.pair, None, t.right, 5),
        "over left": (None, t.pair, None, t.left, 6),
        "pair lo": (None, t.on(t.plane, 2), lo, t.pair, 7),
        "pair hi": (None, t.on(t.plane, 2), hi, t.pair, 8),
    }

    def copy(name):
        src, block, part, to, i = copies[name]
        dst = buf.at[block] if part is None else buf.at[block, part]
        return send(dst if src is None else src, dst, send_sem.at[i], recv_sem.at[i], to)

    for name in ("right", "left", "pair"):
        copy(name).start()
    copy("right").wait_recv()
    copy("far lo").start()
    copy("left").wait_recv()
    copy("far hi").start()
    copy("pair").wait_recv()
    copy("over right").start()
    copy("over left").start()
    copy("far lo").wait_recv()
    copy("pair lo").start()
    copy("far hi").wait_recv()
    copy("pair hi").start()
    for name in ("over right", "over left", "pair lo", "pair hi"):
        copy(name).wait_recv()
    for name in copies:
        copy(name).wait_send()


def tail_kernel(
    heads_ref, tokens_hbm, gain_ref, w_hbm, up_hbm, up_pair_hbm, down_hbm, down_pair_hbm, out_ref,
    heads, w_out, up, down, tokens, mixed, term, own, half_in, edge_in, edge_sum,
    a_send, a_recv, s_send, s_recv, g_send, g_recv, load_sem,
):
    t = Tensor()
    half, model = mixed.shape
    part = half // RING
    there = 1 - t.plane
    valid = tokens_hbm.shape[0] - half
    loads = [
        pltpu.make_async_copy(w_hbm, w_out, load_sem.at[0]),
        pltpu.make_async_copy(up_hbm, up.at[0], load_sem.at[1]),
        pltpu.make_async_copy(up_pair_hbm, up.at[1], load_sem.at[2]),
        pltpu.make_async_copy(down_hbm, down.at[0], load_sem.at[3]),
        pltpu.make_async_copy(down_pair_hbm, down.at[1], load_sem.at[4]),
    ]
    first = pltpu.make_async_copy(tokens_hbm.at[pl.ds(0, half)], tokens, load_sem.at[5])
    second = pltpu.make_async_copy(tokens_hbm.at[pl.ds(half, valid)], tokens.at[pl.ds(0, valid)], load_sem.at[5])

    @pl.when(t.plane == 0)
    def _():
        first.start()

    @pl.when(t.plane == 1)
    def _():
        second.start()
        tokens[valid:] = jnp.zeros((half - valid, model), BF16)

    for load in loads:
        load.start()
    t.meet()

    cut = heads_ref.shape[0] // 2
    lo, hi = pl.ds(0, cut), pl.ds(cut, cut)
    lanes = lambda plane: pl.ds(pl.multiple_of(plane * half, half), half)

    def copy(src, block, rows, to, i):
        dst = heads.at[block] if rows is None else heads.at[block, rows]
        return send(dst if src is None else src, dst, a_send.at[i], a_recv.at[i], to)

    mine, theirs = heads_ref.at[:, lanes(t.plane)], heads_ref.at[:, lanes(there)]
    copies = [
        copy(mine, t.me, None, t.right, 0),
        copy(mine, t.me, None, t.left, 1),
        copy(theirs, t.me, None, t.pair, 2),
        copy(None, t.left, lo, t.right, 3),
        copy(None, t.right, hi, t.left, 4),
        copy(None, t.pair, None, t.right, 5),
        copy(None, t.pair, None, t.left, 6),
        copy(None, t.on(there, 3), lo, t.right, 7),
        copy(None, t.on(there, 1), hi, t.left, 8),
    ]
    for i in (2, 0, 1):
        copies[i].start()
    heads[t.me] = heads_ref[:, lanes(t.plane)]

    @pl.when(t.plane == 0)
    def _():
        first.wait()

    @pl.when(t.plane == 1)
    def _():
        second.wait()

    mixed[...] = tokens[...].astype(F32)
    loads[0].wait()

    def group(i, carry):
        for when, waits, starts in (
            (1, (2,), (5, 6)),
            (2, (0,), (3,)),
            (3, (1, 5), (4, 7)),
            (4, (6,), (8,)),
            (6, (3, 4), ()),
            (7, (7, 8), ()),
        ):
            @pl.when(i == when)
            def _():
                for one in waits:
                    copies[one].wait_recv()
                for one in starts:
                    copies[one].start()

        step = lax.rem(3 * (i // 2) * (i // 2 + 1) // 2, RING)
        side = lax.rem(t.plane + i, 2)
        who = side * RING + lax.rem(t.x + step, RING)
        mixed[...] += lax.dot_general(
            heads[who], w_out[who], (((0,), (0,)), ((), ())), preferred_element_type=F32
        )
        return carry

    lax.fori_loop(0, 2 * RING, group, 0)
    for load in loads[1:]:
        load.wait()

    cut = part // 2
    lo, hi = pl.ds(0, cut), pl.ds(cut, cut)
    right, left, far = (lax.rem(t.x + step, RING) for step in (1, 3, 2))

    def sums(src, dst, i, to):
        return send(src, dst, s_send.at[i], s_recv.at[i], to)

    half_left = sums(term.at[far, lo], half_in.at[0], 0, t.left)
    half_right = sums(term.at[far, hi], half_in.at[1], 1, t.right)
    edge_right = sums(term.at[right, lo], edge_in.at[0, lo], 2, t.right)
    edge_left = sums(term.at[left, hi], edge_in.at[1, hi], 3, t.left)
    sum_left = sums(edge_sum.at[0], edge_in.at[1, lo], 4, t.left)
    sum_right = sums(edge_sum.at[1], edge_in.at[0, hi], 5, t.right)
    rows_of = lambda b: pl.ds(pl.multiple_of(b * part, part), part)

    def feed(i, carry):
        b = lax.rem(t.x + 2 + 3 * i * (i + 1) // 2, RING)
        post = layer_norm(mixed[rows_of(b)], gain_ref[...]).astype(BF16)
        wide = lambda k: jax.nn.gelu(dot(post, up[k]), approximate=True).astype(BF16)
        term[b] = (dot(wide(0), down[0]) + dot(wide(1), down[1])).astype(BF16)
        for when, starts in ((0, (half_left, half_right)), (1, (edge_right,)), (2, (edge_left,))):
            @pl.when(i == when)
            def _():
                for one in starts:
                    one.start()
        return carry

    lax.fori_loop(0, RING, feed, 0)
    half_left.wait_recv()
    edge_sum[0] = (half_in[0].astype(F32) + term[left, lo].astype(F32)).astype(BF16)
    sum_left.start()
    half_right.wait_recv()
    edge_sum[1] = (half_in[1].astype(F32) + term[right, hi].astype(F32)).astype(BF16)
    sum_right.start()
    base = mixed[rows_of(t.x)] + term[t.x].astype(F32)
    mixed[rows_of(t.x)] = base
    for one in (edge_right, edge_left, sum_left, sum_right):
        one.wait_recv()
    own[...] = (mixed[rows_of(t.x)] + edge_in[0].astype(F32) + edge_in[1].astype(F32)).astype(BF16)
    out_ref[t.me] = own[...]
    for one in (*copies, half_left, half_right, edge_right, edge_left, sum_left, sum_right):
        one.wait_send()
    gather(t, own, out_ref, cut, g_send, g_recv)


def tail(heads, tokens, gain, w_out, up, up_pair, down, down_pair, part):
    n_tensor, span, model = w_out.shape
    half = RING * part
    dma = lambda n: pltpu.SemaphoreType.DMA((n,))
    vmem = pl.BlockSpec(memory_space=pltpu.VMEM)
    hbm = pl.BlockSpec(memory_space=pltpu.HBM)
    return pl.pallas_call(
        tail_kernel,
        in_specs=[vmem, hbm, vmem, hbm, hbm, hbm, hbm, hbm],
        out_specs=vmem,
        out_shape=jax.ShapeDtypeStruct((n_tensor, part, model), BF16),
        scratch_shapes=[
            pltpu.VMEM((n_tensor, span, half), BF16),
            pltpu.VMEM(w_out.shape, BF16),
            pltpu.VMEM((2, *up.shape), BF16),
            pltpu.VMEM((2, *down.shape), BF16),
            pltpu.VMEM((half, model), BF16),
            pltpu.VMEM((half, model), F32),
            pltpu.VMEM((RING, part, model), BF16),
            pltpu.VMEM((part, model), BF16),
            pltpu.VMEM((2, part // 2, model), BF16),
            pltpu.VMEM((2, part, model), BF16),
            pltpu.VMEM((2, part // 2, model), BF16),
            dma(9), dma(9), dma(6), dma(6), dma(9), dma(9), dma(6),
        ],
        cost_estimate=pl.CostEstimate(flops=60 * 10**9, bytes_accessed=20 << 20, transcendentals=0),
        compiler_params=pltpu.CompilerParams(vmem_limit_bytes=62 << 20, collective_id=1, has_side_effects=True),
    )(heads, tokens, gain, w_out, up, up_pair, down, down_pair)


def per_device(n_seq, n_tensor, tokens, norm_gain, w_qkv, w_out, post_gain, w_up, w_down):
    rows, model = tokens.shape
    span = w_qkv.shape[2]
    part = -(-rows // (16 * n_tensor)) * 16
    padded = n_tensor * part

    attended, w_out_all, up_pair, down_pair = attend(
        tokens, norm_gain.reshape(1, model), w_qkv.transpose(1, 2, 0).reshape(3 * span, model),
        w_out, w_up, w_down, padded, n_tensor,
    )
    out = tail(
        attended.reshape(span, padded), tokens, post_gain.reshape(1, model), w_out_all,
        w_up, up_pair.reshape(w_up.shape), w_down, down_pair.reshape(w_down.shape), part,
    )
    return out.reshape(padded, model)[:rows]


def solution(mesh):
    placed = (
        P("seq", None),
        P(),
        P(None, None, "tensor"),
        P("tensor", None),
        P(),
        P(None, "tensor"),
        P("tensor", None),
    )
    body = functools.partial(per_device, mesh.shape["seq"], mesh.shape["tensor"])
    return jax.shard_map(
        body, mesh=mesh, in_specs=placed, out_specs=P("seq", None), check_vma=False
    )
```

```python
import functools
import jax
import jax.numpy as jnp
from jax import lax
from jax.experimental import pallas as pl
from jax.experimental.pallas import tpu as pltpu
from jax.sharding import PartitionSpec as P

HD = 48
LOG2E = 1.4426950408889634
MESH = pl.DeviceIdType.MESH
F32 = jnp.float32
BF16 = jnp.bfloat16
RING = 4
GRANT = 61 << 20
BLOCKS = 16
TILES = (slice(0, 256), slice(256, 512), slice(512, 720))


def layer_norm(values, gain):
    mean = jnp.mean(values, axis=-1, keepdims=True)
    centred = values - mean
    var = jnp.mean(centred * centred, axis=-1, keepdims=True)
    return centred * lax.rsqrt(var + 1e-05) * gain


def dot(a, b):
    return jnp.dot(a, b, preferred_element_type=F32)


def remote(src, dst, send, recv, seq):
    return pltpu.make_async_remote_copy(
        src_ref=src, dst_ref=dst, send_sem=send, recv_sem=recv, device_id={"seq": seq}, device_id_type=MESH
    )


def attend_kernel(
    tokens_hbm, gain_ref, w_qkv_hbm, w_hbm, post_gain_ref, up_hbm, down_hbm, out_ref,
    heads_ref, w_all, up, down, tokens, w_qkv, q_ref, kv_ref, q_in, kv_in, key_rows, values, acc, peak, scores, obuf,
    q_send, q_recv, y_send, z_send, d_send, kv_recv, o_send, o_recv, w_send, w_recv, t_send, t_recv, w_own,
    f_send, f_recv, g_send, g_recv, h_send, h_recv, load_sem, *tail_scratch,
):
    rows = q_ref.shape[2]
    loads = (
        pltpu.make_async_copy(tokens_hbm, tokens, load_sem.at[0]),
        pltpu.make_async_copy(w_qkv_hbm, w_qkv, load_sem.at[1]),
    )
    for load in loads:
        load.start()
    me = lax.axis_index("seq")
    half, y, core = me // (2 * RING), (me // 2) % RING, me % 2

    def at(step):
        return half * (2 * RING) + lax.rem(y + step, RING) * 2 + core

    twin = me - core + (1 - core)
    far = lax.rem(me + 2 * RING, BLOCKS)
    peers = [at(1), at(2), at(3), twin, far]
    tensor = lax.axis_index("tensor")
    plane, x = tensor // RING, lax.rem(tensor, RING)

    def on(side, step):
        return side * RING + lax.rem(x + step, RING)

    friends = [on(plane, 1), on(plane, 2), on(plane, 3), on(1 - plane, 0)]
    barrier = pltpu.get_barrier_semaphore()
    for peer in peers:
        pl.semaphore_signal(barrier, inc=1, device_id={"seq": peer}, device_id_type=MESH)
    for friend in friends:
        pl.semaphore_signal(barrier, inc=1, device_id={"tensor": friend}, device_id_type=MESH)
    across = on(1 - plane, 0)
    pl.semaphore_signal(barrier, inc=1, device_id={"seq": far, "tensor": across}, device_id_type=MESH)
    w_load = pltpu.make_async_copy(w_hbm, w_all.at[tensor], w_own.at[0])
    w_load.start()
    values[:, HD:, :] = jnp.ones((BLOCKS, values.shape[1] - HD, rows), BF16)
    acc[...] = jnp.zeros_like(acc)
    peak[...] = jnp.full_like(peak, -1e30)
    obuf[:, :, rows:] = jnp.zeros((RING, HD, obuf.shape[2] - rows), BF16)
    loads[0].wait()
    some = rows // 5

    def norm(i, carry):
        where = pl.ds(pl.multiple_of(i * some, some), some)
        tokens[where] = layer_norm(tokens[where].astype(F32), gain_ref[...].reshape(1, -1)).astype(BF16)
        return carry

    lax.fori_loop(0, 5, norm, 0)
    loads[1].wait()
    for lanes in TILES:
        found = lax.dot_general(
            w_qkv[...], tokens[lanes], (((1,), (1,)), ((), ())), preferred_element_type=F32
        ).reshape(3, RING, HD, lanes.stop - lanes.start)
        q_ref[:, :, lanes] = (found[0] * (LOG2E / HD**0.5)).astype(BF16)
        kv_ref[:, :HD, lanes] = found[1].astype(BF16)
        kv_ref[:, HD:, lanes] = found[2].astype(BF16)
    pl.semaphore_wait(barrier, len(peers) + len(friends) + 1)

    pieces = 2 * RING
    both = ((up_hbm, up), (down_hbm, down))

    def spot(k, number):
        size = both[k][0].shape[0] // pieces
        return both[k][1].at[1, pl.ds(pl.multiple_of(number * size, size), size)]

    def piece(j, which):
        return lax.rem(y + (0, 2, 1, 3)[j], RING) * 2 + which

    def f_copy(k, j):
        ref = both[k][0]
        size = ref.shape[0] // pieces
        number = piece(j, core)
        src = ref.at[pl.ds(pl.multiple_of(number * size, size), size)]
        device = {"tensor": across} if k == 0 else {"seq": far, "tensor": across}
        return pltpu.make_async_remote_copy(
            src_ref=src, dst_ref=spot(k, number), send_sem=f_send.at[2 * k + j], recv_sem=f_recv.at[2 * k + j],
            device_id=device, device_id_type=MESH,
        )

    def g_copy(k, step):
        number = piece(0, core)
        i = 2 * k + step // 2
        j = 2 * k + 1 - step // 2
        return remote(spot(k, number), spot(k, number), g_send.at[i], g_recv.at[j], at(step))

    def h_copy(k, j, which):
        number = piece(j, which)
        i = 4 * k + j
        return remote(spot(k, number), spot(k, number), h_send.at[i], h_recv.at[i], twin)

    cut = w_hbm.shape[0] // 2
    rows_of = lambda which: pl.ds(pl.multiple_of(which * cut, cut), cut)

    def w_copy(src, owner, index, friend):
        return pltpu.make_async_remote_copy(
            src_ref=src, dst_ref=w_all.at[owner, rows_of(core)], send_sem=w_send.at[index], recv_sem=w_recv.at[index],
            device_id={"tensor": friend}, device_id_type=MESH,
        )

    def w_of(side, step, index, friend):
        owner = on(side, step)
        return w_copy(w_all.at[owner, rows_of(core)], owner, index, friend)

    def t_copy(index, which):
        owner = on(plane, index + 1) if index < 3 else on(1 - plane, index - 3)
        return remote(
            w_all.at[owner, rows_of(which)], w_all.at[owner, rows_of(which)], t_send.at[index], t_recv.at[index], twin
        )

    w_mine = w_all.at[tensor, rows_of(core)]

    def arrived(index):
        w_copy(w_mine, tensor, index, tensor).wait_recv()
        t_copy(index, core).start()

    def pass_on(c):
        @pl.when(c == 5)
        def _():
            for k in range(2):
                f_copy(k, 0).wait_recv()
                for step in (1, 3):
                    g_copy(k, step).start()
                h_copy(k, 0, core).start()

        @pl.when(c == 6)
        def _():
            arrived(3)
            for step in (1, 3, 2):
                w_copy(w_all.at[across, rows_of(core)], across, 3 + RING - step, on(plane, step)).start()

        @pl.when(c == 7)
        def _():
            for k in range(2):
                f_copy(k, 1).start()

        @pl.when(c == 11)
        def _():
            for index in (0, 2, 1):
                arrived(index)

    def q_copy(step):
        return remote(
            q_ref.at[lax.rem(y + step, RING)], q_in.at[RING - step], q_send.at[step], q_recv.at[RING - step], at(step)
        )

    def y_copy(step):
        slot = {1: 3, 2: 6, 3: 2}[step]
        return remote(
            kv_ref.at[lax.rem(y + step, RING)], kv_in.at[slot], y_send.at[step], kv_recv.at[slot], at(step)
        )

    def z_copy(src, slot):
        return remote(src, kv_in.at[slot], z_send.at[slot], kv_recv.at[slot], far)

    def d_copy(src, slot):
        return remote(src, kv_in.at[slot], d_send.at[slot], kv_recv.at[slot], twin)

    own = kv_ref.at[y]
    for step in (1, 3, 2):
        q_copy(step).start()
    d_copy(own, 1).start()
    for step in (1, 3, 2):
        y_copy(step).start()
    z_copy(own, 8).start()
    f_copy(0, 0).start()
    f_copy(1, 0).start()
    w_load.wait()
    w_copy(w_mine, tensor, 3, across).start()
    for step in (1, 3, 2):
        w_copy(w_mine, tensor, RING - step - 1, on(plane, step)).start()

    q_in[0] = q_ref[y]
    key_rows[0] = kv_ref[y, :HD].T
    values[0, :HD] = kv_ref[y, HD:]

    def arrive(c):
        d_copy(kv_in.at[c], c).wait_recv()

        @pl.when((c == 2) | (c == 3))
        def _():
            d_copy(kv_in.at[c], c + 2).start()
            z_copy(kv_in.at[c], 2 * c + 6).start()

        @pl.when(c == 6)
        def _():
            d_copy(kv_in.at[c], c + 1).start()
            z_copy(kv_in.at[c], 14).start()

        @pl.when((c >= 8) & (lax.rem(c, 2) == 0))
        def _():
            d_copy(kv_in.at[c], c + 1).start()

        pass_on(c)

    def prepare(c):
        key_rows[c] = kv_in[c, :HD].T
        values[c, :HD] = kv_in[c, HD:]

    def score(c, s, b):
        for lanes in TILES:
            found = dot(key_rows[c], q_in[s, :, lanes])
            scores[b, :rows, lanes] = found
            scores[b, rows : rows + 1, lanes] = jnp.max(found, axis=0, keepdims=True)

    def weigh(c, s, b):
        for lanes in TILES:
            old = peak[s, :, lanes]
            new = jnp.maximum(old, scores[b, rows : rows + 1, lanes])
            peak[s, :, lanes] = new
            weights = jnp.exp2(scores[b, :rows, lanes] - new).astype(BF16)
            acc[s, :, lanes] = acc[s, :, lanes] * jnp.exp2(old - new) + dot(values[c], weights)

    head = lambda which: pl.ds(pl.multiple_of(which * HD, HD), HD)

    def o_copy(step):
        return remote(obuf.at[step], heads_ref.at[head(y)], o_send.at[step], o_recv.at[RING - step], at(step))

    opening = [(c, s) for s in (0, 1, 3, 2) for c in (0, 1)]
    last = 12
    order = (3, 0, 1, 2)
    score(0, 0, 0)
    for i, (c, s) in enumerate(opening):
        if i == 0:
            arrive(jnp.int32(1))
            prepare(1)
        elif i == len(opening) - 1:
            arrive(jnp.int32(2))
            prepare(2)
        after = opening[i + 1] if i + 1 < len(opening) else (2, order[0])
        if i in (1, 3, 5):
            q_copy(RING - after[1]).wait_recv()
        score(*after, (i + 1) % 2)
        weigh(c, s, i % 2)

    def body(c, carry):
        arrive(c + 1)

        @pl.when(c == last - 1)
        def _():
            arrive(jnp.int32(14))

        for i, s in enumerate(order):
            if i < 3:
                score(c, order[i + 1], 1 - i % 2)
            else:
                score(c + 1, order[0], 0)
            if i == 2:
                prepare(c + 1)
            weigh(c, s, i % 2)
        return carry

    lax.fori_loop(2, last, body, 0)

    arrive(jnp.int32(13))
    arrive(jnp.int32(15))
    for k in range(2):
        for step in (1, 3):
            g_copy(k, step).wait_recv()
        for j in (2, 3):
            h_copy(k, j, core).start()
    for c in range(last + 1, BLOCKS):
        prepare(c)

    def close(i, carry):
        s = RING - 1 - i
        for k in range(RING):
            if k < RING - 1:
                score(last + k + 1, s, 1 - k % 2)
            else:
                score(last, jnp.maximum(s - 1, 0), 0)
            weigh(last + k, s, k % 2)
        result = (acc[s, :HD] / acc[s, HD : HD + 1]).astype(BF16)

        @pl.when(s > 0)
        def _():
            obuf[s, :, :rows] = result
            o_copy(s).start()

        @pl.when(s == 0)
        def _():
            heads_ref[head(y), :rows] = result

        @pl.when(s == 1)
        def _():
            for k in range(2):
                f_copy(k, 1).wait_recv()
                h_copy(k, 1, core).start()
            for index in (4, 6, 5):
                arrived(index)

        return carry

    lax.fori_loop(0, RING, close, 0)
    heads_ref[head(y), rows:] = jnp.zeros((HD, heads_ref.shape[1] - rows), BF16)

    def o_wait(step):
        return remote(
            obuf.at[step], heads_ref.at[head(lax.rem(y + step, RING))], o_send.at[step], o_recv.at[step], at(step)
        )

    for step in (1, 2, 3):
        q_copy(step).wait_send()
        y_copy(step).wait_send()
        o_copy(step).wait_send()
    for slot in (8, 10, 12, 14):
        z_copy(own, slot).wait_send()
    for slot in (1, 4, 5, 7, 9, 11, 13, 15):
        d_copy(own, slot).wait_send()
    for step in (1, 3, 2):
        o_wait(step).wait_recv()

    def weights_out():
        for index in range(7):
            t_copy(index, 1 - core).wait_recv()

    def weights_in():
        for k in range(2):
            for j in range(4):
                h_copy(k, j, 1 - core).wait_recv()

    tail_kernel(
        heads_ref, tokens_hbm, post_gain_ref, up_hbm, down_hbm, out_ref, w_all, up, down,
        weights_out, weights_in, *tail_scratch,
    )
    for index in range(7):
        w_copy(w_mine, tensor, index, tensor).wait_send()
        t_copy(index, core).wait_send()
    for k in range(2):
        for j in range(2):
            f_copy(k, j).wait_send()
        for step in (1, 3):
            g_copy(k, step).wait_send()
        for j in range(4):
            h_copy(k, j, core).wait_send()


class Tensor:
    def __init__(self):
        self.me = lax.axis_index("tensor")
        self.plane, self.x = self.me // RING, lax.rem(self.me, RING)
        self.right, self.left = self.on(self.plane, 1), self.on(self.plane, 3)
        self.pair = self.on(1 - self.plane, 0)

    def on(self, side, step):
        return side * RING + lax.rem(self.x + step, RING)

    def meet(self):
        barrier = pltpu.get_barrier_semaphore()
        for friend in (self.right, self.left, self.pair):
            pl.semaphore_signal(barrier, inc=1, device_id={"tensor": friend}, device_id_type=MESH)
        pl.semaphore_wait(barrier, 3)


def send(src, dst, send_sem, recv_sem, friend):
    return pltpu.make_async_remote_copy(
        src_ref=src, dst_ref=dst, send_sem=send_sem, recv_sem=recv_sem,
        device_id={"tensor": friend}, device_id_type=MESH,
    )


def gather(t, mine, buf, cut, send_sem, recv_sem):
    lo, hi = pl.ds(0, cut), pl.ds(cut, cut)
    copies = {
        "right": (mine, t.me, None, t.right, 0),
        "left": (mine, t.me, None, t.left, 1),
        "pair": (mine, t.me, None, t.pair, 2),
        "far lo": (None, t.left, lo, t.right, 3),
        "far hi": (None, t.right, hi, t.left, 4),
        "over right": (None, t.pair, None, t.right, 5),
        "over left": (None, t.pair, None, t.left, 6),
        "pair lo": (None, t.on(t.plane, 2), lo, t.pair, 7),
        "pair hi": (None, t.on(t.plane, 2), hi, t.pair, 8),
    }

    def copy(name):
        src, block, part, to, i = copies[name]
        dst = buf.at[block] if part is None else buf.at[block, part]
        return send(dst if src is None else src, dst, send_sem.at[i], recv_sem.at[i], to)

    for name in ("right", "left", "pair"):
        copy(name).start()
    copy("right").wait_recv()
    copy("far lo").start()
    copy("left").wait_recv()
    copy("far hi").start()
    copy("pair").wait_recv()
    copy("over right").start()
    copy("over left").start()
    copy("far lo").wait_recv()
    copy("pair lo").start()
    copy("far hi").wait_recv()
    copy("pair hi").start()
    for name in ("over right", "over left", "pair lo", "pair hi"):
        copy(name).wait_recv()
    for name in copies:
        copy(name).wait_send()


def tail_kernel(
    heads_ref, tokens_hbm, gain_ref, up_hbm, down_hbm, out_ref, w_out, up, down, weights_out, weights_in,
    heads, tokens, mixed, term, own, half_in, edge_in, edge_sum,
    a_send, a_recv, s_send, s_recv, g_send, g_recv, load_sem,
):
    t = Tensor()
    half, model = mixed.shape
    part = half // RING
    there = 1 - t.plane
    valid = tokens_hbm.shape[0] - half
    loads = [
        pltpu.make_async_copy(up_hbm, up.at[0], load_sem.at[0]),
        pltpu.make_async_copy(down_hbm, down.at[0], load_sem.at[1]),
    ]
    first = pltpu.make_async_copy(tokens_hbm.at[pl.ds(0, half)], tokens, load_sem.at[2])
    second = pltpu.make_async_copy(tokens_hbm.at[pl.ds(half, valid)], tokens.at[pl.ds(0, valid)], load_sem.at[2])

    @pl.when(t.plane == 0)
    def _():
        first.start()

    @pl.when(t.plane == 1)
    def _():
        second.start()
        tokens[valid:] = jnp.zeros((half - valid, model), BF16)

    for load in loads:
        load.start()

    cut = heads_ref.shape[0] // 2
    lo, hi = pl.ds(0, cut), pl.ds(cut, cut)
    lanes = lambda plane: pl.ds(pl.multiple_of(plane * half, half), half)

    def copy(src, block, rows, to, i):
        dst = heads.at[block] if rows is None else heads.at[block, rows]
        return send(dst if src is None else src, dst, a_send.at[i], a_recv.at[i], to)

    mine, theirs = heads_ref.at[:, lanes(t.plane)], heads_ref.at[:, lanes(there)]
    copies = [
        copy(mine, t.me, None, t.right, 0),
        copy(mine, t.me, None, t.left, 1),
        copy(theirs, t.me, None, t.pair, 2),
        copy(None, t.left, lo, t.right, 3),
        copy(None, t.right, hi, t.left, 4),
        copy(None, t.pair, None, t.right, 5),
        copy(None, t.pair, None, t.left, 6),
        copy(None, t.on(there, 3), lo, t.right, 7),
        copy(None, t.on(there, 1), hi, t.left, 8),
    ]
    for i in (2, 0, 1):
        copies[i].start()
    heads[t.me] = heads_ref[:, lanes(t.plane)]

    @pl.when(t.plane == 0)
    def _():
        first.wait()

    @pl.when(t.plane == 1)
    def _():
        second.wait()

    mixed[...] = tokens[...].astype(F32)
    weights_out()

    def group(i, carry):
        for when, waits, starts in (
            (1, (2,), (5, 6)),
            (2, (0,), (3,)),
            (3, (1, 5), (4, 7)),
            (4, (6,), (8,)),
            (6, (3, 4), ()),
            (7, (7, 8), ()),
        ):
            @pl.when(i == when)
            def _():
                for one in waits:
                    copies[one].wait_recv()
                for one in starts:
                    copies[one].start()

        step = lax.rem(3 * (i // 2) * (i // 2 + 1) // 2, RING)
        side = lax.rem(t.plane + i, 2)
        who = side * RING + lax.rem(t.x + step, RING)
        mixed[...] += lax.dot_general(
            heads[who], w_out[who], (((0,), (0,)), ((), ())), preferred_element_type=F32
        )
        return carry

    lax.fori_loop(0, 2 * RING, group, 0)
    for load in loads:
        load.wait()
    weights_in()

    cut = part // 2
    lo, hi = pl.ds(0, cut), pl.ds(cut, cut)
    right, left, far = (lax.rem(t.x + step, RING) for step in (1, 3, 2))

    def sums(src, dst, i, to):
        return send(src, dst, s_send.at[i], s_recv.at[i], to)

    half_left = sums(term.at[far, lo], half_in.at[0], 0, t.left)
    half_right = sums(term.at[far, hi], half_in.at[1], 1, t.right)
    edge_right = sums(term.at[right, lo], edge_in.at[0, lo], 2, t.right)
    edge_left = sums(term.at[left, hi], edge_in.at[1, hi], 3, t.left)
    sum_left = sums(edge_sum.at[0], edge_in.at[1, lo], 4, t.left)
    sum_right = sums(edge_sum.at[1], edge_in.at[0, hi], 5, t.right)
    rows_of = lambda b: pl.ds(pl.multiple_of(b * part, part), part)

    def feed(i, carry):
        b = lax.rem(t.x + 2 + 3 * i * (i + 1) // 2, RING)
        post = layer_norm(mixed[rows_of(b)], gain_ref[...].reshape(1, -1)).astype(BF16)
        wide = lambda k: jax.nn.gelu(dot(post, up[k]), approximate=True).astype(BF16)
        term[b] = (dot(wide(0), down[0]) + dot(wide(1), down[1])).astype(BF16)
        for when, starts in ((0, (half_left, half_right)), (1, (edge_right,)), (2, (edge_left,))):
            @pl.when(i == when)
            def _():
                for one in starts:
                    one.start()
        return carry

    lax.fori_loop(0, RING, feed, 0)
    half_left.wait_recv()
    edge_sum[0] = (half_in[0].astype(F32) + term[left, lo].astype(F32)).astype(BF16)
    sum_left.start()
    half_right.wait_recv()
    edge_sum[1] = (half_in[1].astype(F32) + term[right, hi].astype(F32)).astype(BF16)
    sum_right.start()
    base = mixed[rows_of(t.x)] + term[t.x].astype(F32)
    mixed[rows_of(t.x)] = base
    for one in (edge_right, edge_left, sum_left, sum_right):
        one.wait_recv()
    own[...] = (mixed[rows_of(t.x)] + edge_in[0].astype(F32) + edge_in[1].astype(F32)).astype(BF16)
    out_ref[t.me] = own[...]
    for one in (*copies, half_left, half_right, edge_right, edge_left, sum_left, sum_right):
        one.wait_send()
    gather(t, own, out_ref, cut, g_send, g_recv)


def layer(tokens, gain, w_qkv, w_out, post_gain, up, down, part, n_tensor):
    rows, model = tokens.shape
    half, padded = RING * part, n_tensor * part
    span = w_out.shape[0]
    dma = lambda n: pltpu.SemaphoreType.DMA((n,))
    vmem = pl.BlockSpec(memory_space=pltpu.VMEM)
    hbm = pl.BlockSpec(memory_space=pltpu.HBM)
    held = lambda *shape: pltpu.VMEM(shape, BF16)
    return pl.pallas_call(
        attend_kernel,
        in_specs=[hbm, vmem, hbm, hbm, vmem, hbm, hbm],
        out_specs=vmem,
        out_shape=jax.ShapeDtypeStruct((n_tensor, part, model), BF16),
        scratch_shapes=[
            held(span, padded),
            held(n_tensor, *w_out.shape),
            held(2, *up.shape),
            held(2, *down.shape),
            held(*tokens.shape),
            held(*w_qkv.shape),
            held(RING, HD, rows),
            held(RING, 2 * HD, rows),
            held(RING, HD, rows),
            held(BLOCKS, 2 * HD, rows),
            held(BLOCKS, rows, HD),
            held(BLOCKS, HD + 16, rows),
            pltpu.VMEM((RING, HD + 16, rows), F32),
            pltpu.VMEM((RING, 1, rows), F32),
            pltpu.VMEM((2, rows + 8, rows), F32),
            held(RING, HD, padded),
            dma(RING), dma(RING), dma(RING), dma(BLOCKS), dma(BLOCKS), dma(BLOCKS), dma(RING), dma(RING),
            dma(7), dma(7), dma(7), dma(7), dma(1),
            dma(4), dma(4), dma(4), dma(4), dma(8), dma(8), dma(2),
            held(n_tensor, span, half),
            held(half, model),
            pltpu.VMEM((half, model), F32),
            held(RING, part, model),
            held(part, model),
            held(2, part // 2, model),
            held(2, part, model),
            held(2, part // 2, model),
            dma(9), dma(9), dma(6), dma(6), dma(9), dma(9), dma(3),
        ],
        cost_estimate=pl.CostEstimate(flops=100 * 10**9, bytes_accessed=30 << 20, transcendentals=0),
        compiler_params=pltpu.CompilerParams(
            vmem_limit_bytes=GRANT, collective_id=0, has_side_effects=True
        ),
    )(tokens, gain, w_qkv, w_out, post_gain, up, down)


def per_device(n_seq, n_tensor, tokens, norm_gain, w_qkv, w_out, post_gain, w_up, w_down):
    rows, model = tokens.shape
    span = w_qkv.shape[2]
    part = -(-rows // (16 * n_tensor)) * 16
    out = layer(
        tokens, norm_gain, w_qkv.transpose(1, 2, 0).reshape(3 * span, model), w_out, post_gain, w_up, w_down,
        part, n_tensor,
    )
    return out.reshape(n_tensor * part, model)[:rows]


def solution(mesh):
    placed = (
        P("seq", None),
        P(),
        P(None, None, "tensor"),
        P("tensor", None),
        P(),
        P(None, "tensor"),
        P("tensor", None),
    )
    body = functools.partial(per_device, mesh.shape["seq"], mesh.shape["tensor"])
    return jax.shard_map(
        body, mesh=mesh, in_specs=placed, out_specs=P("seq", None), check_vma=False
    )
```

```python
import functools
import jax
import jax.numpy as jnp
from jax import lax
from jax.experimental import pallas as pl
from jax.experimental.pallas import tpu as pltpu
from jax.sharding import PartitionSpec as P

HD = 48
LOG2E = 1.4426950408889634
MESH = pl.DeviceIdType.MESH
F32 = jnp.float32
BF16 = jnp.bfloat16
RING = 4
GRANT = 58 << 20
BLOCKS = 16
TILES = (slice(0, 256), slice(256, 512), slice(512, 720))


def layer_norm(values, gain):
    mean = jnp.mean(values, axis=-1, keepdims=True)
    centred = values - mean
    var = jnp.mean(centred * centred, axis=-1, keepdims=True)
    return centred * lax.rsqrt(var + 1e-05) * gain


def dot(a, b):
    return jnp.dot(a, b, preferred_element_type=F32)


def remote(src, dst, send, recv, seq):
    return pltpu.make_async_remote_copy(
        src_ref=src, dst_ref=dst, send_sem=send, recv_sem=recv, device_id={"seq": seq}, device_id_type=MESH
    )


def attend_kernel(
    tokens_hbm, gain_ref, w_qkv_hbm, w_hbm, post_gain_ref, up_hbm, down_hbm, out_ref,
    heads_ref, w_all, up, down, tokens, w_qkv, q_ref, kv_ref, q_in, kv_in, key_rows, values, acc, peak, scores, obuf,
    q_send, q_recv, y_send, z_send, d_send, kv_recv, o_send, o_recv, w_send, w_recv, t_send, t_recv, w_own,
    f_send, f_recv, g_send, g_recv, h_send, h_recv, load_sem, *tail_scratch,
):
    rows = q_ref.shape[2]
    loads = (
        pltpu.make_async_copy(tokens_hbm, tokens, load_sem.at[0]),
        pltpu.make_async_copy(w_qkv_hbm, w_qkv, load_sem.at[1]),
    )
    for load in loads:
        load.start()
    me = lax.axis_index("seq")
    half, y, core = me // (2 * RING), (me // 2) % RING, me % 2

    def at(step):
        return half * (2 * RING) + lax.rem(y + step, RING) * 2 + core

    twin = me - core + (1 - core)
    far = lax.rem(me + 2 * RING, BLOCKS)
    peers = [at(1), at(2), at(3), twin, far]
    tensor = lax.axis_index("tensor")
    plane, x = tensor // RING, lax.rem(tensor, RING)

    def on(side, step):
        return side * RING + lax.rem(x + step, RING)

    friends = [on(plane, 1), on(plane, 2), on(plane, 3), on(1 - plane, 0)]
    barrier = pltpu.get_barrier_semaphore()
    for peer in peers:
        pl.semaphore_signal(barrier, inc=1, device_id={"seq": peer}, device_id_type=MESH)
    for friend in friends:
        pl.semaphore_signal(barrier, inc=1, device_id={"tensor": friend}, device_id_type=MESH)
    across = on(1 - plane, 0)
    pl.semaphore_signal(barrier, inc=1, device_id={"seq": far, "tensor": across}, device_id_type=MESH)
    w_load = pltpu.make_async_copy(w_hbm, w_all.at[tensor], w_own.at[0])
    w_load.start()
    values[:, HD:, :] = jnp.ones((BLOCKS, values.shape[1] - HD, rows), BF16)
    acc[...] = jnp.zeros_like(acc)
    peak[...] = jnp.full_like(peak, -1e30)
    obuf[:, :, rows:] = jnp.zeros((RING, HD, obuf.shape[2] - rows), BF16)
    loads[0].wait()
    some = rows // 5

    def norm(i, carry):
        where = pl.ds(pl.multiple_of(i * some, some), some)
        tokens[where] = layer_norm(tokens[where].astype(F32), gain_ref[...].reshape(1, -1)).astype(BF16)
        return carry

    lax.fori_loop(0, 5, norm, 0)
    loads[1].wait()
    for lanes in TILES:
        found = lax.dot_general(
            w_qkv[...], tokens[lanes], (((1,), (1,)), ((), ())), preferred_element_type=F32
        ).reshape(3, RING, HD, lanes.stop - lanes.start)
        q_ref[:, :, lanes] = (found[0] * (LOG2E / HD**0.5)).astype(BF16)
        kv_ref[:, :HD, lanes] = found[1].astype(BF16)
        kv_ref[:, HD:, lanes] = found[2].astype(BF16)
    pl.semaphore_wait(barrier, len(peers) + len(friends) + 1)

    pieces = 2 * RING
    both = ((up_hbm, up), (down_hbm, down))

    def spot(k, number):
        size = both[k][0].shape[0] // pieces
        return both[k][1].at[1, pl.ds(pl.multiple_of(number * size, size), size)]

    def piece(j, which):
        return lax.rem(y + (0, 2, 1, 3)[j], RING) * 2 + which

    def f_copy(k, j):
        ref = both[k][0]
        size = ref.shape[0] // pieces
        number = piece(j, core)
        src = ref.at[pl.ds(pl.multiple_of(number * size, size), size)]
        device = {"tensor": across} if k == 0 else {"seq": far, "tensor": across}
        return pltpu.make_async_remote_copy(
            src_ref=src, dst_ref=spot(k, number), send_sem=f_send.at[2 * k + j], recv_sem=f_recv.at[2 * k + j],
            device_id=device, device_id_type=MESH,
        )

    def g_copy(k, step):
        number = piece(0, core)
        i = 2 * k + step // 2
        j = 2 * k + 1 - step // 2
        return remote(spot(k, number), spot(k, number), g_send.at[i], g_recv.at[j], at(step))

    def h_copy(k, j, which):
        number = piece(j, which)
        i = 4 * k + j
        return remote(spot(k, number), spot(k, number), h_send.at[i], h_recv.at[i], twin)

    cut = w_hbm.shape[0] // 2
    rows_of = lambda which: pl.ds(pl.multiple_of(which * cut, cut), cut)

    def w_copy(src, owner, index, friend):
        return pltpu.make_async_remote_copy(
            src_ref=src, dst_ref=w_all.at[owner, rows_of(core)], send_sem=w_send.at[index], recv_sem=w_recv.at[index],
            device_id={"tensor": friend}, device_id_type=MESH,
        )

    def w_of(side, step, index, friend):
        owner = on(side, step)
        return w_copy(w_all.at[owner, rows_of(core)], owner, index, friend)

    def t_copy(index, which):
        owner = on(plane, index + 1) if index < 3 else on(1 - plane, index - 3)
        return remote(
            w_all.at[owner, rows_of(which)], w_all.at[owner, rows_of(which)], t_send.at[index], t_recv.at[index], twin
        )

    w_mine = w_all.at[tensor, rows_of(core)]

    def arrived(index):
        w_copy(w_mine, tensor, index, tensor).wait_recv()
        t_copy(index, core).start()

    def pass_on(c):
        @pl.when(c == 5)
        def _():
            for k in range(2):
                f_copy(k, 0).wait_recv()
                for step in (1, 3):
                    g_copy(k, step).start()
                h_copy(k, 0, core).start()

        @pl.when(c == 6)
        def _():
            arrived(3)
            for step in (1, 3, 2):
                w_copy(w_all.at[across, rows_of(core)], across, 3 + RING - step, on(plane, step)).start()

        @pl.when(c == 7)
        def _():
            for k in range(2):
                f_copy(k, 1).start()

        @pl.when(c == 11)
        def _():
            for index in (0, 2, 1):
                arrived(index)

    def q_copy(step):
        return remote(
            q_ref.at[lax.rem(y + step, RING)], q_in.at[RING - step], q_send.at[step], q_recv.at[RING - step], at(step)
        )

    def y_copy(step):
        slot = {1: 3, 2: 6, 3: 2}[step]
        return remote(
            kv_ref.at[lax.rem(y + step, RING)], kv_in.at[slot], y_send.at[step], kv_recv.at[slot], at(step)
        )

    def z_copy(src, slot):
        return remote(src, kv_in.at[slot], z_send.at[slot], kv_recv.at[slot], far)

    def d_copy(src, slot):
        return remote(src, kv_in.at[slot], d_send.at[slot], kv_recv.at[slot], twin)

    own = kv_ref.at[y]
    d_copy(own, 1).start()
    for step in (1, 3):
        q_copy(step).start()
    for step in (1, 3):
        y_copy(step).start()
    q_copy(2).start()
    y_copy(2).start()
    z_copy(own, 8).start()
    f_copy(0, 0).start()
    f_copy(1, 0).start()
    w_load.wait()
    w_copy(w_mine, tensor, 3, across).start()
    for step in (1, 3, 2):
        w_copy(w_mine, tensor, RING - step - 1, on(plane, step)).start()

    q_in[0] = q_ref[y]
    key_rows[0] = kv_ref[y, :HD].T
    values[0, :HD] = kv_ref[y, HD:]

    def arrive(c):
        d_copy(kv_in.at[c], c).wait_recv()

        @pl.when((c == 2) | (c == 3))
        def _():
            d_copy(kv_in.at[c], c + 2).start()
            z_copy(kv_in.at[c], 2 * c + 6).start()

        @pl.when(c == 6)
        def _():
            d_copy(kv_in.at[c], c + 1).start()
            z_copy(kv_in.at[c], 14).start()

        @pl.when((c >= 8) & (lax.rem(c, 2) == 0))
        def _():
            d_copy(kv_in.at[c], c + 1).start()

        pass_on(c)

    def prepare(c):
        key_rows[c] = kv_in[c, :HD].T
        values[c, :HD] = kv_in[c, HD:]

    def score(c, s, b):
        for lanes in TILES:
            found = dot(key_rows[c], q_in[s, :, lanes])
            scores[b, :rows, lanes] = found
            scores[b, rows : rows + 1, lanes] = jnp.max(found, axis=0, keepdims=True)

    def weigh(c, s, b):
        for lanes in TILES:
            old = peak[s, :, lanes]
            new = jnp.maximum(old, scores[b, rows : rows + 1, lanes])
            peak[s, :, lanes] = new
            weights = jnp.exp2(scores[b, :rows, lanes] - new).astype(BF16)
            acc[s, :, lanes] = acc[s, :, lanes] * jnp.exp2(old - new) + dot(values[c], weights)

    head = lambda which: pl.ds(pl.multiple_of(which * HD, HD), HD)

    def o_copy(step):
        return remote(obuf.at[step], heads_ref.at[head(y)], o_send.at[step], o_recv.at[RING - step], at(step))

    opening = [(c, s) for s in (0, 1, 3) for c in (0, 1)] + [(2, s) for s in (3, 0, 1)] + [(c, 2) for c in (0, 1, 2)]
    last = 12
    order = (3, 0, 1, 2)
    met = {0}
    score(0, 0, 0)
    for i, (c, s) in enumerate(opening):
        after = opening[i + 1] if i + 1 < len(opening) else (3, order[0])
        if i in (0, 5, len(opening) - 1):
            arrive(jnp.int32(after[0]))
            prepare(after[0])
        if after[1] not in met:
            q_copy(RING - after[1]).wait_recv()
            met.add(after[1])
        score(*after, (i + 1) % 2)
        weigh(c, s, i % 2)

    def body(c, carry):
        arrive(c + 1)

        @pl.when(c == last - 1)
        def _():
            arrive(jnp.int32(14))

        for i, s in enumerate(order):
            if i < 3:
                score(c, order[i + 1], 1 - i % 2)
            else:
                score(c + 1, order[0], 0)
            if i == 2:
                prepare(c + 1)
            weigh(c, s, i % 2)
        return carry

    lax.fori_loop(3, last, body, 0)

    arrive(jnp.int32(13))
    arrive(jnp.int32(15))
    for k in range(2):
        for step in (1, 3):
            g_copy(k, step).wait_recv()
        for j in (2, 3):
            h_copy(k, j, core).start()
    for c in range(last + 1, BLOCKS):
        prepare(c)

    def close(i, carry):
        s = RING - 1 - i
        for k in range(RING):
            if k < RING - 1:
                score(last + k + 1, s, 1 - k % 2)
            else:
                score(last, jnp.maximum(s - 1, 0), 0)
            weigh(last + k, s, k % 2)
        result = (acc[s, :HD] / acc[s, HD : HD + 1]).astype(BF16)

        @pl.when(s > 0)
        def _():
            obuf[s, :, :rows] = result
            o_copy(s).start()

        @pl.when(s == 0)
        def _():
            heads_ref[head(y), :rows] = result

        @pl.when(s == 1)
        def _():
            for k in range(2):
                f_copy(k, 1).wait_recv()
                h_copy(k, 1, core).start()
            for index in (4, 6, 5):
                arrived(index)

        return carry

    lax.fori_loop(0, RING, close, 0)
    heads_ref[head(y), rows:] = jnp.zeros((HD, heads_ref.shape[1] - rows), BF16)

    def o_wait(step):
        return remote(
            obuf.at[step], heads_ref.at[head(lax.rem(y + step, RING))], o_send.at[step], o_recv.at[step], at(step)
        )

    for step in (1, 2, 3):
        q_copy(step).wait_send()
        y_copy(step).wait_send()
        o_copy(step).wait_send()
    for slot in (8, 10, 12, 14):
        z_copy(own, slot).wait_send()
    for slot in (1, 4, 5, 7, 9, 11, 13, 15):
        d_copy(own, slot).wait_send()
    for step in (1, 3, 2):
        o_wait(step).wait_recv()

    def weights_out():
        for index in range(7):
            t_copy(index, 1 - core).wait_recv()

    def weights_in():
        for k in range(2):
            for j in range(4):
                h_copy(k, j, 1 - core).wait_recv()

    tail_kernel(
        heads_ref, tokens_hbm, post_gain_ref, up_hbm, down_hbm, out_ref, w_all, up, down,
        weights_out, weights_in, *tail_scratch,
    )
    for index in range(7):
        w_copy(w_mine, tensor, index, tensor).wait_send()
        t_copy(index, core).wait_send()
    for k in range(2):
        for j in range(2):
            f_copy(k, j).wait_send()
        for step in (1, 3):
            g_copy(k, step).wait_send()
        for j in range(4):
            h_copy(k, j, core).wait_send()


class Tensor:
    def __init__(self):
        self.me = lax.axis_index("tensor")
        self.plane, self.x = self.me // RING, lax.rem(self.me, RING)
        self.right, self.left = self.on(self.plane, 1), self.on(self.plane, 3)
        self.pair = self.on(1 - self.plane, 0)

    def on(self, side, step):
        return side * RING + lax.rem(self.x + step, RING)

    def meet(self):
        barrier = pltpu.get_barrier_semaphore()
        for friend in (self.right, self.left, self.pair):
            pl.semaphore_signal(barrier, inc=1, device_id={"tensor": friend}, device_id_type=MESH)
        pl.semaphore_wait(barrier, 3)


def send(src, dst, send_sem, recv_sem, friend):
    return pltpu.make_async_remote_copy(
        src_ref=src, dst_ref=dst, send_sem=send_sem, recv_sem=recv_sem,
        device_id={"tensor": friend}, device_id_type=MESH,
    )


def gather(t, mine, buf, cut, send_sem, recv_sem):
    lo, hi = pl.ds(0, cut), pl.ds(cut, cut)
    copies = {
        "right lo": (mine, t.me, lo, t.right, 0),
        "left hi": (mine, t.me, hi, t.left, 1),
        "over lo": (mine, t.me, lo, t.pair, 2),
        "right hi": (mine, t.me, hi, t.right, 3),
        "left lo": (mine, t.me, lo, t.left, 4),
        "over hi": (mine, t.me, hi, t.pair, 5),
        "far lo": (None, t.left, lo, t.right, 6),
        "far hi": (None, t.right, hi, t.left, 7),
        "over right": (None, t.pair, None, t.right, 8),
        "over left": (None, t.pair, None, t.left, 9),
        "pair lo": (None, t.on(t.plane, 2), lo, t.pair, 10),
        "pair hi": (None, t.on(t.plane, 2), hi, t.pair, 11),
    }

    def copy(name):
        src, block, part, to, i = copies[name]
        dst = buf.at[block] if part is None else buf.at[block, part]
        return send(dst if src is None else src.at[part], dst, send_sem.at[i], recv_sem.at[i], to)

    for name in ("right lo", "left hi", "over lo", "right hi", "left lo", "over hi"):
        copy(name).start()
    copy("right lo").wait_recv()
    copy("far lo").start()
    copy("left hi").wait_recv()
    copy("far hi").start()
    copy("over lo").wait_recv()
    copy("over hi").wait_recv()
    copy("over right").start()
    copy("over left").start()
    copy("far lo").wait_recv()
    copy("pair lo").start()
    copy("far hi").wait_recv()
    copy("pair hi").start()
    for name in ("right hi", "left lo", "over right", "over left", "pair lo", "pair hi"):
        copy(name).wait_recv()
    for name in copies:
        copy(name).wait_send()


def tail_kernel(
    heads_ref, tokens_hbm, gain_ref, up_hbm, down_hbm, out_ref, w_out, up, down, weights_out, weights_in,
    heads, tokens, mixed, term, own, half_in, edge_in, edge_sum,
    a_send, a_recv, s_send, s_recv, g_send, g_recv, load_sem,
):
    t = Tensor()
    half, model = mixed.shape
    part = half // RING
    there = 1 - t.plane
    valid = tokens_hbm.shape[0] - half
    loads = [
        pltpu.make_async_copy(up_hbm, up.at[0], load_sem.at[0]),
        pltpu.make_async_copy(down_hbm, down.at[0], load_sem.at[1]),
    ]
    first = pltpu.make_async_copy(tokens_hbm.at[pl.ds(0, half)], tokens, load_sem.at[2])
    second = pltpu.make_async_copy(tokens_hbm.at[pl.ds(half, valid)], tokens.at[pl.ds(0, valid)], load_sem.at[2])

    @pl.when(t.plane == 0)
    def _():
        first.start()

    @pl.when(t.plane == 1)
    def _():
        second.start()
        tokens[valid:] = jnp.zeros((half - valid, model), BF16)

    for load in loads:
        load.start()

    cut = heads_ref.shape[0] // 2
    lo, hi = pl.ds(0, cut), pl.ds(cut, cut)
    lanes = lambda plane: pl.ds(pl.multiple_of(plane * half, half), half)

    def copy(src, block, rows, to, i):
        dst = heads.at[block] if rows is None else heads.at[block, rows]
        return send(dst if src is None else src, dst, a_send.at[i], a_recv.at[i], to)

    mine = lambda rows: heads_ref.at[rows, lanes(t.plane)]
    copies = [
        copy(mine(lo), t.me, lo, t.right, 0),
        copy(mine(hi), t.me, hi, t.left, 1),
        copy(heads_ref.at[:, lanes(there)], t.me, None, t.pair, 2),
        copy(mine(hi), t.me, hi, t.right, 3),
        copy(mine(lo), t.me, lo, t.left, 4),
        copy(None, t.left, lo, t.right, 5),
        copy(None, t.right, hi, t.left, 6),
        copy(None, t.pair, lo, t.right, 7),
        copy(None, t.pair, hi, t.left, 8),
        copy(None, t.pair, hi, t.right, 9),
        copy(None, t.pair, lo, t.left, 10),
        copy(None, t.on(there, 3), lo, t.right, 11),
        copy(None, t.on(there, 1), hi, t.left, 12),
    ]
    for i in (2, 0, 1, 3, 4):
        copies[i].start()
    heads[t.me] = heads_ref[:, lanes(t.plane)]

    @pl.when(t.plane == 0)
    def _():
        first.wait()

    @pl.when(t.plane == 1)
    def _():
        second.wait()

    mixed[...] = tokens[...].astype(F32)
    weights_out()

    def group(i, carry):
        for when, pairs in (
            (1, ((2, (7, 8, 9, 10)),)),
            (2, ((0, (5,)), (1, (6,)), (3, ()))),
            (3, ((7, (11,)), (8, (12,)), (9, ()))),
            (4, ((4, ()),)),
            (5, ((10, ()),)),
            (6, ((5, ()), (6, ()))),
            (7, ((11, ()), (12, ()))),
        ):
            @pl.when(i == when)
            def _():
                for wait, starts in pairs:
                    copies[wait].wait_recv()
                    for one in starts:
                        copies[one].start()

        step = lax.rem(3 * (i // 2) * (i // 2 + 1) // 2, RING)
        side = lax.rem(t.plane + i, 2)
        who = side * RING + lax.rem(t.x + step, RING)
        mixed[...] += lax.dot_general(
            heads[who], w_out[who], (((0,), (0,)), ((), ())), preferred_element_type=F32
        )
        return carry

    lax.fori_loop(0, 2 * RING, group, 0)
    for load in loads:
        load.wait()
    weights_in()

    cut = part // 2
    lo, hi = pl.ds(0, cut), pl.ds(cut, cut)
    right, left, far = (lax.rem(t.x + step, RING) for step in (1, 3, 2))

    def sums(src, dst, i, to):
        return send(src, dst, s_send.at[i], s_recv.at[i], to)

    half_left = sums(term.at[far, lo], half_in.at[0], 0, t.left)
    half_right = sums(term.at[far, hi], half_in.at[1], 1, t.right)
    edge_right = sums(term.at[right, lo], edge_in.at[0, lo], 2, t.right)
    edge_left = sums(term.at[left, hi], edge_in.at[1, hi], 3, t.left)
    sum_left = sums(edge_sum.at[0], edge_in.at[1, lo], 4, t.left)
    sum_right = sums(edge_sum.at[1], edge_in.at[0, hi], 5, t.right)
    rows_of = lambda b: pl.ds(pl.multiple_of(b * part, part), part)

    def feed(i, carry):
        b = lax.rem(t.x + 2 + 3 * i * (i + 1) // 2, RING)
        post = layer_norm(mixed[rows_of(b)], gain_ref[...].reshape(1, -1)).astype(BF16)
        wide = lambda k: jax.nn.gelu(dot(post, up[k]), approximate=True).astype(BF16)
        term[b] = (dot(wide(0), down[0]) + dot(wide(1), down[1])).astype(BF16)
        for when, starts in ((0, (half_left, half_right)), (1, (edge_right,)), (2, (edge_left,))):
            @pl.when(i == when)
            def _():
                for one in starts:
                    one.start()
        return carry

    lax.fori_loop(0, RING, feed, 0)
    half_left.wait_recv()
    edge_sum[0] = (half_in[0].astype(F32) + term[left, lo].astype(F32)).astype(BF16)
    sum_left.start()
    half_right.wait_recv()
    edge_sum[1] = (half_in[1].astype(F32) + term[right, hi].astype(F32)).astype(BF16)
    sum_right.start()
    base = mixed[rows_of(t.x)] + term[t.x].astype(F32)
    mixed[rows_of(t.x)] = base
    for one in (edge_right, edge_left, sum_left, sum_right):
        one.wait_recv()
    own[...] = (mixed[rows_of(t.x)] + edge_in[0].astype(F32) + edge_in[1].astype(F32)).astype(BF16)
    out_ref[t.me] = own[...]
    for one in (*copies, half_left, half_right, edge_right, edge_left, sum_left, sum_right):
        one.wait_send()
    gather(t, own, out_ref, cut, g_send, g_recv)


def layer(tokens, gain, w_qkv, w_out, post_gain, up, down, part, n_tensor):
    rows, model = tokens.shape
    half, padded = RING * part, n_tensor * part
    span = w_out.shape[0]
    dma = lambda n: pltpu.SemaphoreType.DMA((n,))
    vmem = pl.BlockSpec(memory_space=pltpu.VMEM)
    hbm = pl.BlockSpec(memory_space=pltpu.HBM)
    held = lambda *shape: pltpu.VMEM(shape, BF16)
    return pl.pallas_call(
        attend_kernel,
        in_specs=[hbm, vmem, hbm, hbm, vmem, hbm, hbm],
        out_specs=vmem,
        out_shape=pltpu.VMEM((n_tensor, part, model), BF16),
        scratch_shapes=[
            held(span, padded),
            held(n_tensor, *w_out.shape),
            held(2, *up.shape),
            held(2, *down.shape),
            held(*tokens.shape),
            held(*w_qkv.shape),
            held(RING, HD, rows),
            held(RING, 2 * HD, rows),
            held(RING, HD, rows),
            held(BLOCKS, 2 * HD, rows),
            held(BLOCKS, rows, HD),
            held(BLOCKS, HD + 16, rows),
            pltpu.VMEM((RING, HD + 16, rows), F32),
            pltpu.VMEM((RING, 1, rows), F32),
            pltpu.VMEM((2, rows + 8, rows), F32),
            held(RING, HD, padded),
            dma(RING), dma(RING), dma(RING), dma(BLOCKS), dma(BLOCKS), dma(BLOCKS), dma(RING), dma(RING),
            dma(7), dma(7), dma(7), dma(7), dma(1),
            dma(4), dma(4), dma(4), dma(4), dma(8), dma(8), dma(2),
            held(n_tensor, span, half),
            held(half, model),
            pltpu.VMEM((half, model), F32),
            held(RING, part, model),
            held(part, model),
            held(2, part // 2, model),
            held(2, part, model),
            held(2, part // 2, model),
            dma(13), dma(13), dma(6), dma(6), dma(12), dma(12), dma(3),
        ],
        cost_estimate=pl.CostEstimate(flops=100 * 10**9, bytes_accessed=30 << 20, transcendentals=0),
        compiler_params=pltpu.CompilerParams(
            vmem_limit_bytes=GRANT, collective_id=0, has_side_effects=True
        ),
    )(tokens, gain, w_qkv, w_out, post_gain, up, down)


def per_device(n_seq, n_tensor, tokens, norm_gain, w_qkv, w_out, post_gain, w_up, w_down):
    rows, model = tokens.shape
    span = w_qkv.shape[2]
    part = -(-rows // (16 * n_tensor)) * 16
    out = layer(
        tokens, norm_gain, w_qkv.transpose(1, 2, 0).reshape(3 * span, model), w_out, post_gain, w_up, w_down,
        part, n_tensor,
    )
    return out.reshape(n_tensor * part, model)[:rows]


def solution(mesh):
    placed = (
        P("seq", None),
        P(),
        P(None, None, "tensor"),
        P("tensor", None),
        P(),
        P(None, "tensor"),
        P("tensor", None),
    )
    body = functools.partial(per_device, mesh.shape["seq"], mesh.shape["tensor"])
    return jax.shard_map(
        body, mesh=mesh, in_specs=placed, out_specs=P("seq", None), check_vma=False
    )
```

```python
import functools
import jax
import jax.numpy as jnp
from jax import lax
from jax.experimental import pallas as pl
from jax.experimental.pallas import tpu as pltpu
from jax.sharding import PartitionSpec as P

HD = 48
LOG2E = 1.4426950408889634
MESH = pl.DeviceIdType.MESH
F32 = jnp.float32
BF16 = jnp.bfloat16
RING = 4
GRANT = 58 << 20
BLOCKS = 16
TILES = (slice(0, 256), slice(256, 512), slice(512, 720))


def layer_norm(values, gain):
    mean = jnp.mean(values, axis=-1, keepdims=True)
    centred = values - mean
    var = jnp.mean(centred * centred, axis=-1, keepdims=True)
    return centred * lax.rsqrt(var + 1e-05) * gain


def dot(a, b):
    return jnp.dot(a, b, preferred_element_type=F32)


def remote(src, dst, send, recv, seq):
    return pltpu.make_async_remote_copy(
        src_ref=src, dst_ref=dst, send_sem=send, recv_sem=recv, device_id={"seq": seq}, device_id_type=MESH
    )


def attend_kernel(
    tokens_hbm, gain_ref, w_qkv_hbm, w_hbm, post_gain_ref, up_hbm, down_hbm, out_ref,
    heads_ref, w_all, up, down, tokens, w_qkv, q_ref, kv_ref, q_in, kv_in, key_rows, values, acc, peak, scores, obuf,
    q_send, q_recv, y_send, z_send, d_send, kv_recv, o_send, o_recv, w_send, w_recv, t_send, t_recv, w_own,
    f_send, f_recv, g_send, g_recv, h_send, h_recv, load_sem, *tail_scratch,
):
    rows = q_ref.shape[2]
    loads = [
        *(pltpu.make_async_copy(tokens_hbm.at[pl.ds(t.start, t.stop - t.start)], tokens.at[pl.ds(t.start, t.stop - t.start)], load_sem.at[i]) for i, t in enumerate(TILES)),
        pltpu.make_async_copy(w_qkv_hbm, w_qkv, load_sem.at[3]),
    ]
    for load in loads:
        load.start()
    me = lax.axis_index("seq")
    half, y, core = me // (2 * RING), (me // 2) % RING, me % 2

    def at(step):
        return half * (2 * RING) + lax.rem(y + step, RING) * 2 + core

    twin = me - core + (1 - core)
    far = lax.rem(me + 2 * RING, BLOCKS)
    peers = [at(1), at(2), at(3), twin, far]
    tensor = lax.axis_index("tensor")
    plane, x = tensor // RING, lax.rem(tensor, RING)

    def on(side, step):
        return side * RING + lax.rem(x + step, RING)

    friends = [on(plane, 1), on(plane, 2), on(plane, 3), on(1 - plane, 0)]
    barrier = pltpu.get_barrier_semaphore()
    for peer in peers:
        pl.semaphore_signal(barrier, inc=1, device_id={"seq": peer}, device_id_type=MESH)
    for friend in friends:
        pl.semaphore_signal(barrier, inc=1, device_id={"tensor": friend}, device_id_type=MESH)
    across = on(1 - plane, 0)
    pl.semaphore_signal(barrier, inc=1, device_id={"seq": far, "tensor": across}, device_id_type=MESH)
    w_load = pltpu.make_async_copy(w_hbm, w_all.at[tensor], w_own.at[0])
    w_load.start()
    values[:, HD:, :] = jnp.ones((BLOCKS, values.shape[1] - HD, rows), BF16)
    acc[...] = jnp.zeros_like(acc)
    peak[...] = jnp.full_like(peak, -1e30)
    obuf[:, :, rows:] = jnp.zeros((RING, HD, obuf.shape[2] - rows), BF16)
    def norm(where):
        tokens[where] = layer_norm(tokens[where].astype(F32), gain_ref[...].reshape(1, -1)).astype(BF16)

    loads[0].wait()
    norm(TILES[0])
    for load in loads[1:]:
        load.wait()
    for i, lanes in enumerate(TILES):
        found = lax.dot_general(
            w_qkv[...], tokens[lanes], (((1,), (1,)), ((), ())), preferred_element_type=F32
        ).reshape(3, RING, HD, lanes.stop - lanes.start)
        if i + 1 < len(TILES):
            norm(TILES[i + 1])
        q_ref[:, :, lanes] = (found[0] * (LOG2E / HD**0.5)).astype(BF16)
        kv_ref[:, :HD, lanes] = found[1].astype(BF16)
        kv_ref[:, HD:, lanes] = found[2].astype(BF16)
    pl.semaphore_wait(barrier, len(peers) + len(friends) + 1)

    pieces = 2 * RING
    both = ((up_hbm, up), (down_hbm, down))

    def spot(k, number):
        size = both[k][0].shape[0] // pieces
        return both[k][1].at[1, pl.ds(pl.multiple_of(number * size, size), size)]

    def piece(j, which):
        return lax.rem(y + (0, 2, 1, 3)[j], RING) * 2 + which

    def f_copy(k, j):
        ref = both[k][0]
        size = ref.shape[0] // pieces
        number = piece(j, core)
        src = ref.at[pl.ds(pl.multiple_of(number * size, size), size)]
        device = {"tensor": across} if k == 0 else {"seq": far, "tensor": across}
        return pltpu.make_async_remote_copy(
            src_ref=src, dst_ref=spot(k, number), send_sem=f_send.at[2 * k + j], recv_sem=f_recv.at[2 * k + j],
            device_id=device, device_id_type=MESH,
        )

    def g_copy(k, step):
        number = piece(0, core)
        i = 2 * k + step // 2
        j = 2 * k + 1 - step // 2
        return remote(spot(k, number), spot(k, number), g_send.at[i], g_recv.at[j], at(step))

    def h_copy(k, j, which):
        number = piece(j, which)
        i = 4 * k + j
        return remote(spot(k, number), spot(k, number), h_send.at[i], h_recv.at[i], twin)

    cut = w_hbm.shape[0] // 2
    rows_of = lambda which: pl.ds(pl.multiple_of(which * cut, cut), cut)

    def w_copy(src, owner, index, friend):
        return pltpu.make_async_remote_copy(
            src_ref=src, dst_ref=w_all.at[owner, rows_of(core)], send_sem=w_send.at[index], recv_sem=w_recv.at[index],
            device_id={"tensor": friend}, device_id_type=MESH,
        )

    def w_of(side, step, index, friend):
        owner = on(side, step)
        return w_copy(w_all.at[owner, rows_of(core)], owner, index, friend)

    def t_copy(index, which):
        owner = on(plane, index + 1) if index < 3 else on(1 - plane, index - 3)
        return remote(
            w_all.at[owner, rows_of(which)], w_all.at[owner, rows_of(which)], t_send.at[index], t_recv.at[index], twin
        )

    w_mine = w_all.at[tensor, rows_of(core)]

    def arrived(index):
        w_copy(w_mine, tensor, index, tensor).wait_recv()
        t_copy(index, core).start()

    def pass_on(c):
        @pl.when(c == 5)
        def _():
            for k in range(2):
                f_copy(k, 0).wait_recv()
                for step in (1, 3):
                    g_copy(k, step).start()
                h_copy(k, 0, core).start()

        @pl.when(c == 6)
        def _():
            arrived(3)
            for step in (1, 3, 2):
                w_copy(w_all.at[across, rows_of(core)], across, 3 + RING - step, on(plane, step)).start()

        @pl.when(c == 7)
        def _():
            for k in range(2):
                f_copy(k, 1).start()

        @pl.when(c == 11)
        def _():
            for index in (0, 2, 1):
                arrived(index)

    def q_copy(step):
        return remote(
            q_ref.at[lax.rem(y + step, RING)], q_in.at[RING - step], q_send.at[step], q_recv.at[RING - step], at(step)
        )

    def y_copy(step):
        slot = {1: 3, 2: 6, 3: 2}[step]
        return remote(
            kv_ref.at[lax.rem(y + step, RING)], kv_in.at[slot], y_send.at[step], kv_recv.at[slot], at(step)
        )

    def z_copy(src, slot):
        return remote(src, kv_in.at[slot], z_send.at[slot], kv_recv.at[slot], far)

    def d_copy(src, slot):
        return remote(src, kv_in.at[slot], d_send.at[slot], kv_recv.at[slot], twin)

    own = kv_ref.at[y]
    d_copy(own, 1).start()
    for step in (1, 3):
        q_copy(step).start()
    for step in (1, 3):
        y_copy(step).start()
    q_copy(2).start()
    y_copy(2).start()
    z_copy(own, 8).start()
    f_copy(0, 0).start()
    f_copy(1, 0).start()
    w_load.wait()
    w_copy(w_mine, tensor, 3, across).start()
    for step in (1, 3, 2):
        w_copy(w_mine, tensor, RING - step - 1, on(plane, step)).start()

    q_in[0] = q_ref[y]
    key_rows[0] = kv_ref[y, :HD].T
    values[0, :HD] = kv_ref[y, HD:]

    def arrive(c):
        d_copy(kv_in.at[c], c).wait_recv()

        @pl.when((c == 2) | (c == 3))
        def _():
            d_copy(kv_in.at[c], c + 2).start()
            z_copy(kv_in.at[c], 2 * c + 6).start()

        @pl.when(c == 6)
        def _():
            d_copy(kv_in.at[c], c + 1).start()
            z_copy(kv_in.at[c], 14).start()

        @pl.when((c >= 8) & (lax.rem(c, 2) == 0))
        def _():
            d_copy(kv_in.at[c], c + 1).start()

        pass_on(c)

    def prepare(c):
        key_rows[c] = kv_in[c, :HD].T
        values[c, :HD] = kv_in[c, HD:]

    def score(c, s, b):
        for lanes in TILES:
            found = dot(key_rows[c], q_in[s, :, lanes])
            scores[b, :rows, lanes] = found
            scores[b, rows : rows + 1, lanes] = jnp.max(found, axis=0, keepdims=True)

    def weigh(c, s, b):
        for lanes in TILES:
            old = peak[s, :, lanes]
            new = jnp.maximum(old, scores[b, rows : rows + 1, lanes])
            peak[s, :, lanes] = new
            weights = jnp.exp2(scores[b, :rows, lanes] - new).astype(BF16)
            acc[s, :, lanes] = acc[s, :, lanes] * jnp.exp2(old - new) + dot(values[c], weights)

    head = lambda which: pl.ds(pl.multiple_of(which * HD, HD), HD)

    def o_copy(step):
        return remote(obuf.at[step], heads_ref.at[head(y)], o_send.at[step], o_recv.at[RING - step], at(step))

    opening = [(c, s) for s in (0, 1, 3) for c in (0, 1)] + [(2, s) for s in (3, 0, 1)] + [(c, 2) for c in (0, 1, 2)]
    last = 12
    order = (3, 0, 1, 2)
    met = {0}
    score(0, 0, 0)
    for i, (c, s) in enumerate(opening):
        after = opening[i + 1] if i + 1 < len(opening) else (3, order[0])
        if i in (0, 5, len(opening) - 1):
            arrive(jnp.int32(after[0]))
            prepare(after[0])
        if after[1] not in met:
            q_copy(RING - after[1]).wait_recv()
            met.add(after[1])
        score(*after, (i + 1) % 2)
        weigh(c, s, i % 2)

    def body(c, carry):
        arrive(c + 1)

        @pl.when(c == last - 1)
        def _():
            arrive(jnp.int32(14))

        for i, s in enumerate(order):
            if i < 3:
                score(c, order[i + 1], 1 - i % 2)
            else:
                score(c + 1, order[0], 0)
            if i == 2:
                prepare(c + 1)
            weigh(c, s, i % 2)
        return carry

    lax.fori_loop(3, last, body, 0)

    arrive(jnp.int32(13))
    arrive(jnp.int32(15))
    for k in range(2):
        for step in (1, 3):
            g_copy(k, step).wait_recv()
        for j in (2, 3):
            h_copy(k, j, core).start()
    for c in range(last + 1, BLOCKS):
        prepare(c)

    def close(i, carry):
        s = RING - 1 - i
        for k in range(RING):
            if k < RING - 1:
                score(last + k + 1, s, 1 - k % 2)
            else:
                score(last, jnp.maximum(s - 1, 0), 0)
            weigh(last + k, s, k % 2)
        result = (acc[s, :HD] / acc[s, HD : HD + 1]).astype(BF16)

        @pl.when(s > 0)
        def _():
            obuf[s, :, :rows] = result
            o_copy(s).start()

        @pl.when(s == 0)
        def _():
            heads_ref[head(y), :rows] = result

        @pl.when(s == 1)
        def _():
            for k in range(2):
                f_copy(k, 1).wait_recv()
                h_copy(k, 1, core).start()
            for index in (4, 6, 5):
                arrived(index)

        return carry

    lax.fori_loop(0, RING, close, 0)
    heads_ref[head(y), rows:] = jnp.zeros((HD, heads_ref.shape[1] - rows), BF16)

    def o_wait(step):
        return remote(
            obuf.at[step], heads_ref.at[head(lax.rem(y + step, RING))], o_send.at[step], o_recv.at[step], at(step)
        )

    for step in (1, 2, 3):
        q_copy(step).wait_send()
        y_copy(step).wait_send()
        o_copy(step).wait_send()
    for slot in (8, 10, 12, 14):
        z_copy(own, slot).wait_send()
    for slot in (1, 4, 5, 7, 9, 11, 13, 15):
        d_copy(own, slot).wait_send()
    for step in (1, 3, 2):
        o_wait(step).wait_recv()

    def weights_out():
        for index in range(7):
            t_copy(index, 1 - core).wait_recv()

    def weights_in():
        for k in range(2):
            for j in range(4):
                h_copy(k, j, 1 - core).wait_recv()

    tail_kernel(
        heads_ref, tokens_hbm, post_gain_ref, up_hbm, down_hbm, out_ref, w_all, up, down,
        weights_out, weights_in, *tail_scratch,
    )
    for index in range(7):
        w_copy(w_mine, tensor, index, tensor).wait_send()
        t_copy(index, core).wait_send()
    for k in range(2):
        for j in range(2):
            f_copy(k, j).wait_send()
        for step in (1, 3):
            g_copy(k, step).wait_send()
        for j in range(4):
            h_copy(k, j, core).wait_send()


class Tensor:
    def __init__(self):
        self.me = lax.axis_index("tensor")
        self.plane, self.x = self.me // RING, lax.rem(self.me, RING)
        self.right, self.left = self.on(self.plane, 1), self.on(self.plane, 3)
        self.pair = self.on(1 - self.plane, 0)

    def on(self, side, step):
        return side * RING + lax.rem(self.x + step, RING)

    def meet(self):
        barrier = pltpu.get_barrier_semaphore()
        for friend in (self.right, self.left, self.pair):
            pl.semaphore_signal(barrier, inc=1, device_id={"tensor": friend}, device_id_type=MESH)
        pl.semaphore_wait(barrier, 3)


def send(src, dst, send_sem, recv_sem, friend):
    return pltpu.make_async_remote_copy(
        src_ref=src, dst_ref=dst, send_sem=send_sem, recv_sem=recv_sem,
        device_id={"tensor": friend}, device_id_type=MESH,
    )


def gather(t, mine, buf, cut, send_sem, recv_sem):
    lo, hi = pl.ds(0, cut), pl.ds(cut, cut)
    copies = {
        "right lo": (mine, t.me, lo, t.right, 0),
        "left hi": (mine, t.me, hi, t.left, 1),
        "over lo": (mine, t.me, lo, t.pair, 2),
        "right hi": (mine, t.me, hi, t.right, 3),
        "left lo": (mine, t.me, lo, t.left, 4),
        "over hi": (mine, t.me, hi, t.pair, 5),
        "far lo": (None, t.left, lo, t.right, 6),
        "far hi": (None, t.right, hi, t.left, 7),
        "over right": (None, t.pair, None, t.right, 8),
        "over left": (None, t.pair, None, t.left, 9),
        "pair lo": (None, t.on(t.plane, 2), lo, t.pair, 10),
        "pair hi": (None, t.on(t.plane, 2), hi, t.pair, 11),
    }

    def copy(name):
        src, block, part, to, i = copies[name]
        dst = buf.at[block] if part is None else buf.at[block, part]
        return send(dst if src is None else src.at[part], dst, send_sem.at[i], recv_sem.at[i], to)

    for name in ("right lo", "left hi", "over lo", "right hi", "left lo", "over hi"):
        copy(name).start()
    copy("right lo").wait_recv()
    copy("far lo").start()
    copy("left hi").wait_recv()
    copy("far hi").start()
    copy("over lo").wait_recv()
    copy("over hi").wait_recv()
    copy("over right").start()
    copy("over left").start()
    copy("far lo").wait_recv()
    copy("pair lo").start()
    copy("far hi").wait_recv()
    copy("pair hi").start()
    for name in ("right hi", "left lo", "over right", "over left", "pair lo", "pair hi"):
        copy(name).wait_recv()
    for name in copies:
        copy(name).wait_send()


def tail_kernel(
    heads_ref, tokens_hbm, gain_ref, up_hbm, down_hbm, out_ref, w_out, up, down, weights_out, weights_in,
    heads, tokens, mixed, term, own, half_in, edge_in, edge_sum,
    a_send, a_recv, s_send, s_recv, g_send, g_recv, load_sem,
):
    t = Tensor()
    half, model = mixed.shape
    part = half // RING
    there = 1 - t.plane
    valid = tokens_hbm.shape[0] - half
    loads = [
        pltpu.make_async_copy(up_hbm, up.at[0], load_sem.at[0]),
        pltpu.make_async_copy(down_hbm, down.at[0], load_sem.at[1]),
    ]
    first = pltpu.make_async_copy(tokens_hbm.at[pl.ds(0, half)], tokens, load_sem.at[2])
    second = pltpu.make_async_copy(tokens_hbm.at[pl.ds(half, valid)], tokens.at[pl.ds(0, valid)], load_sem.at[2])

    @pl.when(t.plane == 0)
    def _():
        first.start()

    @pl.when(t.plane == 1)
    def _():
        second.start()
        tokens[valid:] = jnp.zeros((half - valid, model), BF16)

    for load in loads:
        load.start()

    cut = heads_ref.shape[0] // 2
    lo, hi = pl.ds(0, cut), pl.ds(cut, cut)
    lanes = lambda plane: pl.ds(pl.multiple_of(plane * half, half), half)

    def copy(src, block, rows, to, i):
        dst = heads.at[block] if rows is None else heads.at[block, rows]
        return send(dst if src is None else src, dst, a_send.at[i], a_recv.at[i], to)

    mine = lambda rows: heads_ref.at[rows, lanes(t.plane)]
    copies = [
        copy(mine(lo), t.me, lo, t.right, 0),
        copy(mine(hi), t.me, hi, t.left, 1),
        copy(heads_ref.at[:, lanes(there)], t.me, None, t.pair, 2),
        copy(mine(hi), t.me, hi, t.right, 3),
        copy(mine(lo), t.me, lo, t.left, 4),
        copy(None, t.left, lo, t.right, 5),
        copy(None, t.right, hi, t.left, 6),
        copy(None, t.pair, lo, t.right, 7),
        copy(None, t.pair, hi, t.left, 8),
        copy(None, t.pair, hi, t.right, 9),
        copy(None, t.pair, lo, t.left, 10),
        copy(None, t.on(there, 3), lo, t.right, 11),
        copy(None, t.on(there, 1), hi, t.left, 12),
    ]
    for i in (2, 0, 1, 3, 4):
        copies[i].start()
    heads[t.me] = heads_ref[:, lanes(t.plane)]

    @pl.when(t.plane == 0)
    def _():
        first.wait()

    @pl.when(t.plane == 1)
    def _():
        second.wait()

    mixed[...] = tokens[...].astype(F32)
    weights_out()

    def group(i, carry):
        for when, pairs in (
            (1, ((2, (7, 8, 9, 10)),)),
            (2, ((0, (5,)), (1, (6,)), (3, ()))),
            (3, ((7, (11,)), (8, (12,)), (9, ()))),
            (4, ((4, ()),)),
            (5, ((10, ()),)),
            (6, ((5, ()), (6, ()))),
            (7, ((11, ()), (12, ()))),
        ):
            @pl.when(i == when)
            def _():
                for wait, starts in pairs:
                    copies[wait].wait_recv()
                    for one in starts:
                        copies[one].start()

        step = lax.rem(3 * (i // 2) * (i // 2 + 1) // 2, RING)
        side = lax.rem(t.plane + i, 2)
        who = side * RING + lax.rem(t.x + step, RING)
        mixed[...] += lax.dot_general(
            heads[who], w_out[who], (((0,), (0,)), ((), ())), preferred_element_type=F32
        )
        return carry

    lax.fori_loop(0, 2 * RING, group, 0)
    for load in loads:
        load.wait()
    weights_in()

    cut = part // 2
    lo, hi = pl.ds(0, cut), pl.ds(cut, cut)
    right, left, far = (lax.rem(t.x + step, RING) for step in (1, 3, 2))

    def sums(src, dst, i, to):
        return send(src, dst, s_send.at[i], s_recv.at[i], to)

    half_left = sums(term.at[far, lo], half_in.at[0], 0, t.left)
    half_right = sums(term.at[far, hi], half_in.at[1], 1, t.right)
    edge_right = sums(term.at[right, lo], edge_in.at[0, lo], 2, t.right)
    edge_left = sums(term.at[left, hi], edge_in.at[1, hi], 3, t.left)
    sum_left = sums(edge_sum.at[0], edge_in.at[1, lo], 4, t.left)
    sum_right = sums(edge_sum.at[1], edge_in.at[0, hi], 5, t.right)
    rows_of = lambda b: pl.ds(pl.multiple_of(b * part, part), part)

    def feed(i, carry):
        b = lax.rem(t.x + 2 + 3 * i * (i + 1) // 2, RING)
        post = layer_norm(mixed[rows_of(b)], gain_ref[...].reshape(1, -1)).astype(BF16)
        wide = lambda k: jax.nn.gelu(dot(post, up[k]), approximate=True).astype(BF16)
        term[b] = (dot(wide(0), down[0]) + dot(wide(1), down[1])).astype(BF16)
        for when, starts in ((0, (half_left, half_right)), (1, (edge_right,)), (2, (edge_left,))):
            @pl.when(i == when)
            def _():
                for one in starts:
                    one.start()
        return carry

    lax.fori_loop(0, RING, feed, 0)
    half_left.wait_recv()
    edge_sum[0] = (half_in[0].astype(F32) + term[left, lo].astype(F32)).astype(BF16)
    sum_left.start()
    half_right.wait_recv()
    edge_sum[1] = (half_in[1].astype(F32) + term[right, hi].astype(F32)).astype(BF16)
    sum_right.start()
    base = mixed[rows_of(t.x)] + term[t.x].astype(F32)
    mixed[rows_of(t.x)] = base
    for one in (edge_right, edge_left, sum_left, sum_right):
        one.wait_recv()
    own[...] = (mixed[rows_of(t.x)] + edge_in[0].astype(F32) + edge_in[1].astype(F32)).astype(BF16)
    out_ref[t.me] = own[...]
    for one in (*copies, half_left, half_right, edge_right, edge_left, sum_left, sum_right):
        one.wait_send()
    gather(t, own, out_ref, cut, g_send, g_recv)


def layer(tokens, gain, w_qkv, w_out, post_gain, up, down, part, n_tensor):
    rows, model = tokens.shape
    half, padded = RING * part, n_tensor * part
    span = w_out.shape[0]
    dma = lambda n: pltpu.SemaphoreType.DMA((n,))
    vmem = pl.BlockSpec(memory_space=pltpu.VMEM)
    hbm = pl.BlockSpec(memory_space=pltpu.HBM)
    held = lambda *shape: pltpu.VMEM(shape, BF16)
    return pl.pallas_call(
        attend_kernel,
        in_specs=[hbm, vmem, hbm, hbm, vmem, hbm, hbm],
        out_specs=vmem,
        out_shape=pltpu.VMEM((n_tensor, part, model), BF16),
        scratch_shapes=[
            held(span, padded),
            held(n_tensor, *w_out.shape),
            held(2, *up.shape),
            held(2, *down.shape),
            held(*tokens.shape),
            held(*w_qkv.shape),
            held(RING, HD, rows),
            held(RING, 2 * HD, rows),
            held(RING, HD, rows),
            held(BLOCKS, 2 * HD, rows),
            held(BLOCKS, rows, HD),
            held(BLOCKS, HD + 16, rows),
            pltpu.VMEM((RING, HD + 16, rows), F32),
            pltpu.VMEM((RING, 1, rows), F32),
            pltpu.VMEM((2, rows + 8, rows), F32),
            held(RING, HD, padded),
            dma(RING), dma(RING), dma(RING), dma(BLOCKS), dma(BLOCKS), dma(BLOCKS), dma(RING), dma(RING),
            dma(7), dma(7), dma(7), dma(7), dma(1),
            dma(4), dma(4), dma(4), dma(4), dma(8), dma(8), dma(4),
            held(n_tensor, span, half),
            held(half, model),
            pltpu.VMEM((half, model), F32),
            held(RING, part, model),
            held(part, model),
            held(2, part // 2, model),
            held(2, part, model),
            held(2, part // 2, model),
            dma(13), dma(13), dma(6), dma(6), dma(12), dma(12), dma(3),
        ],
        cost_estimate=pl.CostEstimate(flops=100 * 10**9, bytes_accessed=30 << 20, transcendentals=0),
        compiler_params=pltpu.CompilerParams(
            vmem_limit_bytes=GRANT, collective_id=0, has_side_effects=True
        ),
    )(tokens, gain, w_qkv, w_out, post_gain, up, down)


def per_device(n_seq, n_tensor, tokens, norm_gain, w_qkv, w_out, post_gain, w_up, w_down):
    rows, model = tokens.shape
    span = w_qkv.shape[2]
    part = -(-rows // (16 * n_tensor)) * 16
    out = layer(
        tokens, norm_gain, w_qkv.transpose(1, 2, 0).reshape(3 * span, model), w_out, post_gain, w_up, w_down,
        part, n_tensor,
    )
    return out.reshape(n_tensor * part, model)[:rows]


def solution(mesh):
    placed = (
        P("seq", None),
        P(),
        P(None, None, "tensor"),
        P("tensor", None),
        P(),
        P(None, "tensor"),
        P("tensor", None),
    )
    body = functools.partial(per_device, mesh.shape["seq"], mesh.shape["tensor"])
    return jax.shard_map(
        body, mesh=mesh, in_specs=placed, out_specs=P("seq", None), check_vma=False
    )
```
